8 devices in a mesh: dp: 2 (over z, y), tp: 4 (over x, core).
Axes of the slice: x: 2, y: 2, z: 1, core: 2. Of those that a mesh axis runs over, the one named last changes fastest.
Arguments:
- x_in: bfloat16 [8, 1024, 640], P('dp', 'tp'), parts along dimension 0
- grad_y: bfloat16 [8, 1024, 640], P('dp', 'tp'), parts along dimension 0
- pad_mask: int32 [8, 1024], P('dp'), parts along dimension 0
- ln1_gain: float32 [640], replicated
- ln1_bias: float32 [640], replicated
- w_qkv: bfloat16 [3, 640, 20, 32], P(None, None, 'tp')
- b_qkv: float32 [3, 20, 32], P(None, 'tp')
- w_out: bfloat16 [20, 32, 640], P('tp')
- b_out: float32 [640], replicated
- ln2_gain: float32 [640], replicated
- ln2_bias: float32 [640], replicated
- w_up: bfloat16 [640, 2560], P(None, 'tp')
- b_up: float32 [2560], P('tp')
- w_down: bfloat16 [2560, 640], P('tp')
- b_down: float32 [640], replicated
Outputs:
- output 1: bfloat16 [8, 1024, 640], P('dp', 'tp'), parts along dimension 0
- output 2: bfloat16 [8, 1024, 640], P('dp', 'tp'), parts along dimension 0
- output 3: float32 [1280], P('dp'), parts along dimension 0
- output 4: float32 [1280], P('dp'), parts along dimension 0
- output 5: float32 [6, 640, 20, 32], P('dp', None, 'tp'), parts along dimension 0
- output 6: float32 [6, 20, 32], P('dp', 'tp'), parts along dimension 0
- output 7: float32 [40, 32, 640], P(('dp', 'tp')), parts along dimension 0
- output 8: float32 [1280], P('dp'), parts along dimension 0
- output 9: float32 [1280], P('dp'), parts along dimension 0
- output 10: float32 [1280], P('dp'), parts along dimension 0
- output 11: float32 [1280, 2560], P('dp', 'tp'), parts along dimension 0
- output 12: float32 [5120], P(('dp', 'tp')), parts along dimension 0
- output 13: float32 [5120, 640], P(('dp', 'tp')), parts along dimension 0
- output 14: float32 [1280], P('dp'), parts along dimension 0
There are 2 independent parts. The reference program is written for one: setup_inputs(seed, part) draws one part's arguments, and reference() takes and returns one part's arrays. A program takes and returns all parts, laid end to end along the dimension named above; an argument that names none is the same for every part.
All inputs are finite; a program needn't handle non-finite values.
Results may differ from the reference program's by a relative error of at most 0.0125188.
Values are sent between devices in bfloat16 or wider.
A program may use at most 1 GiB of HBM per device.

```python
import jax
import jax.numpy as jnp
from jax import lax

BATCH_SEQS = 4
SEQ_LEN = 1024
MODEL_DIM = 640
NUM_HEADS = 20
HEAD_DIM = 32
FFN_DIM = 2560
HALF_DIM = HEAD_DIM // 2
TOKENS = BATCH_SEQS * SEQ_LEN
LN_EPS = 1e-5
ROPE_BASE = 10000.0
INV_SQRT2 = 0.7071067811865476
INV_SQRT_2PI = 0.3989422804014327
NEG_LARGE = -1e30


def setup_inputs(seed: int = 0, part: int = 0) -> dict:
    root_key = jax.random.key(seed)
    shared_key, data_key = jax.random.split(root_key)
    weight_keys = jax.random.split(shared_key, 12)
    part_key = jax.random.fold_in(data_key, part)
    data_keys = jax.random.split(part_key, 4)
    tok_shape = (BATCH_SEQS, SEQ_LEN, MODEL_DIM)
    row_scale = 0.5 + jax.random.uniform(data_keys[0], (BATCH_SEQS, SEQ_LEN, 1), jnp.float32)
    x_in = (jax.random.normal(data_keys[1], tok_shape, jnp.float32) * row_scale).astype(jnp.bfloat16)
    grad_y = jax.random.normal(data_keys[2], tok_shape, jnp.float32).astype(jnp.bfloat16)
    lengths = jax.random.randint(data_keys[3], (BATCH_SEQS,), SEQ_LEN // 8, SEQ_LEN + 1)
    pad_mask = (jnp.arange(SEQ_LEN)[None, :] < lengths[:, None]).astype(jnp.int32)
    qkv_gain = jnp.array([1.5, 1.5, 1.0], jnp.float32)[:, None, None, None]
    w_qkv = jax.random.normal(weight_keys[0], (3, MODEL_DIM, NUM_HEADS, HEAD_DIM), jnp.float32) * qkv_gain * MODEL_DIM ** -0.5
    w_out = jax.random.normal(weight_keys[1], (NUM_HEADS, HEAD_DIM, MODEL_DIM), jnp.float32) * MODEL_DIM ** -0.5
    w_up = jax.random.normal(weight_keys[2], (MODEL_DIM, FFN_DIM), jnp.float32) * MODEL_DIM ** -0.5
    w_down = jax.random.normal(weight_keys[3], (FFN_DIM, MODEL_DIM), jnp.float32) * FFN_DIM ** -0.5
    return {
        'x_in': x_in,
        'grad_y': grad_y,
        'pad_mask': pad_mask,
        'ln1_gain': 1.0 + 0.2 * jax.random.normal(weight_keys[4], (MODEL_DIM,), jnp.float32),
        'ln1_bias': 0.2 * jax.random.normal(weight_keys[5], (MODEL_DIM,), jnp.float32),
        'w_qkv': w_qkv.astype(jnp.bfloat16),
        'b_qkv': 0.5 * jax.random.normal(weight_keys[6], (3, NUM_HEADS, HEAD_DIM), jnp.float32),
        'w_out': w_out.astype(jnp.bfloat16),
        'b_out': 0.3 * jax.random.normal(weight_keys[7], (MODEL_DIM,), jnp.float32),
        'ln2_gain': 1.0 + 0.2 * jax.random.normal(weight_keys[8], (MODEL_DIM,), jnp.float32),
        'ln2_bias': 0.2 * jax.random.normal(weight_keys[9], (MODEL_DIM,), jnp.float32),
        'w_up': w_up.astype(jnp.bfloat16),
        'b_up': 0.5 * jax.random.normal(weight_keys[10], (FFN_DIM,), jnp.float32),
        'w_down': w_down.astype(jnp.bfloat16),
        'b_down': 0.3 * jax.random.normal(weight_keys[11], (MODEL_DIM,), jnp.float32),
    }


def layer_norm(values, ln_gain, ln_bias):
    centered = values - jnp.mean(values, axis=-1, keepdims=True)
    inv_std = lax.rsqrt(jnp.mean(centered * centered, axis=-1, keepdims=True) + LN_EPS)
    x_hat = centered * inv_std
    return x_hat * ln_gain + ln_bias, x_hat, inv_std


def layer_norm_grad(d_out, x_hat, inv_std, ln_gain):
    d_hat = d_out * ln_gain
    return inv_std * (d_hat - jnp.mean(d_hat, axis=-1, keepdims=True) - x_hat * jnp.mean(d_hat * x_hat, axis=-1, keepdims=True))


def rope_tables():
    inv_freq = ROPE_BASE ** (-2.0 * jnp.arange(HALF_DIM, dtype=jnp.float32) / HEAD_DIM)
    angles = jnp.arange(SEQ_LEN, dtype=jnp.float32)[:, None] * inv_freq[None, :]
    angles = jnp.concatenate([angles, angles], axis=-1)
    return jnp.cos(angles)[:, None, :], jnp.sin(angles)[:, None, :]


def rotate(tensor, cos_tab, sin_tab):
    swapped = jnp.concatenate([-tensor[..., HALF_DIM:], tensor[..., :HALF_DIM]], axis=-1)
    return tensor * cos_tab + swapped * sin_tab


def rotate_back(grad_in, cos_tab, sin_tab):
    scaled = grad_in * sin_tab
    swapped = jnp.concatenate([scaled[..., HALF_DIM:], -scaled[..., :HALF_DIM]], axis=-1)
    return grad_in * cos_tab + swapped


def attention_probs(q_seq, k_seq, key_ok):
    scores = jnp.einsum('qhk,shk->hqs', q_seq.astype(jnp.float32), k_seq.astype(jnp.float32))
    return jax.nn.softmax(jnp.where(key_ok[None, None, :], scores, NEG_LARGE), axis=-1)


def seq_attention(operands):
    q_seq, k_seq, v_seq, key_ok = operands
    probs_low = attention_probs(q_seq, k_seq, key_ok).astype(jnp.bfloat16)
    return jnp.einsum('hqs,shk->qhk', probs_low.astype(jnp.float32), v_seq.astype(jnp.float32)).astype(jnp.bfloat16)


def seq_attention_grad(operands):
    q_seq, k_seq, v_seq, key_ok, d_out = operands
    attn_probs = attention_probs(q_seq, k_seq, key_ok)
    probs_low = attn_probs.astype(jnp.bfloat16).astype(jnp.float32)
    d_out_f = d_out.astype(jnp.float32)
    d_value = jnp.einsum('hqs,qhk->shk', probs_low, d_out_f)
    d_probs = jnp.einsum('qhk,shk->hqs', d_out_f, v_seq.astype(jnp.float32))
    d_scores = attn_probs * (d_probs - jnp.sum(d_probs * attn_probs, axis=-1, keepdims=True))
    d_scores_low = d_scores.astype(jnp.bfloat16).astype(jnp.float32)
    d_query = jnp.einsum('hqs,shk->qhk', d_scores_low, k_seq.astype(jnp.float32))
    d_key = jnp.einsum('hqs,qhk->shk', d_scores_low, q_seq.astype(jnp.float32))
    return d_query, d_key, d_value


def reference(x_in, grad_y, pad_mask, ln1_gain, ln1_bias, w_qkv, b_qkv, w_out, b_out, ln2_gain, ln2_bias, w_up, b_up, w_down, b_down):
    q_scale = HEAD_DIM ** -0.5
    cos_tab, sin_tab = rope_tables()
    key_ok = pad_mask > 0
    x_f = x_in.astype(jnp.float32)
    h1_f, x_hat1, inv_std1 = layer_norm(x_f, ln1_gain, ln1_bias)
    h1_b = h1_f.astype(jnp.bfloat16)
    qkv_all = jnp.einsum('bsd,idhk->ibshk', h1_b.astype(jnp.float32), w_qkv.astype(jnp.float32)) + b_qkv[:, None, None]
    q_rot = rotate(qkv_all[0] * q_scale, cos_tab, sin_tab).astype(jnp.bfloat16)
    k_rot = rotate(qkv_all[1], cos_tab, sin_tab).astype(jnp.bfloat16)
    v_heads = qkv_all[2].astype(jnp.bfloat16)
    attn_o = lax.map(seq_attention, (q_rot, k_rot, v_heads, key_ok))
    attn_sum = jnp.einsum('bshk,hkd->bsd', attn_o.astype(jnp.float32), w_out.astype(jnp.float32)) + b_out
    x1_f = (x_f + attn_sum).astype(jnp.bfloat16).astype(jnp.float32)
    h2_f, x_hat2, inv_std2 = layer_norm(x1_f, ln2_gain, ln2_bias)
    h2_flat = h2_f.astype(jnp.bfloat16).reshape(TOKENS, MODEL_DIM)
    pre_act = jnp.dot(h2_flat, w_up, preferred_element_type=jnp.float32) + b_up
    erf_term = lax.erf(pre_act * INV_SQRT2)
    act_b = (0.5 * pre_act * (1.0 + erf_term)).astype(jnp.bfloat16)
    gelu_slope = 0.5 * (1.0 + erf_term) + pre_act * jnp.exp(-0.5 * pre_act * pre_act) * INV_SQRT_2PI
    mlp_sum = jnp.dot(act_b, w_down, preferred_element_type=jnp.float32) + b_down
    y_out = (x1_f + mlp_sum.reshape(x_f.shape)).astype(jnp.bfloat16)
    dy_flat = grad_y.reshape(TOKENS, MODEL_DIM)
    dy_f = grad_y.astype(jnp.float32)
    grad_b_down = jnp.sum(dy_f, axis=(0, 1))
    grad_w_down = jnp.dot(act_b.T, dy_flat, preferred_element_type=jnp.float32)
    d_act = jnp.dot(dy_flat, w_down.T, preferred_element_type=jnp.float32)
    d_pre = d_act * gelu_slope
    grad_b_up = jnp.sum(d_pre, axis=0)
    d_pre_b = d_pre.astype(jnp.bfloat16)
    grad_w_up = jnp.dot(h2_flat.T, d_pre_b, preferred_element_type=jnp.float32)
    d_h2 = jnp.dot(d_pre_b, w_up.T, preferred_element_type=jnp.float32).reshape(x_f.shape)
    grad_ln2_gain = jnp.sum(d_h2 * x_hat2, axis=(0, 1))
    grad_ln2_bias = jnp.sum(d_h2, axis=(0, 1))
    d_x1 = dy_f + layer_norm_grad(d_h2, x_hat2, inv_std2, ln2_gain)
    grad_b_out = jnp.sum(d_x1, axis=(0, 1))
    d_x1_b = d_x1.astype(jnp.bfloat16).astype(jnp.float32)
    grad_w_out = jnp.einsum('bshk,bsd->hkd', attn_o.astype(jnp.float32), d_x1_b)
    d_attn_o = jnp.einsum('bsd,hkd->bshk', d_x1_b, w_out.astype(jnp.float32)).astype(jnp.bfloat16)
    d_query, d_key, d_value = lax.map(seq_attention_grad, (q_rot, k_rot, v_heads, key_ok, d_attn_o))
    d_qkv = jnp.stack([rotate_back(d_query, cos_tab, sin_tab) * q_scale, rotate_back(d_key, cos_tab, sin_tab), d_value])
    grad_b_qkv = jnp.sum(d_qkv, axis=(1, 2))
    d_qkv_b = d_qkv.astype(jnp.bfloat16).astype(jnp.float32)
    grad_w_qkv = jnp.einsum('bsd,ibshk->idhk', h1_b.astype(jnp.float32), d_qkv_b)
    d_h1 = jnp.einsum('ibshk,idhk->bsd', d_qkv_b, w_qkv.astype(jnp.float32))
    grad_ln1_gain = jnp.sum(d_h1 * x_hat1, axis=(0, 1))
    grad_ln1_bias = jnp.sum(d_h1, axis=(0, 1))
    grad_x = (d_x1 + layer_norm_grad(d_h1, x_hat1, inv_std1, ln1_gain)).astype(jnp.bfloat16)
    return (y_out, grad_x, grad_ln1_gain, grad_ln1_bias, grad_w_qkv, grad_b_qkv, grad_w_out, grad_b_out, grad_ln2_gain, grad_ln2_bias, grad_w_up, grad_b_up, grad_w_down, grad_b_down)
```

```python
import functools

import jax
import jax.numpy as jnp
from jax import lax
from jax.experimental import pallas as pl
from jax.experimental.pallas import tpu as pltpu
from jax.sharding import PartitionSpec as P

LN_EPS = 1e-5
ROPE_BASE = 10000.0
INV_SQRT2 = 0.7071067811865476
INV_SQRT_2PI = 0.3989422804014327
NEG_LARGE = -1e30
F32 = jnp.float32
BF16 = jnp.bfloat16
KEY_STEP = 256


def dot(lhs, rhs):
    return jnp.dot(lhs, rhs, preferred_element_type=F32)


def layer_norm(values, ln_gain, ln_bias):
    centered = values - jnp.mean(values, axis=-1, keepdims=True)
    inv_std = lax.rsqrt(jnp.mean(centered * centered, axis=-1, keepdims=True) + LN_EPS)
    x_hat = centered * inv_std
    return x_hat * ln_gain + ln_bias, x_hat, inv_std


def layer_norm_grad(d_out, x_hat, inv_std, ln_gain):
    d_hat = d_out * ln_gain
    return inv_std * (d_hat - jnp.mean(d_hat, axis=-1, keepdims=True) - x_hat * jnp.mean(d_hat * x_hat, axis=-1, keepdims=True))


def rope_tables(seq_len, head_dim):
    half_dim = head_dim // 2
    inv_freq = ROPE_BASE ** (-2.0 * jnp.arange(half_dim, dtype=F32) / head_dim)
    angles = inv_freq[:, None] * jnp.arange(seq_len, dtype=F32)[None, :]
    angles = jnp.concatenate([angles, angles], axis=0)
    return jnp.cos(angles), jnp.sin(angles)


def rotate(tensor, cos_tab, sin_tab):
    half_dim = tensor.shape[-2] // 2
    swapped = jnp.concatenate([-tensor[..., half_dim:, :], tensor[..., :half_dim, :]], axis=-2)
    return tensor * cos_tab + swapped * sin_tab


def rotate_back(grad_in, cos_tab, sin_tab):
    half_dim = grad_in.shape[-2] // 2
    scaled = grad_in * sin_tab
    swapped = jnp.concatenate([scaled[..., half_dim:, :], -scaled[..., :half_dim, :]], axis=-2)
    return grad_in * cos_tab + swapped


def masked_scores(k_ref, q, length, keys):
    scores = dot(k_ref[0, :, :keys].T, q)
    tail = keys - KEY_STEP
    rows = lax.broadcasted_iota(jnp.int32, (KEY_STEP, scores.shape[1]), 0) + tail
    last = jnp.where(rows < length, scores[tail:], NEG_LARGE)
    return last if tail == 0 else jnp.concatenate([scores[:tail], last], axis=0)


def for_key_count(length, seq_len, body):
    blocks = lax.div(length + KEY_STEP - 1, KEY_STEP)
    for count in range(1, seq_len // KEY_STEP + 1):
        pl.when(blocks == count)(functools.partial(body, count * KEY_STEP))


def attn_fwd_kernel(len_ref, q_ref, k_ref, v_ref, o_ref, o_wide_ref, lse_ref):
    length = len_ref[0]

    def body(keys):
        scores = masked_scores(k_ref, q_ref[0], length, keys)
        top = jnp.max(scores, axis=0, keepdims=True)
        weights = jnp.exp(scores - top)
        total = jnp.sum(weights, axis=0, keepdims=True)
        out = dot(v_ref[0, :, :keys], weights.astype(BF16)) / total
        o_ref[0] = out.astype(BF16)
        o_wide_ref[0] = out
        lse_ref[0] = top + jnp.log(total)

    for_key_count(length, q_ref.shape[-1], body)


def attn_bwd_kernel(len_ref, q_ref, k_ref, v_ref, do_ref, o_wide_ref, lse_ref, dq_ref, dk_ref, dv_ref):
    length = len_ref[0]
    dk_ref[...] = jnp.zeros_like(dk_ref)
    dv_ref[...] = jnp.zeros_like(dv_ref)

    def body(keys):
        q, d_out = q_ref[0], do_ref[0]
        delta = jnp.sum(d_out.astype(F32) * o_wide_ref[0], axis=0, keepdims=True)
        probs = jnp.exp(masked_scores(k_ref, q, length, keys) - lse_ref[0])
        d_probs = dot(v_ref[0, :, :keys].T, d_out)
        d_scores = (probs * (d_probs - delta)).astype(BF16)
        dv_ref[0, :, :keys] = dot(probs.astype(BF16), d_out.T).T
        dk_ref[0, :, :keys] = dot(d_scores, q.T).T
        dq_ref[0] = dot(k_ref[0, :, :keys], d_scores)

    for_key_count(length, q_ref.shape[-1], body)


def head_call(kernel, name, length, ins, outs, cost):
    heads = ins[0].shape[0]

    def spec(array):
        return pl.BlockSpec((1,) + array.shape[1:], lambda head, *_: (head, 0, 0))

    return pl.pallas_call(
        kernel,
        grid_spec=pltpu.PrefetchScalarGridSpec(num_scalar_prefetch=1, grid=(heads,), in_specs=[spec(a) for a in ins], out_specs=[spec(a) for a in outs]),
        out_shape=outs,
        compiler_params=pltpu.CompilerParams(vmem_limit_bytes=40 << 20),
        cost_estimate=pl.CostEstimate(flops=cost, bytes_accessed=1 << 24, transcendentals=1 << 24),
        name=name,
    )(length, *ins)


def solution(mesh):
    tp = mesh.shape['tp']
    act_spec = P('dp', 'tp', None)
    rep_vec = P(None)
    part_vec = P('dp')
    in_specs = (act_spec, act_spec, P('dp', None), rep_vec, rep_vec, P(None, None, 'tp', None), P(None, 'tp', None),
                P('tp', None, None), rep_vec, rep_vec, rep_vec, P(None, 'tp'), P('tp'), P('tp', None), rep_vec)
    out_specs = (act_spec, act_spec, part_vec, part_vec, P('dp', None, 'tp', None), P('dp', 'tp', None),
                 P(('dp', 'tp'), None, None), part_vec, part_vec, part_vec, P('dp', 'tp'), P(('dp', 'tp')),
                 P(('dp', 'tp'), None), part_vec)

    def swap(value, mask):
        return lax.ppermute(value, 'tp', [(i, i ^ mask) for i in range(tp)])

    def to_sequence(local, me):
        chunk, width = local.shape[1:]
        full = jnp.zeros((tp * chunk, width), local.dtype)
        for mask in range(tp):
            other = me ^ mask
            piece = lax.dynamic_index_in_dim(local, other, 0, keepdims=False)
            piece = swap(piece, mask) if mask else piece
            full = lax.dynamic_update_slice(full, piece, (other * chunk, 0))
        return full

    def from_sequence(full, me):
        rows, width = full.shape
        chunk = rows // tp
        local = jnp.zeros((tp, chunk, width), full.dtype)
        for mask in range(tp):
            other = me ^ mask
            piece = lax.dynamic_slice(full, (other * chunk, 0), (chunk, width))
            piece = swap(piece, mask) if mask else piece
            local = lax.dynamic_update_slice(local, piece[None], (other, 0, 0))
        return local

    def gather(shard):
        far = swap(shard, 2)
        near = swap(jnp.stack([shard, far]), 1)
        return jnp.stack([shard, near[0], far, near[1]])

    def scatter_sum(parts):
        near = jnp.stack([parts[0], parts[2]]) + swap(jnp.stack([parts[1], parts[3]]), 1)
        return near[0] + swap(near[1], 2)

    def all_sum(value):
        value = value + swap(value, 1)
        return value + swap(value, 2)

    def device_step(x_in, grad_y, pad_mask, ln1_gain, ln1_bias, w_qkv, b_qkv, w_out, b_out, ln2_gain, ln2_bias, w_up, b_up, w_down, b_down):
        me = lax.axis_index('tp')
        seq_len = pad_mask.shape[1]
        local_heads, head_dim = w_qkv.shape[2:]
        width = x_in.shape[2]
        heads = local_heads * tp
        q_scale = head_dim ** -0.5
        cos_tab, sin_tab = rope_tables(seq_len, head_dim)
        length = jnp.sum((lax.dynamic_index_in_dim(pad_mask, me, 0) > 0).astype(jnp.int32), axis=1)
        x_f = to_sequence(x_in, me).astype(F32)
        qkv_rows = 3 * local_heads * head_dim
        wq_all = gather(w_qkv.transpose(0, 2, 3, 1).reshape(qkv_rows, width)).reshape(tp * qkv_rows, width)
        bq_all = gather(b_qkv.reshape(1, qkv_rows)).reshape(tp, 3, local_heads, head_dim)
        h1_f, x_hat1, inv_std1 = layer_norm(x_f, ln1_gain, ln1_bias)
        h1 = h1_f.astype(BF16)
        qkv_all = lax.dot_general(wq_all, h1, (((1,), (1,)), ((), ())), preferred_element_type=F32)
        qkv_all = qkv_all.reshape(tp, 3, local_heads, head_dim, seq_len) + bq_all[..., None]

        def by_head(value):
            return value.reshape(heads, head_dim, seq_len)

        q_rot = by_head(rotate(qkv_all[:, 0] * q_scale, cos_tab, sin_tab).astype(BF16))
        k_rot = by_head(rotate(qkv_all[:, 1], cos_tab, sin_tab).astype(BF16))
        v_heads = by_head(qkv_all[:, 2].astype(BF16))
        head_bf16 = jax.ShapeDtypeStruct((heads, head_dim, seq_len), BF16)
        head_f32 = jax.ShapeDtypeStruct((heads, head_dim, seq_len), F32)
        head_row = jax.ShapeDtypeStruct((heads, 1, seq_len), F32)
        attn_o, attn_wide, lse = head_call(attn_fwd_kernel, 'attn_fwd', length, (q_rot, k_rot, v_heads), (head_bf16, head_f32, head_row), 30 * 10 ** 9)
        wo_all = gather(w_out.reshape(local_heads * head_dim, width)).reshape(heads * head_dim, width)
        wu_all = gather(w_up)
        bu_all = gather(b_up)
        wd_all = gather(w_down)
        dy_full = to_sequence(grad_y, me)
        attn_sum = lax.dot_general(attn_o.reshape(heads * head_dim, seq_len), wo_all, (((0,), (0,)), ((), ())), preferred_element_type=F32) + b_out
        x1_f = (x_f + attn_sum).astype(BF16).astype(F32)
        h2_f, x_hat2, inv_std2 = layer_norm(x1_f, ln2_gain, ln2_bias)
        h2 = h2_f.astype(BF16)
        pre_act = jnp.einsum('sd,mdf->msf', h2, wu_all, preferred_element_type=F32) + bu_all[:, None, :]
        erf_term = lax.erf(pre_act * INV_SQRT2)
        act_b = (0.5 * pre_act * (1.0 + erf_term)).astype(BF16)
        gelu_slope = 0.5 * (1.0 + erf_term) + pre_act * jnp.exp(-0.5 * pre_act * pre_act) * INV_SQRT_2PI
        mlp_sum = jnp.einsum('msf,mfd->sd', act_b, wd_all, preferred_element_type=F32) + b_down
        y_out = from_sequence((x1_f + mlp_sum).astype(BF16), me)
        dy_f = dy_full.astype(F32)
        d_pre = jnp.einsum('sd,mfd->msf', dy_full, wd_all, preferred_element_type=F32) * gelu_slope
        d_pre_b = d_pre.astype(BF16)
        d_h2 = jnp.einsum('msf,mdf->sd', d_pre_b, wu_all, preferred_element_type=F32)
        d_x1 = dy_f + layer_norm_grad(d_h2, x_hat2, inv_std2, ln2_gain)
        d_x1_b = d_x1.astype(BF16)
        d_attn = lax.dot_general(wo_all, d_x1_b, (((1,), (1,)), ((), ())), preferred_element_type=F32).astype(BF16).reshape(heads, head_dim, seq_len)
        grad_w_down = scatter_sum(jnp.einsum('msf,sd->mfd', act_b, dy_full, preferred_element_type=F32))
        grad_w_up = scatter_sum(jnp.einsum('sd,msf->mdf', h2, d_pre_b, preferred_element_type=F32))
        grad_w_out = scatter_sum(jnp.einsum('ms,sd->md', attn_o.reshape(heads * head_dim, seq_len), d_x1_b, preferred_element_type=F32).reshape(tp, local_heads * head_dim, width))
        grad_b_up = scatter_sum(jnp.sum(d_pre, axis=1))
        mid_sums = all_sum(jnp.stack([jnp.sum(dy_f, axis=0), jnp.sum(d_h2 * x_hat2, axis=0), jnp.sum(d_h2, axis=0), jnp.sum(d_x1, axis=0)]))
        d_query, d_key, d_value = head_call(attn_bwd_kernel, 'attn_bwd', length, (q_rot, k_rot, v_heads, d_attn, attn_wide, lse), (head_f32,) * 3, 60 * 10 ** 9)

        def by_shard(value):
            return value.reshape(tp, local_heads, head_dim, seq_len)

        d_qkv = jnp.stack([by_shard(rotate_back(d_query, cos_tab, sin_tab) * q_scale), by_shard(rotate_back(d_key, cos_tab, sin_tab)), by_shard(d_value)], axis=1)
        grad_b_qkv = scatter_sum(jnp.sum(d_qkv, axis=-1).reshape(tp, qkv_rows)).reshape(3, local_heads, head_dim)
        d_qkv_b = d_qkv.astype(BF16).reshape(tp * qkv_rows, seq_len)
        d_h1 = lax.dot_general(d_qkv_b, wq_all, (((0,), (0,)), ((), ())), preferred_element_type=F32)
        grad_w_qkv = scatter_sum(dot(d_qkv_b, h1).reshape(tp, qkv_rows, width))
        grad_w_qkv = grad_w_qkv.reshape(3, local_heads, head_dim, width).transpose(0, 3, 1, 2)
        ln1_sums = all_sum(jnp.stack([jnp.sum(d_h1 * x_hat1, axis=0), jnp.sum(d_h1, axis=0)]))
        grad_x = from_sequence((d_x1 + layer_norm_grad(d_h1, x_hat1, inv_std1, ln1_gain)).astype(BF16), me)
        grad_w_out = grad_w_out.reshape(local_heads, head_dim, width)
        return (y_out, grad_x, ln1_sums[0], ln1_sums[1], grad_w_qkv, grad_b_qkv, grad_w_out, mid_sums[3],
                mid_sums[1], mid_sums[2], grad_w_up, grad_b_up, grad_w_down, mid_sums[0])

    return jax.shard_map(device_step, mesh=mesh, in_specs=in_specs, out_specs=out_specs, check_vma=False)
```

```python
import functools

import jax
import jax.numpy as jnp
from jax import lax
from jax.experimental import pallas as pl
from jax.experimental.pallas import tpu as pltpu
from jax.sharding import PartitionSpec as P

LN_EPS = 1e-5
ROPE_BASE = 10000.0
INV_SQRT2 = 0.7071067811865476
INV_SQRT_2PI = 0.3989422804014327
NEG_LARGE = -1e30
F32 = jnp.float32
BF16 = jnp.bfloat16
KEY_STEP = 256
MESH = pl.DeviceIdType.MESH


def dot(lhs, rhs):
    return jnp.dot(lhs, rhs, preferred_element_type=F32)


def layer_norm(values, ln_gain, ln_bias):
    centered = values - jnp.mean(values, axis=-1, keepdims=True)
    inv_std = lax.rsqrt(jnp.mean(centered * centered, axis=-1, keepdims=True) + LN_EPS)
    x_hat = centered * inv_std
    return x_hat * ln_gain + ln_bias, x_hat, inv_std


def layer_norm_grad(d_out, x_hat, inv_std, ln_gain):
    d_hat = d_out * ln_gain
    return inv_std * (d_hat - jnp.mean(d_hat, axis=-1, keepdims=True) - x_hat * jnp.mean(d_hat * x_hat, axis=-1, keepdims=True))


def rope_tables(seq_len, head_dim):
    half_dim = head_dim // 2
    inv_freq = ROPE_BASE ** (-2.0 * jnp.arange(half_dim, dtype=F32) / head_dim)
    angles = inv_freq[:, None] * jnp.arange(seq_len, dtype=F32)[None, :]
    angles = jnp.concatenate([angles, angles], axis=0)
    return jnp.cos(angles), jnp.sin(angles)


def rotate(tensor, cos_tab, sin_tab):
    half_dim = tensor.shape[-2] // 2
    swapped = jnp.concatenate([-tensor[..., half_dim:, :], tensor[..., :half_dim, :]], axis=-2)
    return tensor * cos_tab + swapped * sin_tab


def rotate_back(grad_in, cos_tab, sin_tab):
    half_dim = grad_in.shape[-2] // 2
    scaled = grad_in * sin_tab
    swapped = jnp.concatenate([scaled[..., half_dim:, :], -scaled[..., :half_dim, :]], axis=-2)
    return grad_in * cos_tab + swapped


def masked_scores(k_ref, q, length, keys):
    scores = dot(k_ref[0, :, :keys].T, q)
    tail = keys - KEY_STEP
    rows = lax.broadcasted_iota(jnp.int32, (KEY_STEP, scores.shape[1]), 0) + tail
    last = jnp.where(rows < length, scores[tail:], NEG_LARGE)
    return last if tail == 0 else jnp.concatenate([scores[:tail], last], axis=0)


def for_key_count(length, seq_len, body):
    blocks = lax.div(length + KEY_STEP - 1, KEY_STEP)
    for count in range(1, seq_len // KEY_STEP + 1):
        pl.when(blocks == count)(functools.partial(body, count * KEY_STEP))


def attn_bwd_kernel(len_ref, q_ref, k_ref, v_ref, do_ref, o_wide_ref, lse_ref, dq_ref, dk_ref, dv_ref):
    length = len_ref[0]
    dk_ref[...] = jnp.zeros_like(dk_ref)
    dv_ref[...] = jnp.zeros_like(dv_ref)

    def body(keys):
        q, d_out = q_ref[0], do_ref[0]
        delta = jnp.sum(d_out.astype(F32) * o_wide_ref[0], axis=0, keepdims=True)
        probs = jnp.exp(masked_scores(k_ref, q, length, keys) - lse_ref[0])
        d_probs = dot(v_ref[0, :, :keys].T, d_out)
        d_scores = (probs * (d_probs - delta)).astype(BF16)
        dv_ref[0, :, :keys] = dot(probs.astype(BF16), d_out.T).T
        dk_ref[0, :, :keys] = dot(d_scores, q.T).T
        dq_ref[0] = dot(k_ref[0, :, :keys], d_scores)

    for_key_count(length, q_ref.shape[-1], body)


def head_call(kernel, name, length, ins, outs, cost):
    heads = ins[0].shape[0]

    def spec(array):
        return pl.BlockSpec((1,) + array.shape[1:], lambda head, *_: (head, 0, 0))

    return pl.pallas_call(
        kernel,
        grid_spec=pltpu.PrefetchScalarGridSpec(num_scalar_prefetch=1, grid=(heads,), in_specs=[spec(a) for a in ins], out_specs=[spec(a) for a in outs]),
        out_shape=outs,
        compiler_params=pltpu.CompilerParams(vmem_limit_bytes=40 << 20),
        cost_estimate=pl.CostEstimate(flops=cost, bytes_accessed=1 << 24, transcendentals=1 << 24),
        name=name,
    )(length, *ins)


def remote(src, dst, send_sem, recv_sem, device):
    return pltpu.make_async_remote_copy(src_ref=src, dst_ref=dst, send_sem=send_sem, recv_sem=recv_sem, device_id={'tp': device}, device_id_type=MESH)


def greet(me):
    barrier = pltpu.get_barrier_semaphore()
    for mask in (1, 2, 3):
        pl.semaphore_signal(barrier, inc=1, device_id={'tp': me ^ mask}, device_id_type=MESH)
    pl.semaphore_wait(barrier, 3)


class Gather:
    def __init__(self, src, dst, base, send_sem, recv_sem, me):
        self.near = remote(src, dst.at[1 - base], send_sem.at[0], recv_sem.at[0], me ^ 1)
        self.far = remote(src, dst.at[2 - base], send_sem.at[1], recv_sem.at[1], me ^ 2)
        self.relay = remote(dst.at[2 - base], dst.at[3 - base], send_sem.at[2], recv_sem.at[2], me ^ 1)

    def start(self):
        self.far.start()
        self.near.start()

    def forward(self):
        self.far.wait_recv()
        self.relay.start()

    def finish(self):
        self.near.wait()
        self.far.wait_send()
        self.relay.wait()


class ToSequence:
    def __init__(self, src, dst, send_sem, recv_sem, me, chunk):
        self.copies = {mask: remote(src.at[me ^ mask], dst.at[pl.ds(pl.multiple_of(me * chunk, chunk), chunk)], send_sem.at[mask], recv_sem.at[mask], me ^ mask) for mask in (2, 3, 1)}

    def start(self):
        for copy in self.copies.values():
            copy.start()

    def wait_recv(self):
        for copy in self.copies.values():
            copy.wait_recv()

    def wait_send(self):
        for copy in self.copies.values():
            copy.wait_send()


def forward_kernel(dims, x_ref, wq_ref, bq_ref, mask_ref, gain_ref, bias_ref, cos_ref, sin_ref, wo_ref, wu_ref, wd_ref, bu_ref, dy_ref,
                   x_full, wq_all, h1_ref, q_all, k_all, v_all, o_ref, wide_ref, lse_ref, wo_all, wu_all, wd_all, bu_all, dy_full,
                   h1t_ref, bq_all, own_sem, send_sem, recv_sem):
    chunk, local_heads, head_dim = dims
    me = lax.axis_index('tp')
    half = head_dim // 2
    greet(me)
    x_move = ToSequence(x_ref, x_full, send_sem.at[0], recv_sem.at[0], me, chunk)
    dy_move = ToSequence(dy_ref, dy_full, send_sem.at[1], recv_sem.at[1], me, chunk)
    wq = Gather(wq_ref, wq_all, 0, send_sem.at[2], recv_sem.at[2], me)
    bq = Gather(bq_ref, bq_all, 0, send_sem.at[3], recv_sem.at[3], me)
    others = [Gather(src, dst, 1, send_sem.at[4 + i], recv_sem.at[4 + i], me) for i, (src, dst) in enumerate(((wo_ref, wo_all), (bu_ref, bu_all), (wu_ref, wu_all), (wd_ref, wd_all)))]
    x_move.start()
    bq.start()
    wq.start()
    own_wq = pltpu.make_async_copy(wq_ref, wq_all.at[0], own_sem.at[0])
    own_wq.start()
    own_rows = pl.ds(pl.multiple_of(me * chunk, chunk), chunk)
    own_dy = pltpu.make_async_copy(dy_ref.at[me], dy_full.at[own_rows], own_sem.at[1])
    own_dy.start()
    for move in others[:3]:
        move.start()
    dy_move.start()
    others[3].start()
    x_full[own_rows] = x_ref[me]
    bq_all[0] = bq_ref[...]
    x_move.wait_recv()
    x_f = x_full[...].astype(F32)
    h1, _, _ = layer_norm(x_f, gain_ref[...], bias_ref[...])
    h1 = h1.astype(BF16)
    h1_ref[...] = h1
    h1t_ref[...] = h1.T
    own_wq.wait()

    @pl.loop(0, 4)
    def _(m):
        @pl.when(m == 1)
        def _():
            bq.near.wait_recv()
            wq.near.wait_recv()

        @pl.when(m == 2)
        def _():
            bq.forward()
            wq.forward()

        @pl.when(m == 3)
        def _():
            bq.relay.wait_recv()
            wq.relay.wait_recv()

        bias = bq_all[m].T[:, :1]
        qkv = dot(wq_all[m], h1t_ref[...]) + bias
        cos, sin = cos_ref[...], sin_ref[...]
        group = local_heads * head_dim
        ones = (lax.broadcasted_iota(jnp.int32, (half, cos.shape[1]), 0) == 0).astype(BF16)
        for j in range(local_heads):
            head = m * local_heads + j
            for which, (dst, scale, extra) in enumerate(((q_all, head_dim ** -0.5, ones), (k_all, None, mask_ref[...]))):
                rows = qkv[which * group + j * head_dim:which * group + (j + 1) * head_dim]
                rows = rows * scale if scale is not None else rows
                low, high = rows[:half], rows[half:]
                dst[head, :half] = (low * cos - high * sin).astype(BF16)
                dst[head, half:head_dim] = (high * cos + low * sin).astype(BF16)
                dst[head, head_dim:] = extra
            v_all[head] = qkv[2 * group + j * head_dim:2 * group + (j + 1) * head_dim].astype(BF16)

        @pl.loop(0, local_heads)
        def _(j):
            head = m * local_heads + j
            scores = dot(k_all[head].T, q_all[head])
            top = jnp.max(scores, axis=0, keepdims=True)
            weights = jnp.exp(scores - top)
            total = jnp.sum(weights, axis=0, keepdims=True)
            out = dot(v_all[head], weights.astype(BF16)) / total
            o_ref[head] = out.astype(BF16)
            wide_ref[head] = out
            lse_ref[head] = top + jnp.log(total)

    x_move.wait_send()
    for move in (bq, wq):
        move.near.wait_send()
        move.far.wait_send()
        move.relay.wait_send()
    for move in others:
        move.forward()
    for move in others:
        move.finish()
    own_dy.wait()
    dy_move.wait_recv()
    dy_move.wait_send()


def forward_call(x_in, wq, bq, key_bias, gain, bias, cos, sin, wo, wu, wd, bu, dy, local_heads, head_dim):
    tp, chunk, width = x_in.shape
    seq_len = tp * chunk
    heads = tp * local_heads
    ext = head_dim + head_dim // 2
    vmem, anywhere = pl.BlockSpec(memory_space=pltpu.VMEM), pl.BlockSpec(memory_space=pl.ANY)

    def shape(dims, dtype=BF16):
        return jax.ShapeDtypeStruct(dims, dtype)

    outs = [shape((seq_len, width)), shape((tp,) + wq.shape), shape((seq_len, width)), shape((heads, ext, seq_len)), shape((heads, ext, seq_len)),
            shape((heads, head_dim, seq_len)), shape((heads, head_dim, seq_len)), shape((heads, head_dim, seq_len), F32), shape((heads, 1, seq_len), F32),
            shape((tp - 1,) + wo.shape), shape((tp - 1,) + wu.shape), shape((tp - 1,) + wd.shape), shape((tp - 1,) + bu.shape, F32), shape((seq_len, width))]
    return pl.pallas_call(
        functools.partial(forward_kernel, (chunk, local_heads, head_dim)),
        out_shape=outs,
        in_specs=[vmem, anywhere] + [vmem] * 6 + [anywhere] * 5,
        out_specs=[vmem] * 9 + [anywhere] * 5,
        scratch_shapes=[pltpu.VMEM((width, seq_len), BF16), pltpu.VMEM((tp,) + bq.shape, F32), pltpu.SemaphoreType.DMA((2,)), pltpu.SemaphoreType.DMA((8, 4)), pltpu.SemaphoreType.DMA((8, 4))],
        compiler_params=pltpu.CompilerParams(collective_id=0, has_side_effects=True, vmem_limit_bytes=60 << 20),
        name='forward',
    )(x_in, wq, bq, key_bias, gain, bias, cos, sin, wo, wu, wd, bu, dy)


def solution(mesh):
    tp = mesh.shape['tp']
    act_spec = P('dp', 'tp', None)
    rep_vec = P(None)
    part_vec = P('dp')
    in_specs = (act_spec, act_spec, P('dp', None), rep_vec, rep_vec, P(None, None, 'tp', None), P(None, 'tp', None),
                P('tp', None, None), rep_vec, rep_vec, rep_vec, P(None, 'tp'), P('tp'), P('tp', None), rep_vec)
    out_specs = (act_spec, act_spec, part_vec, part_vec, P('dp', None, 'tp', None), P('dp', 'tp', None),
                 P(('dp', 'tp'), None, None), part_vec, part_vec, part_vec, P('dp', 'tp'), P(('dp', 'tp')),
                 P(('dp', 'tp'), None), part_vec)

    def swap(value, mask):
        return lax.ppermute(value, 'tp', [(i, i ^ mask) for i in range(tp)])

    def to_sequence(local, me):
        chunk, width = local.shape[1:]
        full = jnp.zeros((tp * chunk, width), local.dtype)
        for mask in range(tp):
            other = me ^ mask
            piece = lax.dynamic_index_in_dim(local, other, 0, keepdims=False)
            piece = swap(piece, mask) if mask else piece
            full = lax.dynamic_update_slice(full, piece, (other * chunk, 0))
        return full

    def from_sequence(full, me):
        rows, width = full.shape
        chunk = rows // tp
        local = jnp.zeros((tp, chunk, width), full.dtype)
        for mask in range(tp):
            other = me ^ mask
            piece = lax.dynamic_slice(full, (other * chunk, 0), (chunk, width))
            piece = swap(piece, mask) if mask else piece
            local = lax.dynamic_update_slice(local, piece[None], (other, 0, 0))
        return local

    def gather(shard):
        far = swap(shard, 2)
        near = swap(jnp.stack([shard, far]), 1)
        return jnp.stack([shard, near[0], far, near[1]])

    def scatter_sum(parts):
        near = jnp.stack([parts[0], parts[2]]) + swap(jnp.stack([parts[1], parts[3]]), 1)
        return near[0] + swap(near[1], 2)

    def all_sum(value):
        value = value + swap(value, 1)
        return value + swap(value, 2)

    def device_step(x_in, grad_y, pad_mask, ln1_gain, ln1_bias, w_qkv, b_qkv, w_out, b_out, ln2_gain, ln2_bias, w_up, b_up, w_down, b_down):
        me = lax.axis_index('tp')
        seq_len = pad_mask.shape[1]
        local_heads, head_dim = w_qkv.shape[2:]
        width = x_in.shape[2]
        heads = local_heads * tp
        q_scale = head_dim ** -0.5
        cos_tab, sin_tab = rope_tables(seq_len, head_dim)
        length = jnp.sum((lax.dynamic_index_in_dim(pad_mask, me, 0) > 0).astype(jnp.int32), axis=1)
        qkv_rows = 3 * local_heads * head_dim
        half_dim = head_dim // 2
        key_bias = jnp.where(jnp.arange(seq_len) < length[0], 0.0, NEG_LARGE).astype(BF16)
        key_bias = jnp.zeros((half_dim, seq_len), BF16).at[0].set(key_bias)
        wq_own = w_qkv.transpose(0, 2, 3, 1).reshape(qkv_rows, width)
        bq_own = jnp.broadcast_to(b_qkv.reshape(1, qkv_rows), (8, qkv_rows))
        wo_own = w_out.reshape(local_heads * head_dim, width)
        bu_own = jnp.broadcast_to(b_up[None], (8,) + b_up.shape)
        (x_full, wq_all, h1, q_ext, k_ext, v_heads, attn_o, attn_wide, lse, wo_all, wu_all, wd_all, bu_all, dy_full) = forward_call(
            x_in, wq_own, bq_own, key_bias, ln1_gain[None], ln1_bias[None], cos_tab[:half_dim], sin_tab[:half_dim], wo_own, w_up, w_down, bu_own, grad_y, local_heads, head_dim)
        wq_all = wq_all.reshape(tp * qkv_rows, width)
        wo_all = jnp.concatenate([wo_own[None], wo_all]).reshape(heads * head_dim, width)
        wu_all = jnp.concatenate([w_up[None], wu_all])
        wd_all = jnp.concatenate([w_down[None], wd_all])
        bu_all = jnp.concatenate([bu_own[None], bu_all])[:, 0]
        x_f = x_full.astype(F32)
        _, x_hat1, inv_std1 = layer_norm(x_f, ln1_gain, ln1_bias)
        q_rot, k_rot = q_ext[:, :head_dim], k_ext[:, :head_dim]
        head_f32 = jax.ShapeDtypeStruct((heads, head_dim, seq_len), F32)
        attn_sum = lax.dot_general(attn_o.reshape(heads * head_dim, seq_len), wo_all, (((0,), (0,)), ((), ())), preferred_element_type=F32) + b_out
        x1_f = (x_f + attn_sum).astype(BF16).astype(F32)
        h2_f, x_hat2, inv_std2 = layer_norm(x1_f, ln2_gain, ln2_bias)
        h2 = h2_f.astype(BF16)
        pre_act = jnp.einsum('sd,mdf->msf', h2, wu_all, preferred_element_type=F32) + bu_all[:, None, :]
        erf_term = lax.erf(pre_act * INV_SQRT2)
        act_b = (0.5 * pre_act * (1.0 + erf_term)).astype(BF16)
        gelu_slope = 0.5 * (1.0 + erf_term) + pre_act * jnp.exp(-0.5 * pre_act * pre_act) * INV_SQRT_2PI
        mlp_sum = jnp.einsum('msf,mfd->sd', act_b, wd_all, preferred_element_type=F32) + b_down
        y_out = from_sequence((x1_f + mlp_sum).astype(BF16), me)
        dy_f = dy_full.astype(F32)
        d_pre = jnp.einsum('sd,mfd->msf', dy_full, wd_all, preferred_element_type=F32) * gelu_slope
        d_pre_b = d_pre.astype(BF16)
        d_h2 = jnp.einsum('msf,mdf->sd', d_pre_b, wu_all, preferred_element_type=F32)
        d_x1 = dy_f + layer_norm_grad(d_h2, x_hat2, inv_std2, ln2_gain)
        d_x1_b = d_x1.astype(BF16)
        d_attn = lax.dot_general(wo_all, d_x1_b, (((1,), (1,)), ((), ())), preferred_element_type=F32).astype(BF16).reshape(heads, head_dim, seq_len)
        grad_w_down = scatter_sum(jnp.einsum('msf,sd->mfd', act_b, dy_full, preferred_element_type=F32))
        grad_w_up = scatter_sum(jnp.einsum('sd,msf->mdf', h2, d_pre_b, preferred_element_type=F32))
        grad_w_out = scatter_sum(jnp.einsum('ms,sd->md', attn_o.reshape(heads * head_dim, seq_len), d_x1_b, preferred_element_type=F32).reshape(tp, local_heads * head_dim, width))
        grad_b_up = scatter_sum(jnp.sum(d_pre, axis=1))
        mid_sums = all_sum(jnp.stack([jnp.sum(dy_f, axis=0), jnp.sum(d_h2 * x_hat2, axis=0), jnp.sum(d_h2, axis=0), jnp.sum(d_x1, axis=0)]))
        d_query, d_key, d_value = head_call(attn_bwd_kernel, 'attn_bwd', length, (q_rot, k_rot, v_heads, d_attn, attn_wide, lse), (head_f32,) * 3, 60 * 10 ** 9)

        def by_shard(value):
            return value.reshape(tp, local_heads, head_dim, seq_len)

        d_qkv = jnp.stack([by_shard(rotate_back(d_query, cos_tab, sin_tab) * q_scale), by_shard(rotate_back(d_key, cos_tab, sin_tab)), by_shard(d_value)], axis=1)
        grad_b_qkv = scatter_sum(jnp.sum(d_qkv, axis=-1).reshape(tp, qkv_rows)).reshape(3, local_heads, head_dim)
        d_qkv_b = d_qkv.astype(BF16).reshape(tp * qkv_rows, seq_len)
        d_h1 = lax.dot_general(d_qkv_b, wq_all, (((0,), (0,)), ((), ())), preferred_element_type=F32)
        grad_w_qkv = scatter_sum(dot(d_qkv_b, h1).reshape(tp, qkv_rows, width))
        grad_w_qkv = grad_w_qkv.reshape(3, local_heads, head_dim, width).transpose(0, 3, 1, 2)
        ln1_sums = all_sum(jnp.stack([jnp.sum(d_h1 * x_hat1, axis=0), jnp.sum(d_h1, axis=0)]))
        grad_x = from_sequence((d_x1 + layer_norm_grad(d_h1, x_hat1, inv_std1, ln1_gain)).astype(BF16), me)
        grad_w_out = grad_w_out.reshape(local_heads, head_dim, width)
        return (y_out, grad_x, ln1_sums[0], ln1_sums[1], grad_w_qkv, grad_b_qkv, grad_w_out, mid_sums[3],
                mid_sums[1], mid_sums[2], grad_w_up, grad_b_up, grad_w_down, mid_sums[0])

    return jax.shard_map(device_step, mesh=mesh, in_specs=in_specs, out_specs=out_specs, check_vma=False)
```

```python
import functools

import jax
import jax.numpy as jnp
from jax import lax
from jax.experimental import pallas as pl
from jax.experimental.pallas import tpu as pltpu
from jax.sharding import PartitionSpec as P

LN_EPS = 1e-5
ROPE_BASE = 10000.0
INV_SQRT2 = 0.7071067811865476
INV_SQRT_2PI = 0.3989422804014327
NEG_LARGE = -1e30
F32 = jnp.float32
BF16 = jnp.bfloat16
MESH = pl.DeviceIdType.MESH


def dot(lhs, rhs):
    return jnp.dot(lhs, rhs, preferred_element_type=F32)


def layer_norm(values, ln_gain, ln_bias):
    centered = values - jnp.mean(values, axis=-1, keepdims=True)
    inv_std = lax.rsqrt(jnp.mean(centered * centered, axis=-1, keepdims=True) + LN_EPS)
    x_hat = centered * inv_std
    return x_hat * ln_gain + ln_bias, x_hat, inv_std


def rope_tables(seq_len, head_dim):
    half_dim = head_dim // 2
    inv_freq = ROPE_BASE ** (-2.0 * jnp.arange(half_dim, dtype=F32) / head_dim)
    angles = inv_freq[:, None] * jnp.arange(seq_len, dtype=F32)[None, :]
    angles = jnp.concatenate([angles, angles], axis=0)
    return jnp.cos(angles), jnp.sin(angles)


def remote(src, dst, send_sem, recv_sem, device):
    return pltpu.make_async_remote_copy(src_ref=src, dst_ref=dst, send_sem=send_sem, recv_sem=recv_sem, device_id={'tp': device}, device_id_type=MESH)


def greet(me):
    barrier = pltpu.get_barrier_semaphore()
    for mask in (1, 2, 3):
        pl.semaphore_signal(barrier, inc=1, device_id={'tp': me ^ mask}, device_id_type=MESH)
    pl.semaphore_wait(barrier, 3)


class Gather:
    def __init__(self, src, dst, base, send_sem, recv_sem, me):
        self.near = remote(src, dst.at[1 - base], send_sem.at[0], recv_sem.at[0], me ^ 1)
        self.far = remote(src, dst.at[2 - base], send_sem.at[1], recv_sem.at[1], me ^ 2)
        self.relay = remote(dst.at[2 - base], dst.at[3 - base], send_sem.at[2], recv_sem.at[2], me ^ 1)

    def start(self):
        self.far.start()
        self.near.start()

    def forward(self):
        self.far.wait_recv()
        self.relay.start()

    def finish(self):
        self.near.wait()
        self.far.wait_send()
        self.relay.wait()


class ToSequence:
    def __init__(self, src, dst, send_sem, recv_sem, me, chunk):
        self.copies = {mask: remote(src.at[me ^ mask], dst.at[pl.ds(pl.multiple_of(me * chunk, chunk), chunk)], send_sem.at[mask], recv_sem.at[mask], me ^ mask) for mask in (2, 3, 1)}

    def start(self):
        for copy in self.copies.values():
            copy.start()

    def wait_recv(self):
        for copy in self.copies.values():
            copy.wait_recv()

    def wait_send(self):
        for copy in self.copies.values():
            copy.wait_send()


def forward_kernel(dims, x_ref, wq_ref, bq_ref, mask_ref, gain_ref, bias_ref, cos_ref, sin_ref, wo_ref, wu_ref, wd_ref, bu_ref, dy_ref,
                   x_full, wq_all, h1_ref, q_all, k_all, v_all, o_ref, wide_ref, lse_ref, wo_all, wu_all, wd_all, bu_all, dy_full,
                   h1t_ref, bq_all, own_sem, send_sem, recv_sem):
    chunk, local_heads, head_dim = dims
    me = lax.axis_index('tp')
    half = head_dim // 2
    greet(me)
    x_move = ToSequence(x_ref, x_full, send_sem.at[0], recv_sem.at[0], me, chunk)
    dy_move = ToSequence(dy_ref, dy_full, send_sem.at[1], recv_sem.at[1], me, chunk)
    wq = Gather(wq_ref, wq_all, 0, send_sem.at[2], recv_sem.at[2], me)
    bq = Gather(bq_ref, bq_all, 0, send_sem.at[3], recv_sem.at[3], me)
    others = [Gather(src, dst, 1, send_sem.at[4 + i], recv_sem.at[4 + i], me) for i, (src, dst) in enumerate(((wo_ref, wo_all), (bu_ref, bu_all), (wu_ref, wu_all), (wd_ref, wd_all)))]
    x_move.start()
    bq.start()
    wq.start()
    own_wq = pltpu.make_async_copy(wq_ref, wq_all.at[0], own_sem.at[0])
    own_wq.start()
    own_rows = pl.ds(pl.multiple_of(me * chunk, chunk), chunk)
    own_dy = pltpu.make_async_copy(dy_ref.at[me], dy_full.at[own_rows], own_sem.at[1])
    own_dy.start()
    for move in others[:3]:
        move.start()
    dy_move.start()
    others[3].start()
    x_full[own_rows] = x_ref[me]
    bq_all[0] = bq_ref[...]
    x_move.wait_recv()
    x_f = x_full[...].astype(F32)
    h1, _, _ = layer_norm(x_f, gain_ref[...], bias_ref[...])
    h1 = h1.astype(BF16)
    h1_ref[...] = h1
    h1t_ref[...] = h1.T
    own_wq.wait()

    @pl.loop(0, 4)
    def _(m):
        @pl.when(m == 1)
        def _():
            bq.near.wait_recv()
            wq.near.wait_recv()

        @pl.when(m == 2)
        def _():
            bq.forward()
            wq.forward()

        @pl.when(m == 3)
        def _():
            bq.relay.wait_recv()
            wq.relay.wait_recv()

        bias = bq_all[m].T[:, :1]
        qkv = dot(wq_all[m], h1t_ref[...]) + bias
        cos, sin = cos_ref[...], sin_ref[...]
        group = local_heads * head_dim
        ones = (lax.broadcasted_iota(jnp.int32, (half, cos.shape[1]), 0) == 0).astype(BF16)
        for j in range(local_heads):
            head = m * local_heads + j
            for which, (dst, scale, extra) in enumerate(((q_all, head_dim ** -0.5, ones), (k_all, None, mask_ref[...]))):
                rows = qkv[which * group + j * head_dim:which * group + (j + 1) * head_dim]
                rows = rows * scale if scale is not None else rows
                low, high = rows[:half], rows[half:]
                dst[head, :half] = (low * cos - high * sin).astype(BF16)
                dst[head, half:head_dim] = (high * cos + low * sin).astype(BF16)
                dst[head, head_dim:] = extra
            v_all[head] = qkv[2 * group + j * head_dim:2 * group + (j + 1) * head_dim].astype(BF16)

        @pl.loop(0, local_heads)
        def _(j):
            head = m * local_heads + j
            scores = dot(k_all[head].T, q_all[head])
            top = jnp.max(scores, axis=0, keepdims=True)
            weights = jnp.exp(scores - top)
            total = jnp.sum(weights, axis=0, keepdims=True)
            out = dot(v_all[head], weights.astype(BF16)) / total
            o_ref[head] = out.astype(BF16)
            wide_ref[head] = out
            lse_ref[head] = top + jnp.log(total)

    x_move.wait_send()
    for move in (bq, wq):
        move.near.wait_send()
        move.far.wait_send()
        move.relay.wait_send()
    for move in others:
        move.forward()
    for move in others:
        move.finish()
    own_dy.wait()
    dy_move.wait_recv()
    dy_move.wait_send()


def forward_call(x_in, wq, bq, key_bias, gain, bias, cos, sin, wo, wu, wd, bu, dy, local_heads, head_dim):
    tp, chunk, width = x_in.shape
    seq_len = tp * chunk
    heads = tp * local_heads
    ext = head_dim + head_dim // 2
    vmem, anywhere = pl.BlockSpec(memory_space=pltpu.VMEM), pl.BlockSpec(memory_space=pl.ANY)

    def shape(dims, dtype=BF16):
        return jax.ShapeDtypeStruct(dims, dtype)

    outs = [shape((seq_len, width)), shape((tp,) + wq.shape), shape((seq_len, width)), shape((heads, ext, seq_len)), shape((heads, ext, seq_len)),
            shape((heads, head_dim, seq_len)), shape((heads, head_dim, seq_len)), shape((heads, head_dim, seq_len), F32), shape((heads, 1, seq_len), F32),
            shape((tp - 1,) + wo.shape), shape((tp - 1,) + wu.shape), shape((tp - 1,) + wd.shape), shape((tp - 1,) + bu.shape, F32), shape((seq_len, width))]
    return pl.pallas_call(
        functools.partial(forward_kernel, (chunk, local_heads, head_dim)),
        out_shape=outs,
        in_specs=[vmem, anywhere] + [vmem] * 6 + [anywhere] * 5,
        out_specs=[vmem] * 9 + [anywhere] * 5,
        scratch_shapes=[pltpu.VMEM((width, seq_len), BF16), pltpu.VMEM((tp,) + bq.shape, F32), pltpu.SemaphoreType.DMA((2,)), pltpu.SemaphoreType.DMA((8, 4)), pltpu.SemaphoreType.DMA((8, 4))],
        compiler_params=pltpu.CompilerParams(collective_id=0, has_side_effects=True, vmem_limit_bytes=60 << 20),
        name='forward',
    )(x_in, wq, bq, key_bias, gain, bias, cos, sin, wo, wu, wd, bu, dy)


def layer_norm_rows(values, ln_gain, ln_bias):
    centered = values - jnp.mean(values, axis=0, keepdims=True)
    inv_std = lax.rsqrt(jnp.mean(centered * centered, axis=0, keepdims=True) + LN_EPS)
    x_hat = centered * inv_std
    return x_hat * ln_gain + ln_bias, x_hat, inv_std


def layer_norm_rows_grad(d_out, x_hat, inv_std, ln_gain):
    d_hat = d_out * ln_gain
    return inv_std * (d_hat - jnp.mean(d_hat, axis=0, keepdims=True) - x_hat * jnp.mean(d_hat * x_hat, axis=0, keepdims=True))


def dot_tn(lhs, rhs):
    return lax.dot_general(lhs, rhs, (((0,), (0,)), ((), ())), preferred_element_type=F32)


def dot_nt(lhs, rhs):
    return lax.dot_general(lhs, rhs, (((1,), (1,)), ((), ())), preferred_element_type=F32)


def gelu(pre_act):
    half_erf = 0.5 * (1.0 + lax.erf(pre_act * INV_SQRT2))
    act = (pre_act * half_erf).astype(BF16)
    return act, half_erf + pre_act * jnp.exp(-0.5 * pre_act * pre_act) * INV_SQRT_2PI


class FromSequence:
    def __init__(self, src, dst, send_sem, recv_sem, me, chunk):
        self.copies = {mask: remote(src.at[pl.ds(pl.multiple_of((me ^ mask) * chunk, chunk), chunk)], dst.at[me], send_sem.at[mask], recv_sem.at[mask], me ^ mask) for mask in (2, 3, 1)}

    def start(self):
        for copy in self.copies.values():
            copy.start()

    def wait(self):
        for copy in self.copies.values():
            copy.wait()


def middle_kernel(x_ref, o_ref, wo_ref, wo_far_ref, vec_ref, bu_ref, dy_ref, wu_own, wu_far, wd_own, wd_far,
                  y_ref, h2_ref, dx1t_ref, dx1b_ref, do_ref, sums_ref,
                  wu_all, wd_all, slope_ref, act_ref, y_seq, load_sem, send_sem, recv_sem):
    me = lax.axis_index('tp')
    tp, chunk, width = y_ref.shape
    ff = wu_own.shape[1]
    greet(me)
    loads = []
    for m in range(tp):
        wu_src = wu_own if m == 0 else wu_far.at[m - 1]
        wd_src = wd_own if m == 0 else wd_far.at[m - 1]
        loads.append((pltpu.make_async_copy(wu_src, wu_all.at[m], load_sem.at[0, m]), pltpu.make_async_copy(wd_src, wd_all.at[m], load_sem.at[1, m])))
    for load, _ in loads:
        load.start()
    for _, load in loads:
        load.start()
    cols = vec_ref[...].T
    b_out, gain, bias, b_down = (cols[:, i:i + 1] for i in range(4))
    rows = wo_ref.shape[0]
    attn = dot_tn(wo_ref[...], o_ref[:rows]) + dot_tn(wo_far_ref[...], o_ref[rows:])
    x1 = (x_ref[...].T.astype(F32) + (attn + b_out)).astype(BF16).astype(F32)
    h2_f, x_hat, inv_std = layer_norm_rows(x1, gain, bias)
    h2 = h2_f.astype(BF16)
    h2_ref[...] = h2.T
    for load, _ in loads:
        load.wait()

    @pl.loop(0, tp)
    def _(m):
        pre_act = dot_tn(wu_all[m], h2) + bu_ref[m].T[:, :1]
        act, slope = gelu(pre_act)
        act_ref[m] = act
        slope_ref[m] = slope

    for _, load in loads:
        load.wait()
    mlp = dot_tn(wd_all[...].reshape(tp * ff, width), act_ref[...].reshape(tp * ff, tp * chunk))
    y_seq[...] = (x1 + (mlp + b_down)).astype(BF16).T
    dy = dy_ref[...]
    dy_t = dy.T
    dy_f = dy_t.astype(F32)

    @pl.loop(0, tp)
    def _(m):
        act_ref[m] = (dot(wd_all[m], dy_t) * slope_ref[m]).astype(BF16)

    y_move = FromSequence(y_seq, y_ref, send_sem, recv_sem, me, chunk)
    y_move.start()
    y_ref[me] = y_seq[pl.ds(pl.multiple_of(me * chunk, chunk), chunk)]
    d_h2 = dot(wu_all[0], act_ref[0])
    for m in range(1, tp):
        d_h2 = d_h2 + dot(wu_all[m], act_ref[m])
    d_x1 = dy_f + layer_norm_rows_grad(d_h2, x_hat, inv_std, gain)
    dx1t_ref[...] = d_x1
    d_x1_b = d_x1.astype(BF16)
    dx1b_ref[...] = d_x1_b.T
    do_ref[:rows] = dot(wo_ref[...], d_x1_b).astype(BF16)
    do_ref[rows:] = dot(wo_far_ref[...], d_x1_b).astype(BF16)

    def lane_sum(value):
        return jnp.sum(value, axis=1, keepdims=True)

    sums = [lane_sum(dy_f), lane_sum(d_h2 * x_hat), lane_sum(d_h2), lane_sum(d_x1)]
    sums_ref[...] = jnp.concatenate(sums + [jnp.zeros((width, 124), F32)], axis=1).T[:8]
    y_move.wait()


def backward_kernel(dims, q_all, k_all, v_all, do_ref, wide_ref, lse_ref, cos_ref, sin_ref, o_ref, dx1b_ref, h2_ref, dy_ref,
                    dqkv_ref, gb_ref, gwo_ref, h2_all, dy_all,
                    part, near_buf, far_buf, red_send, red_recv, send_sem, recv_sem):
    local_heads, head_dim = dims
    me = lax.axis_index('tp')
    tp = part.shape[0]
    half = head_dim // 2
    greet(me)
    h2_move = Gather(h2_ref, h2_all, 1, send_sem.at[0], recv_sem.at[0], me)
    dy_move = Gather(dy_ref, dy_all, 1, send_sem.at[1], recv_sem.at[1], me)
    h2_move.start()
    dy_move.start()
    reduce_near = [remote(part.at[src], near_buf.at[i], red_send.at[i], red_recv.at[i], me ^ 1) for i, src in enumerate((1, 3))]
    reduce_far = remote(part.at[2], far_buf, red_send.at[2], red_recv.at[2], me ^ 2)
    part[...] = dot(o_ref[...], dx1b_ref[...]).reshape(part.shape)
    cos, sin = cos_ref[...], sin_ref[...]

    def store(m, j, which, low, high):
        grad = jnp.concatenate([low, high], axis=0)
        dqkv_ref[m, which, pl.ds(pl.multiple_of(j * head_dim, head_dim), head_dim)] = grad.astype(BF16)
        gb_ref[m, which, pl.ds(pl.multiple_of(j * head_dim, head_dim), head_dim)] = jnp.broadcast_to(jnp.sum(grad, axis=1, keepdims=True), (head_dim, 128))

    def back(grad):
        low, high = grad[:half], grad[half:]
        return low * cos + high * sin, high * cos - low * sin

    @pl.loop(0, tp * local_heads)
    def _(head):
        m = lax.div(head, local_heads)
        j = lax.rem(head, local_heads)

        @pl.when(head == 1)
        def _():
            for copy in reduce_near:
                copy.start()

        @pl.when(head == 4)
        def _():
            for copy in reduce_near:
                copy.wait()
            part[0] += near_buf[0]
            part[2] += near_buf[1]

        @pl.when(head == 5)
        def _():
            reduce_far.start()

        @pl.when(head == 12)
        def _():
            h2_move.forward()

        q, k, v, d_out = q_all[head], k_all[head], v_all[head], do_ref[head]
        delta = jnp.sum(d_out.astype(F32) * wide_ref[head], axis=0, keepdims=True)
        probs = jnp.exp(dot(k.T, q) - lse_ref[head])
        d_probs = dot(v.T, d_out)
        d_scores = (probs * (d_probs - delta)).astype(BF16)
        d_value = dot(probs.astype(BF16), d_out.T).T
        d_key = dot(d_scores, q[:head_dim].T).T
        d_query = dot(k[:head_dim], d_scores)
        low, high = back(d_query)
        scale = head_dim ** -0.5
        store(m, j, 0, low * scale, high * scale)
        low, high = back(d_key)
        store(m, j, 1, low, high)
        store(m, j, 2, d_value[:half], d_value[half:])

    h2_move.finish()
    dy_move.forward()
    dy_move.finish()
    reduce_far.wait()
    gwo_ref[...] = part[0] + far_buf[...]


def tail_kernel(dqkv_ref, gb_ref, h1_ref, wq_ref, x_ref, dx1t_ref, sums_ref, vec_ref, bu_ref, wu_ref, wd_ref, h2_own, h2_far, dy_own, dy_far,
                gx_ref, gwq_ref, gb_out, sums_out, gwu_ref, gbu_ref, gwd_ref,
                part, near_buf, far_buf, gb_buf, sums_mine, sums_buf, gx_seq, h2_all, dy_all, acc_up, acc_bias,
                load_sem, red_send, red_recv, small_send, small_recv, send_sem, recv_sem):
    me = lax.axis_index('tp')
    tp, chunk, width = gx_ref.shape
    group = dqkv_ref.shape[1]
    seq_len = tp * chunk
    greet(me)
    loads = []
    for m in range(tp):
        loads.append(pltpu.make_async_copy(h2_own if m == 0 else h2_far.at[m - 1], h2_all.at[m], load_sem.at[0, m]))
        loads.append(pltpu.make_async_copy(dy_own if m == 0 else dy_far.at[m - 1], dy_all.at[m], load_sem.at[1, m]))
    for load in loads:
        load.start()
    gb_moves = [remote(gb_ref.at[m], gb_buf.at[m - 1], small_send.at[0, m], small_recv.at[0, m], me ^ m) for m in (1, 2, 3)]
    for move in gb_moves:
        move.start()
    reduce_near = [remote(part.at[src], near_buf.at[i], red_send.at[i], red_recv.at[i], me ^ 1) for i, src in enumerate((1, 3))]
    reduce_far = remote(part.at[2], far_buf, red_send.at[2], red_recv.at[2], me ^ 2)
    part[...] = dot(dqkv_ref[...].reshape(tp * group, seq_len), h1_ref[...]).reshape(part.shape)
    cols = vec_ref[...].T
    gain, bias = cols[:, 0:1], cols[:, 1:2]
    for copy in reduce_near:
        copy.start()
    d_h1 = dot_tn(wq_ref[...].reshape(tp * group, width), dqkv_ref[...].reshape(tp * group, seq_len))
    _, x_hat, inv_std = layer_norm_rows(x_ref[...].T.astype(F32), gain, bias)
    grad_x = (dx1t_ref[...] + layer_norm_rows_grad(d_h1, x_hat, inv_std, gain)).astype(BF16)
    gx_seq[...] = grad_x.T
    for copy in reduce_near:
        copy.wait()
    part[0] += near_buf[0]
    part[2] += near_buf[1]
    sums = [jnp.sum(d_h1 * x_hat, axis=1, keepdims=True), jnp.sum(d_h1, axis=1, keepdims=True)]
    ln1 = jnp.concatenate(sums + [jnp.zeros((width, 126), F32)], axis=1).T
    sums_mine[...] = jnp.concatenate([sums_ref[:4], ln1[:4]], axis=0)
    gx_ref[me] = gx_seq[pl.ds(pl.multiple_of(me * chunk, chunk), chunk)]
    reduce_far.start()
    gx_move = FromSequence(gx_seq, gx_ref, send_sem, recv_sem, me, chunk)
    gx_move.start()
    sums_moves = [remote(sums_mine, sums_buf.at[m - 1], small_send.at[1, m], small_recv.at[1, m], me ^ m) for m in (1, 2, 3)]
    for move in sums_moves:
        move.start()
    for load in loads:
        load.wait()
    acc_up[...] = jnp.zeros_like(acc_up)
    acc_bias[...] = jnp.zeros_like(acc_bias)
    gwd_ref[...] = jnp.zeros_like(gwd_ref)
    wu_t = wu_ref[...].T
    bu_col = bu_ref[...].T[:, :1]

    @pl.loop(0, tp)
    def _(m):
        act, slope = gelu(dot_nt(wu_t, h2_all[m]) + bu_col)
        d_pre = dot_nt(wd_ref[...], dy_all[m]) * slope
        lanes = d_pre[:, :128]
        for i in range(1, seq_len // 128):
            lanes = lanes + d_pre[:, i * 128:(i + 1) * 128]
        acc_bias[...] += lanes
        gwd_ref[...] += dot(act, dy_all[m])
        acc_up[...] += dot(d_pre.astype(BF16), h2_all[m])

    gwu_ref[...] = acc_up[...].T
    gbu_ref[...] = jnp.broadcast_to(jnp.sum(acc_bias[...], axis=1, keepdims=True), acc_bias.shape).T[:8]
    for move in gb_moves + sums_moves:
        move.wait()
    gb_out[...] = gb_ref[0] + gb_buf[0] + (gb_buf[1] + gb_buf[2])
    sums_out[...] = sums_mine[...] + sums_buf[0] + (sums_buf[1] + sums_buf[2])
    reduce_far.wait()
    gwq_ref[...] = part[0] + far_buf[...]
    gx_move.wait()


VMEM_SPEC = pl.BlockSpec(memory_space=pltpu.VMEM)
ANY_SPEC = pl.BlockSpec(memory_space=pl.ANY)


def shape(dims, dtype=BF16):
    return jax.ShapeDtypeStruct(dims, dtype)


def single_call(kernel, name, collective_id, ins, in_any, outs, out_any, scratch):
    dma = pltpu.SemaphoreType.DMA
    return pl.pallas_call(
        kernel,
        out_shape=outs,
        in_specs=[ANY_SPEC if i in in_any else VMEM_SPEC for i in range(len(ins))],
        out_specs=[ANY_SPEC if i in out_any else VMEM_SPEC for i in range(len(outs))],
        scratch_shapes=[dma(s) if isinstance(s, tuple) else pltpu.VMEM(s.shape, s.dtype) for s in scratch],
        compiler_params=pltpu.CompilerParams(collective_id=collective_id, has_side_effects=True, vmem_limit_bytes=60 << 20),
        name=name,
    )(*ins)


def solution(mesh):
    tp = mesh.shape['tp']
    act_spec = P('dp', 'tp', None)
    rep_vec = P(None)
    part_vec = P('dp')
    in_specs = (act_spec, act_spec, P('dp', None), rep_vec, rep_vec, P(None, None, 'tp', None), P(None, 'tp', None),
                P('tp', None, None), rep_vec, rep_vec, rep_vec, P(None, 'tp'), P('tp'), P('tp', None), rep_vec)
    out_specs = (act_spec, act_spec, part_vec, part_vec, P('dp', None, 'tp', None), P('dp', 'tp', None),
                 P(('dp', 'tp'), None, None), part_vec, part_vec, part_vec, P('dp', 'tp'), P(('dp', 'tp')),
                 P(('dp', 'tp'), None), part_vec)

    def device_step(x_in, grad_y, pad_mask, ln1_gain, ln1_bias, w_qkv, b_qkv, w_out, b_out, ln2_gain, ln2_bias, w_up, b_up, w_down, b_down):
        me = lax.axis_index('tp')
        seq_len = pad_mask.shape[1]
        local_heads, head_dim = w_qkv.shape[2:]
        width = x_in.shape[2]
        heads = local_heads * tp
        q_scale = head_dim ** -0.5
        cos_tab, sin_tab = rope_tables(seq_len, head_dim)
        length = jnp.sum((lax.dynamic_index_in_dim(pad_mask, me, 0) > 0).astype(jnp.int32), axis=1)
        qkv_rows = 3 * local_heads * head_dim
        half_dim = head_dim // 2
        key_bias = jnp.where(jnp.arange(seq_len) < length[0], 0.0, NEG_LARGE).astype(BF16)
        key_bias = jnp.zeros((half_dim, seq_len), BF16).at[0].set(key_bias)
        wq_own = w_qkv.transpose(0, 2, 3, 1).reshape(qkv_rows, width)
        bq_own = jnp.broadcast_to(b_qkv.reshape(1, qkv_rows), (8, qkv_rows))
        wo_own = w_out.reshape(local_heads * head_dim, width)
        bu_own = jnp.broadcast_to(b_up[None], (8,) + b_up.shape)
        (x_full, wq_all, h1, q_ext, k_ext, v_heads, attn_o, attn_wide, lse, wo_all, wu_all, wd_all, bu_all, dy_full) = forward_call(
            x_in, wq_own, bq_own, key_bias, ln1_gain[None], ln1_bias[None], cos_tab[:half_dim], sin_tab[:half_dim], wo_own, w_up, w_down, bu_own, grad_y, local_heads, head_dim)
        chunk = seq_len // tp
        ff = w_up.shape[1]
        rows = heads * head_dim
        vec = jnp.stack([b_out, ln2_gain, ln2_bias, b_down, ln1_gain, ln1_bias, b_out, b_out])
        bu_full = jnp.concatenate([bu_own[None], bu_all])
        o_flat = attn_o.reshape(rows, seq_len)
        ins = (x_full, o_flat, wo_own, wo_all.reshape(-1, width), vec, bu_full, dy_full, w_up, wu_all, w_down, wd_all)
        outs = [shape((tp, chunk, width)), shape((seq_len, width)), shape((width, seq_len), F32), shape((seq_len, width)), shape((rows, seq_len)), shape((8, width), F32)]
        scratch = [shape((tp,) + w_up.shape), shape((tp,) + w_down.shape), shape((tp, ff, seq_len), F32), shape((tp, ff, seq_len)), shape((seq_len, width)), (2, 4), (4,), (4,)]
        y_out, h2, dx1_t, dx1_b, d_o, mid_sums = single_call(middle_kernel, 'middle', 1, ins, (7, 8, 9, 10), outs, (), scratch)
        ins = (q_ext, k_ext, v_heads, d_o.reshape(heads, head_dim, seq_len), attn_wide, lse, cos_tab[:half_dim], sin_tab[:half_dim], o_flat, dx1_b, h2, dy_full)
        group = local_heads * head_dim
        outs = [shape((tp, 3, group, seq_len)), shape((tp, 3, group, 128), F32), shape((group, width), F32), shape((tp - 1, seq_len, width)), shape((tp - 1, seq_len, width))]
        scratch = [shape((tp, group, width), F32), shape((2, group, width), F32), shape((group, width), F32), (3,), (3,), (2, 3), (2, 3)]
        dqkv, gb_wide, grad_w_out, h2_all, dy_all = single_call(functools.partial(backward_kernel, (local_heads, head_dim)), 'backward', 2, ins, (10, 11), outs, (3, 4), scratch)
        gb_part = jnp.broadcast_to(gb_wide[..., 0].reshape(tp, 1, qkv_rows), (tp, 8, qkv_rows))
        vec1 = jnp.stack([ln1_gain, ln1_bias] + [ln1_gain] * 6)
        ins = (dqkv.reshape(tp, qkv_rows, seq_len), gb_part, h1, wq_all, x_full, dx1_t, mid_sums, vec1, bu_own, w_up, w_down, h2, h2_all, dy_full, dy_all)
        outs = [shape((tp, chunk, width)), shape((qkv_rows, width), F32), shape((8, qkv_rows), F32), shape((8, width), F32), shape(w_up.shape, F32), shape((8, ff), F32), shape(w_down.shape, F32)]
        scratch = [shape((tp, qkv_rows, width), F32), shape((2, qkv_rows, width), F32), shape((qkv_rows, width), F32), shape((3, 8, qkv_rows), F32), shape((8, width), F32), shape((3, 8, width), F32),
                   shape((seq_len, width)), shape((tp, seq_len, width)), shape((tp, seq_len, width)), shape((ff, width), F32), shape((ff, 128), F32), (2, 4), (3,), (3,), (2, 4), (2, 4), (4,), (4,)]
        grad_x, grad_w_qkv, grad_b_qkv, sums, grad_w_up, grad_b_up, grad_w_down = single_call(tail_kernel, 'tail', 3, ins, (11, 12, 13, 14), outs, (), scratch)
        grad_w_qkv = grad_w_qkv.reshape(3, local_heads, head_dim, width).transpose(0, 3, 1, 2)
        grad_b_qkv = grad_b_qkv[0].reshape(3, local_heads, head_dim)
        grad_w_out = grad_w_out.reshape(local_heads, head_dim, width)
        return (y_out, grad_x, sums[4], sums[5], grad_w_qkv, grad_b_qkv, grad_w_out, sums[3],
                sums[1], sums[2], grad_w_up, grad_b_up[0], grad_w_down, sums[0])

    return jax.shard_map(device_step, mesh=mesh, in_specs=in_specs, out_specs=out_specs, check_vma=False)
```

```python
import functools

import jax
import jax.numpy as jnp
import numpy as np
from jax import lax
from jax.experimental import pallas as pl
from jax.experimental.pallas import tpu as pltpu
from jax.sharding import PartitionSpec as P

LN_EPS = 1e-5
ROPE_BASE = 10000.0
INV_SQRT2 = 0.7071067811865476
INV_SQRT_2PI = 0.3989422804014327
NEG_LARGE = -1e30
F32 = jnp.float32
BF16 = jnp.bfloat16
MESH = pl.DeviceIdType.MESH


def dot(lhs, rhs):
    return jnp.dot(lhs, rhs, preferred_element_type=F32)


def layer_norm(values, ln_gain, ln_bias):
    centered = values - jnp.mean(values, axis=-1, keepdims=True)
    inv_std = lax.rsqrt(jnp.mean(centered * centered, axis=-1, keepdims=True) + LN_EPS)
    x_hat = centered * inv_std
    return x_hat * ln_gain + ln_bias, x_hat, inv_std


def rope_tables(seq_len, head_dim):
    half_dim = head_dim // 2
    inv_freq = np.float32(ROPE_BASE) ** (np.float32(-2.0) * np.arange(half_dim, dtype=np.float32) / np.float32(head_dim))
    angles = inv_freq[:, None] * np.arange(seq_len, dtype=np.float32)[None, :]
    return np.cos(angles), np.sin(angles)


def remote(src, dst, send_sem, recv_sem, device):
    return pltpu.make_async_remote_copy(src_ref=src, dst_ref=dst, send_sem=send_sem, recv_sem=recv_sem, device_id={'tp': device}, device_id_type=MESH)


def greet(me):
    barrier = pltpu.get_barrier_semaphore()
    for mask in (1, 2, 3):
        pl.semaphore_signal(barrier, inc=1, device_id={'tp': me ^ mask}, device_id_type=MESH)
    pl.semaphore_wait(barrier, 3)


class Gather:
    def __init__(self, src, dst, base, send_sem, recv_sem, me):
        self.near = remote(src, dst.at[1 - base], send_sem.at[0], recv_sem.at[0], me ^ 1)
        self.far = remote(src, dst.at[2 - base], send_sem.at[1], recv_sem.at[1], me ^ 2)
        self.relay = remote(dst.at[2 - base], dst.at[3 - base], send_sem.at[2], recv_sem.at[2], me ^ 1)

    def start(self):
        self.far.start()
        self.near.start()

    def forward(self):
        self.far.wait_recv()
        self.relay.start()

    def finish(self):
        self.near.wait()
        self.far.wait_send()
        self.relay.wait()


def layer_norm_rows(values, ln_gain, ln_bias):
    centered = values - jnp.mean(values, axis=0, keepdims=True)
    inv_std = lax.rsqrt(jnp.mean(centered * centered, axis=0, keepdims=True) + LN_EPS)
    x_hat = centered * inv_std
    return x_hat * ln_gain + ln_bias, x_hat, inv_std


def layer_norm_rows_grad(d_out, x_hat, inv_std, ln_gain):
    d_hat = d_out * ln_gain
    return inv_std * (d_hat - jnp.mean(d_hat, axis=0, keepdims=True) - x_hat * jnp.mean(d_hat * x_hat, axis=0, keepdims=True))


def dot_tn(lhs, rhs):
    return lax.dot_general(lhs, rhs, (((0,), (0,)), ((), ())), preferred_element_type=F32)


def dot_nt(lhs, rhs):
    return lax.dot_general(lhs, rhs, (((1,), (1,)), ((), ())), preferred_element_type=F32)


def gelu(pre_act):
    half_erf = 0.5 * (1.0 + lax.erf(pre_act * INV_SQRT2))
    act = (pre_act * half_erf).astype(BF16)
    return act, half_erf + pre_act * jnp.exp(-0.5 * pre_act * pre_act) * INV_SQRT_2PI


class Copies:
    def __init__(self, copies):
        self.copies = copies

    def start(self):
        for copy in self.copies:
            copy.start()

    def wait(self):
        for copy in self.copies:
            copy.wait()

    def wait_recv(self):
        for copy in self.copies:
            copy.wait_recv()

    def wait_send(self):
        for copy in self.copies:
            copy.wait_send()


def rows_of(owner, chunk):
    return pl.ds(pl.multiple_of(owner * chunk, chunk), chunk)


def to_sequence(src, dst, send_sem, recv_sem, me, chunk):
    return Copies([remote(src.at[me ^ mask], dst.at[rows_of(me, chunk)], send_sem.at[mask], recv_sem.at[mask], me ^ mask) for mask in (2, 3, 1)])


def from_sequence(src, dst, send_sem, recv_sem, me, chunk):
    return Copies([remote(src.at[rows_of(me ^ mask, chunk)], dst.at[me], send_sem.at[mask], recv_sem.at[mask], me ^ mask) for mask in (2, 3, 1)])


def lane_sum(value):
    return jnp.sum(value, axis=1, keepdims=True)


def forward_kernel(dims, x_ref, wq_ref, bq_ref, mask_ref, vec_ref, cos_ref, sin_ref, wo_ref, wu_ref, wd_ref,
                   x_out, wq_out, h1_out, q_out, k_out, v_out, o_out, wide_out, lse_out, wo_all, wu_all, wd_all, vec_all,
                   x_full, wq_all, h1_ref, q_all, k_all, v_all, o_ref, wide_ref, lse_ref, h1t_ref, bq_all,
                   own_sem, once_sem, store_sem, send_sem, recv_sem):
    chunk, local_heads, head_dim = dims
    me = lax.axis_index('tp')
    half = head_dim // 2
    seq_len = mask_ref.shape[1]
    greet(me)
    x_move = to_sequence(x_ref, x_full, send_sem.at[0], recv_sem.at[0], me, chunk)
    wq = Gather(wq_ref, wq_all, 0, send_sem.at[1], recv_sem.at[1], me)
    bq = Gather(bq_ref, bq_all, 0, send_sem.at[2], recv_sem.at[2], me)
    others = [Gather(src, dst, 1, send_sem.at[3 + i], recv_sem.at[3 + i], me) for i, (src, dst) in enumerate(((vec_ref, vec_all), (wo_ref, wo_all), (wu_ref, wu_all), (wd_ref, wd_all)))]
    x_move.start()
    bq.start()
    wq.start()
    own_wq = pltpu.make_async_copy(wq_ref, wq_all.at[0], own_sem)
    own_wq.start()
    for move in others:
        move.start()
    own_rows = rows_of(me, chunk)
    x_full[own_rows] = x_ref[me]
    bq_all[0] = bq_ref[...]
    valid = mask_ref[pl.ds(me, 1)] > 0
    first = lax.broadcasted_iota(jnp.int32, (half, seq_len), 0) == 0
    ones = first.astype(F32).astype(BF16)
    key_bias = jnp.where(first, jnp.where(valid, 0.0, NEG_LARGE), 0.0).astype(BF16)
    x_move.wait_recv()
    x_f = x_full[...].astype(F32)
    h1, _, _ = layer_norm(x_f, vec_ref[4:5], vec_ref[5:6])
    h1 = h1.astype(BF16)
    h1_ref[...] = h1
    h1t_ref[...] = h1.T
    once = Copies([pltpu.make_async_copy(src, dst, once_sem.at[i]) for i, (src, dst) in enumerate(((x_full, x_out), (h1_ref, h1_out), (wq_all, wq_out)))])
    for copy in once.copies[:2]:
        copy.start()
    own_wq.wait()

    def stores(m):
        heads = pl.ds(m * local_heads, local_heads)
        pairs = ((q_all, q_out), (k_all, k_out), (v_all, v_out), (o_ref, o_out), (wide_ref, wide_out), (lse_ref, lse_out))
        return Copies([pltpu.make_async_copy(src.at[heads], dst.at[heads], store_sem.at[i, m]) for i, (src, dst) in enumerate(pairs)])

    @pl.loop(0, 4)
    def _(m):
        @pl.when(m == 1)
        def _():
            bq.near.wait_recv()
            wq.near.wait_recv()

        @pl.when(m == 2)
        def _():
            bq.forward()
            wq.forward()

        @pl.when(m == 3)
        def _():
            bq.relay.wait_recv()
            wq.relay.wait_recv()
            once.copies[2].start()

        bias = bq_all[m].T[:, :1]
        qkv = dot(wq_all[m], h1t_ref[...]) + bias
        cos, sin = cos_ref[...], sin_ref[...]
        group = local_heads * head_dim
        for j in range(local_heads):
            head = m * local_heads + j
            for which, (dst, scale, extra) in enumerate(((q_all, head_dim ** -0.5, ones), (k_all, None, key_bias))):
                rows = qkv[which * group + j * head_dim:which * group + (j + 1) * head_dim]
                rows = rows * scale if scale is not None else rows
                low, high = rows[:half], rows[half:]
                dst[head, :half] = (low * cos - high * sin).astype(BF16)
                dst[head, half:head_dim] = (high * cos + low * sin).astype(BF16)
                dst[head, head_dim:] = extra
            v_all[head] = qkv[2 * group + j * head_dim:2 * group + (j + 1) * head_dim].astype(BF16)

        @pl.loop(0, local_heads)
        def _(j):
            head = m * local_heads + j
            scores = dot(k_all[head].T, q_all[head])
            top = jnp.max(scores, axis=0, keepdims=True)
            weights = jnp.exp(scores - top)
            total = jnp.sum(weights, axis=0, keepdims=True)
            out = dot(v_all[head], weights.astype(BF16)) / total
            o_ref[head] = out.astype(BF16)
            wide_ref[head] = out
            lse_ref[head] = top + jnp.log(total)

        stores(m).start()

    x_move.wait_send()
    for move in (bq, wq):
        move.near.wait_send()
        move.far.wait_send()
        move.relay.wait_send()
    for move in others:
        move.forward()
    for m in range(4):
        stores(m).wait()
    once.wait()
    for move in others:
        move.finish()


def middle_kernel(x_ref, o_ref, wo_ref, wo_far_ref, vec_ref, vec_far_ref, dy_ref, wu_own, wu_far, wd_own, wd_far,
                  y_ref, h2_ref, dx1t_ref, dx1b_ref, do_ref, sums_ref, dy_full, h2_all,
                  wu_all, wd_all, vec_all, slope_ref, act_ref, load_sem, send_sem, recv_sem):
    me = lax.axis_index('tp')
    tp, chunk, width = dy_ref.shape
    ff = wu_own.shape[1]
    greet(me)
    dy_move = to_sequence(dy_ref, dy_full, send_sem.at[0], recv_sem.at[0], me, chunk)
    dy_move.start()
    loads = []
    for m in range(tp):
        wu_src = wu_own if m == 0 else wu_far.at[m - 1]
        wd_src = wd_own if m == 0 else wd_far.at[m - 1]
        loads.append((pltpu.make_async_copy(wu_src, wu_all.at[m], load_sem.at[0, m]), pltpu.make_async_copy(wd_src, wd_all.at[m], load_sem.at[1, m])))
    for load, _ in loads:
        load.start()
    for _, load in loads:
        load.start()
    own_rows = rows_of(me, chunk)
    dy_full[own_rows] = dy_ref[me]
    vec_all[0] = vec_ref[...]
    vec_all[1:] = vec_far_ref[...]
    cols = vec_ref[...].T
    b_out, gain, bias, b_down = (cols[:, i:i + 1] for i in range(4))
    rows = wo_ref.shape[0]
    attn = dot_tn(wo_ref[...], o_ref[:rows]) + dot_tn(wo_far_ref[...], o_ref[rows:])
    x1 = (x_ref[...].T.astype(F32) + (attn + b_out)).astype(BF16).astype(F32)
    h2_f, x_hat, inv_std = layer_norm_rows(x1, gain, bias)
    h2 = h2_f.astype(BF16)
    h2_ref[...] = h2.T
    for load, _ in loads:
        load.wait()
    h2_move = Gather(h2_ref.at[:tp * chunk // 2], h2_all, 1, send_sem.at[1], recv_sem.at[1], me)

    @pl.loop(0, tp)
    def _(m):
        @pl.when(m == 1)
        def _():
            h2_move.start()

        pre_act = dot_tn(wu_all[m], h2) + vec_all[m].T[:, 6:7]
        act, slope = gelu(pre_act)
        act_ref[m] = act
        slope_ref[m] = slope

    for _, load in loads:
        load.wait()
    mlp = dot_tn(wd_all[...].reshape(tp * ff, width), act_ref[...].reshape(tp * ff, tp * chunk))
    y_ref[...] = (x1 + (mlp + b_down)).astype(BF16).T
    dy_move.wait_recv()
    dy_t = dy_full[...].T
    dy_f = dy_t.astype(F32)

    @pl.loop(0, tp)
    def _(m):
        act_ref[m] = (dot(wd_all[m], dy_t) * slope_ref[m]).astype(BF16)

    d_h2 = dot(wu_all[0], act_ref[0])
    for m in range(1, tp):
        d_h2 = d_h2 + dot(wu_all[m], act_ref[m])
    d_x1 = dy_f + layer_norm_rows_grad(d_h2, x_hat, inv_std, gain)
    dx1t_ref[...] = d_x1
    d_x1_b = d_x1.astype(BF16)
    dx1b_ref[...] = d_x1_b.T
    do_ref[:rows] = dot(wo_ref[...], d_x1_b).astype(BF16)
    do_ref[rows:] = dot(wo_far_ref[...], d_x1_b).astype(BF16)
    h2_move.forward()
    sums = [lane_sum(dy_f), lane_sum(d_h2 * x_hat), lane_sum(d_h2), lane_sum(d_x1)]
    sums_ref[...] = jnp.concatenate(sums + [jnp.zeros((width, 124), F32)], axis=1).T[:8]
    dy_move.wait_send()
    h2_move.finish()


def backward_kernel(dims, q_in, k_in, v_in, do_in, wide_in, lse_in, cos_ref, sin_ref, o_ref, dx1b_ref, h1_ref, h2_ref, dy_ref, dy_full, y_ref,
                    dqkv_ref, gb_ref, gwo_ref, far_qk, h2_all, dy_all, y_out,
                    q_all, k_all, v_all, do_ref, wide_ref, lse_ref, part, near_buf, far_buf, part_qk, near_qk,
                    load_sem, own_sem, red_send, red_recv, h2_send, h2_recv, dy_send, dy_recv, y_send, y_recv):
    local_heads, head_dim = dims
    me = lax.axis_index('tp')
    tp, chunk, width = dy_ref.shape
    half = head_dim // 2
    group = local_heads * head_dim

    def loads(m):
        heads = pl.ds(m * local_heads, local_heads)
        pairs = ((q_in, q_all), (k_in, k_all), (v_in, v_all), (do_in, do_ref), (wide_in, wide_ref), (lse_in, lse_ref))
        return Copies([pltpu.make_async_copy(src.at[heads], dst.at[heads], load_sem.at[i, m]) for i, (src, dst) in enumerate(pairs)])

    greet(me)
    for m in range(tp - 1, -1, -1):
        loads(m).start()
    mine, across, partner = rows_of(me, chunk), rows_of(me ^ 2, chunk), me ^ 1
    h2_move = Gather(h2_ref.at[tp * chunk // 2:], h2_all, 1, h2_send, h2_recv, me)
    y_move = from_sequence(y_ref, y_out, y_send, y_recv, me, chunk)
    dy_near = Copies([remote(src, dst, dy_send.at[i], dy_recv.at[i], partner) for i, (src, dst) in enumerate((
        (dy_full, dy_all.at[0]), (dy_ref.at[me ^ 2], dy_all.at[2, mine]), (dy_ref.at[me ^ 3], dy_all.at[1, mine])))])
    dy_far = Copies([remote(dy_ref.at[me ^ i], dy_all.at[1 + i, mine], dy_send.at[3 + i], dy_recv.at[3 + i], me ^ 2) for i in (0, 1)])
    dy_relay = Copies([remote(dy_all.at[1 + i, across], dy_all.at[2 - i, across], dy_send.at[5 + i], dy_recv.at[5 + i], partner) for i in (0, 1)])
    own = Copies([pltpu.make_async_copy(dy_ref.at[me ^ 2], dy_all.at[1, mine], own_sem.at[0]), pltpu.make_async_copy(dy_ref.at[me ^ 3], dy_all.at[2, mine], own_sem.at[1]),
                  pltpu.make_async_copy(y_ref.at[mine], y_out.at[me], own_sem.at[2])])
    h2_move.start()
    dy_far.start()
    dy_near.start()
    own.start()
    reduce_near = Copies([remote(part.at[src], near_buf.at[i], red_send.at[i], red_recv.at[i], partner) for i, src in enumerate((1, 3))])
    reduce_far = remote(part.at[2], far_buf, red_send.at[2], red_recv.at[2], me ^ 2)
    qk_near = remote(part_qk.at[1], near_qk, red_send.at[3], red_recv.at[3], partner)
    qk_far = remote(part_qk.at[0], far_qk, red_send.at[4], red_recv.at[4], me ^ 2)
    part[...] = dot(o_ref[...], dx1b_ref[...]).reshape(part.shape)
    cos, sin = cos_ref[...], sin_ref[...]

    def store(m, j, which, low, high):
        grad = jnp.concatenate([low, high], axis=0)
        at = pl.ds(pl.multiple_of(j * head_dim, head_dim), head_dim)
        dqkv_ref[m, which, at] = grad.astype(BF16)
        gb_ref[m, which, at] = jnp.broadcast_to(lane_sum(grad), (head_dim, 128))

    def back(grad):
        low, high = grad[:half], grad[half:]
        return low * cos + high * sin, high * cos - low * sin

    @pl.loop(0, tp * local_heads)
    def _(step):
        m = tp - 1 - lax.div(step, local_heads)
        j = lax.rem(step, local_heads)
        head = m * local_heads + j

        @pl.when(j == 0)
        def _():
            loads(m).wait()

        @pl.when(step == 1)
        def _():
            reduce_near.start()

        @pl.when(step == 3)
        def _():
            reduce_near.wait()
            part[0] += near_buf[0]
            part[2] += near_buf[1]

        @pl.when(step == 4)
        def _():
            reduce_far.start()

        @pl.when(step == 7)
        def _():
            h2_move.forward()

        @pl.when(step == 10)
        def _():
            for i in (0, 1):
                part_qk[i] = dot(dqkv_ref[2 + i, :2].reshape(2 * group, tp * chunk), h1_ref[...])

        @pl.when(step == 11)
        def _():
            qk_near.start()

        @pl.when(step == 12)
        def _():
            qk_near.wait()
            part_qk[0] += near_qk[...]
            dy_far.wait_recv()
            dy_relay.start()

        @pl.when(step == 13)
        def _():
            qk_far.start()
            y_move.start()

        q, k, v, d_out = q_all[head], k_all[head], v_all[head], do_ref[head]
        delta = jnp.sum(d_out.astype(F32) * wide_ref[head], axis=0, keepdims=True)
        probs = jnp.exp(dot(k.T, q) - lse_ref[head])
        d_probs = dot(v.T, d_out)
        d_scores = (probs * (d_probs - delta)).astype(BF16)
        d_value = dot(probs.astype(BF16), d_out.T).T
        d_key = dot(d_scores, q[:head_dim].T).T
        d_query = dot(k[:head_dim], d_scores)
        low, high = back(d_query)
        scale = head_dim ** -0.5
        store(m, j, 0, low * scale, high * scale)
        low, high = back(d_key)
        store(m, j, 1, low, high)
        store(m, j, 2, d_value[:half], d_value[half:])

    own.wait()
    h2_move.finish()
    dy_near.wait()
    dy_far.wait_send()
    dy_relay.wait()
    reduce_far.wait()
    gwo_ref[...] = part[0] + far_buf[...]
    qk_far.wait()
    y_move.wait()


def tail_kernel(dqkv_ref, gb_ref, h1_ref, wq_in, x_in, dx1t_in, sums_ref, vec_ref, far_qk, wu_in, wd_in, h2_own, h2_low, h2_high, dy_own, dy_far,
                gx_ref, gwq_ref, gb_out, sums_out, gwu_ref, gbu_ref, gwd_ref,
                wq_ref, x_ref, dx1t_ref, wu_ref, wd_ref, part, part_v, near_buf, near_v, far_v, gb_buf, sums_mine, sums_buf, gx_seq, h2_all, dy_all, acc_up, acc_bias,
                first_sem, load_sem, red_send, red_recv, small_send, small_recv, send_sem, recv_sem):
    me = lax.axis_index('tp')
    tp, chunk, width = gx_ref.shape
    group = dqkv_ref.shape[1]
    split = group - part_v.shape[1]
    seq_len = tp * chunk
    first = [pltpu.make_async_copy(src, dst, first_sem.at[i]) for i, (src, dst) in enumerate(((wq_in, wq_ref), (x_in, x_ref), (dx1t_in, dx1t_ref), (wu_in, wu_ref), (wd_in, wd_ref)))]
    for load in first:
        load.start()
    greet(me)
    loads = []
    for m in range(tp):
        if m == 0:
            loads.append([pltpu.make_async_copy(h2_own, h2_all.at[0], load_sem.at[0, m])])
        else:
            loads.append([pltpu.make_async_copy(h2_low.at[m - 1], h2_all.at[m, :seq_len // 2], load_sem.at[0, m]), pltpu.make_async_copy(h2_high.at[m - 1], h2_all.at[m, seq_len // 2:], load_sem.at[2, m])])
        loads[m].append(pltpu.make_async_copy(dy_own if m == 0 else dy_far.at[m - 1], dy_all.at[m], load_sem.at[1, m]))
    for pair in loads:
        for load in pair:
            load.start()
    small = [remote(gb_ref.at[m], gb_buf.at[m - 1], small_send.at[0, m], small_recv.at[0, m], me ^ m) for m in (1, 2, 3)]
    for move in small:
        move.start()
    near = Copies([remote(part.at[1], near_buf, red_send.at[0], red_recv.at[0], me ^ 1), remote(part_v.at[1], near_v, red_send.at[1], red_recv.at[1], me ^ 1)])
    reduce_far = remote(part_v.at[0], far_v, red_send.at[2], red_recv.at[2], me ^ 2)
    h1 = h1_ref[...]
    part[...] = dot(dqkv_ref[:2].reshape(2 * group, seq_len), h1).reshape(part.shape)
    for i in (0, 1):
        part_v[i] = dot(dqkv_ref[2 + i, split:], h1)
    cols = vec_ref[...].T
    gain, bias = cols[:, 4:5], cols[:, 5:6]
    first[0].wait()
    near.start()
    d_h1 = dot_tn(wq_ref[...].reshape(tp * group, width), dqkv_ref[...].reshape(tp * group, seq_len))
    near.wait()
    part_v[0] += near_v[...]
    part[0] += near_buf[...]
    for load in first[1:]:
        load.wait()
    _, x_hat, inv_std = layer_norm_rows(x_ref[...].T.astype(F32), gain, bias)
    reduce_far.start()
    grad_x = (dx1t_ref[...] + layer_norm_rows_grad(d_h1, x_hat, inv_std, gain)).astype(BF16)
    gx_seq[...] = grad_x.T
    sums = [lane_sum(d_h1 * x_hat), lane_sum(d_h1)]
    ln1 = jnp.concatenate(sums + [jnp.zeros((width, 126), F32)], axis=1).T
    sums_mine[...] = jnp.concatenate([sums_ref[:4], ln1[:4]], axis=0)
    gx_ref[me] = gx_seq[rows_of(me, chunk)]
    gx_move = from_sequence(gx_seq, gx_ref, send_sem, recv_sem, me, chunk)
    gx_move.start()
    sums_moves = [remote(sums_mine, sums_buf.at[m - 1], small_send.at[1, m], small_recv.at[1, m], me ^ m) for m in (1, 2, 3)]
    for move in sums_moves:
        move.start()
    for pair in loads:
        for load in pair:
            load.wait()
    acc_up[...] = jnp.zeros_like(acc_up)
    acc_bias[...] = jnp.zeros_like(acc_bias)
    gwd_ref[...] = jnp.zeros_like(gwd_ref)
    wu_t = wu_ref[...].T
    bu_col = cols[:, 6:7]

    @pl.loop(0, tp)
    def _(m):
        act, slope = gelu(dot_nt(wu_t, h2_all[m]) + bu_col)
        d_pre = dot_nt(wd_ref[...], dy_all[m]) * slope
        lanes = d_pre[:, :128]
        for i in range(1, seq_len // 128):
            lanes = lanes + d_pre[:, i * 128:(i + 1) * 128]
        acc_bias[...] += lanes
        gwd_ref[...] += dot(act, dy_all[m])
        acc_up[...] += dot(d_pre.astype(BF16), h2_all[m])

    gwu_ref[...] = acc_up[...].T
    gbu_ref[...] = jnp.broadcast_to(lane_sum(acc_bias[...]), acc_bias.shape).T[:8]
    for move in small + sums_moves:
        move.wait()
    gb_out[...] = gb_ref[0] + gb_buf[0] + (gb_buf[1] + gb_buf[2])
    sums_out[...] = sums_mine[...] + sums_buf[0] + (sums_buf[1] + sums_buf[2])
    gwq_ref[:split] = part[0, :split] + far_qk[...]
    reduce_far.wait()
    gwq_ref[split:] = part[0, split:] + far_v[...]
    gx_move.wait()


VMEM_SPEC = pl.BlockSpec(memory_space=pltpu.VMEM)
ANY_SPEC = pl.BlockSpec(memory_space=pl.ANY)


def shape(dims, dtype=BF16):
    return jax.ShapeDtypeStruct(dims, dtype)


def single_call(kernel, name, collective_id, ins, in_any, outs, out_any, scratch):
    dma = pltpu.SemaphoreType.DMA
    return pl.pallas_call(
        kernel,
        out_shape=outs,
        in_specs=[ANY_SPEC if i in in_any else VMEM_SPEC for i in range(len(ins))],
        out_specs=[ANY_SPEC if i in out_any else VMEM_SPEC for i in range(len(outs))],
        scratch_shapes=[dma(s) if isinstance(s, tuple) else pltpu.VMEM(s.shape, s.dtype) for s in scratch],
        compiler_params=pltpu.CompilerParams(collective_id=collective_id, has_side_effects=True, vmem_limit_bytes=60 << 20),
        name=name,
    )(*ins)


def solution(mesh):
    tp = mesh.shape['tp']
    act_spec = P('dp', 'tp', None)
    rep_vec = P(None)
    part_vec = P('dp')
    in_specs = (act_spec, act_spec, P('dp', None), rep_vec, rep_vec, P(None, None, 'tp', None), P(None, 'tp', None),
                P('tp', None, None), rep_vec, rep_vec, rep_vec, P(None, 'tp'), P('tp'), P('tp', None), rep_vec)
    out_specs = (act_spec, act_spec, part_vec, part_vec, P('dp', None, 'tp', None), P('dp', 'tp', None),
                 P(('dp', 'tp'), None, None), part_vec, part_vec, part_vec, P('dp', 'tp'), P(('dp', 'tp')),
                 P(('dp', 'tp'), None), part_vec)

    def device_step(x_in, grad_y, pad_mask, ln1_gain, ln1_bias, w_qkv, b_qkv, w_out, b_out, ln2_gain, ln2_bias, w_up, b_up, w_down, b_down):
        seq_len = pad_mask.shape[1]
        local_heads, head_dim = w_qkv.shape[2:]
        chunk, width = x_in.shape[1:]
        ff = w_up.shape[1]
        heads = local_heads * tp
        group = local_heads * head_dim
        qkv_rows = 3 * group
        rows = heads * head_dim
        ext = head_dim + head_dim // 2
        dims = (local_heads, head_dim)
        cos_tab, sin_tab = (jnp.asarray(table) for table in rope_tables(seq_len, head_dim))
        wq_own = w_qkv.transpose(0, 2, 3, 1).reshape(qkv_rows, width)
        bq_own = jnp.broadcast_to(b_qkv.reshape(1, qkv_rows), (8, qkv_rows))
        wo_own = w_out.reshape(group, width)
        vec = jnp.stack([b_out, ln2_gain, ln2_bias, b_down, ln1_gain, ln1_bias, b_up, b_up])
        ins = (x_in, wq_own, bq_own, pad_mask, vec, cos_tab, sin_tab, wo_own, w_up, w_down)
        held = [shape((seq_len, width)), shape((tp, qkv_rows, width)), shape((seq_len, width)), shape((heads, ext, seq_len)), shape((heads, ext, seq_len)),
                shape((heads, head_dim, seq_len)), shape((heads, head_dim, seq_len)), shape((heads, head_dim, seq_len), F32), shape((heads, 1, seq_len), F32)]
        outs = held + [shape((tp - 1,) + wo_own.shape), shape((tp - 1,) + w_up.shape), shape((tp - 1,) + w_down.shape), shape((tp - 1,) + vec.shape, F32)]
        scratch = held + [shape((width, seq_len)), shape((tp,) + bq_own.shape, F32), (), (3,), (6, 4), (7, 4), (7, 4)]
        (x_full, wq_all, h1, q_ext, k_ext, v_heads, attn_o, attn_wide, lse, wo_all, wu_all, wd_all, vec_all) = single_call(
            functools.partial(forward_kernel, (chunk,) + dims), 'forward', 0, ins, (1, 7, 8, 9), outs, range(13), scratch)
        o_flat = attn_o.reshape(rows, seq_len)
        ins = (x_full, o_flat, wo_own, wo_all.reshape(-1, width), vec, vec_all, grad_y, w_up, wu_all, w_down, wd_all)
        half_rows = shape((tp - 1, seq_len // 2, width))
        outs = [shape((seq_len, width)), shape((seq_len, width)), shape((width, seq_len), F32), shape((seq_len, width)), shape((rows, seq_len)), shape((8, width), F32), shape((seq_len, width)), half_rows]
        scratch = [shape((tp,) + w_up.shape), shape((tp,) + w_down.shape), shape((tp, 8, width), F32), shape((tp, ff, seq_len), F32), shape((tp, ff, seq_len)), (2, 4), (2, 4), (2, 4)]
        y_seq, h2, dx1_t, dx1_b, d_o, mid_sums, dy_full, h2_low = single_call(middle_kernel, 'middle', 1, ins, (7, 8, 9, 10), outs, (7,), scratch)
        ins = (q_ext, k_ext, v_heads, d_o.reshape(heads, head_dim, seq_len), attn_wide, lse, cos_tab, sin_tab, o_flat, dx1_b, h1, h2, grad_y, dy_full, y_seq)
        outs = [shape((tp, 3, group, seq_len)), shape((tp, 3, group, 128), F32), shape((group, width), F32), shape((2 * group, width), F32), half_rows, shape((tp - 1, seq_len, width)), shape((tp, chunk, width))]
        scratch = [shape(a.shape, a.dtype) for a in ins[:6]] + [shape((tp, group, width), F32), shape((2, group, width), F32), shape((group, width), F32), shape((2, 2 * group, width), F32), shape((2 * group, width), F32),
                   (6, 4), (3,), (5,), (5,), (3,), (3,), (7,), (7,), (4,), (4,)]
        dqkv, gb_wide, grad_w_out, far_qk, h2_high, dy_all, y_out = single_call(functools.partial(backward_kernel, dims), 'backward', 2, ins, (0, 1, 2, 3, 4, 5, 11, 12, 13, 14), outs, (4, 5, 6), scratch)
        gb_part = jnp.broadcast_to(gb_wide[..., 0].reshape(tp, 1, qkv_rows), (tp, 8, qkv_rows))
        ins = (dqkv.reshape(tp, qkv_rows, seq_len), gb_part, h1, wq_all, x_full, dx1_t, mid_sums, vec, far_qk, w_up, w_down, h2, h2_low, h2_high, dy_full, dy_all)
        outs = [shape((tp, chunk, width)), shape((qkv_rows, width), F32), shape((8, qkv_rows), F32), shape((8, width), F32), shape(w_up.shape, F32), shape((8, ff), F32), shape(w_down.shape, F32)]
        scratch = [shape(ins[i].shape, ins[i].dtype) for i in (3, 4, 5, 9, 10)] + [
            shape((2, qkv_rows, width), F32), shape((2, group, width), F32), shape((qkv_rows, width), F32), shape((group, width), F32), shape((group, width), F32), shape((3, 8, qkv_rows), F32), shape((8, width), F32),
            shape((3, 8, width), F32), shape((seq_len, width)), shape((tp, seq_len, width)), shape((tp, seq_len, width)), shape((ff, width), F32), shape((ff, 128), F32),
            (5,), (3, 4), (3,), (3,), (2, 4), (2, 4), (4,), (4,)]
        grad_x, grad_w_qkv, grad_b_qkv, sums, grad_w_up, grad_b_up, grad_w_down = single_call(tail_kernel, 'tail', 3, ins, (3, 4, 5, 9, 10, 11, 12, 13, 14, 15), outs, (), scratch)
        grad_w_qkv = grad_w_qkv.reshape(3, local_heads, head_dim, width).transpose(0, 3, 1, 2)
        grad_b_qkv = grad_b_qkv[0].reshape(3, local_heads, head_dim)
        grad_w_out = grad_w_out.reshape(local_heads, head_dim, width)
        return (y_out, grad_x, sums[4], sums[5], grad_w_qkv, grad_b_qkv, grad_w_out, sums[3],
                sums[1], sums[2], grad_w_up, grad_b_up[0], grad_w_down, sums[0])

    return jax.shard_map(device_step, mesh=mesh, in_specs=in_specs, out_specs=out_specs, check_vma=False)
```

```python
import functools

import jax
import jax.numpy as jnp
import numpy as np
from jax import lax
from jax.experimental import pallas as pl
from jax.experimental.pallas import tpu as pltpu
from jax.sharding import PartitionSpec as P

LN_EPS = 1e-5
ROPE_BASE = 10000.0
INV_SQRT2 = 0.7071067811865476
INV_SQRT_2PI = 0.3989422804014327
NEG_LARGE = -1e30
F32 = jnp.float32
BF16 = jnp.bfloat16
MESH = pl.DeviceIdType.MESH


def dot(lhs, rhs):
    return jnp.dot(lhs, rhs, preferred_element_type=F32)


def layer_norm(values, ln_gain, ln_bias):
    centered = values - jnp.mean(values, axis=-1, keepdims=True)
    inv_std = lax.rsqrt(jnp.mean(centered * centered, axis=-1, keepdims=True) + LN_EPS)
    x_hat = centered * inv_std
    return x_hat * ln_gain + ln_bias, x_hat, inv_std


def rope_tables(seq_len, head_dim):
    half_dim = head_dim // 2
    inv_freq = np.float32(ROPE_BASE) ** (np.float32(-2.0) * np.arange(half_dim, dtype=np.float32) / np.float32(head_dim))
    angles = inv_freq[:, None] * np.arange(seq_len, dtype=np.float32)[None, :]
    return np.cos(angles), np.sin(angles)


def remote(src, dst, send_sem, recv_sem, device):
    return pltpu.make_async_remote_copy(src_ref=src, dst_ref=dst, send_sem=send_sem, recv_sem=recv_sem, device_id={'tp': device}, device_id_type=MESH)


def greet(me, groups=False):
    barrier = pltpu.get_barrier_semaphore()
    for mask in (1, 2, 3):
        pl.semaphore_signal(barrier, inc=1, device_id={'tp': me ^ mask}, device_id_type=MESH)
    if groups:
        pl.semaphore_signal(barrier, inc=1, device_id={'dp': lax.axis_index('dp') ^ 1}, device_id_type=MESH)
    pl.semaphore_wait(barrier, 4 if groups else 3)


class Gather:
    def __init__(self, src, dst, base, send_sem, recv_sem, me):
        self.near = remote(src, dst.at[1 - base], send_sem.at[0], recv_sem.at[0], me ^ 1)
        self.far = remote(src, dst.at[2 - base], send_sem.at[1], recv_sem.at[1], me ^ 2)
        self.relay = remote(dst.at[2 - base], dst.at[3 - base], send_sem.at[2], recv_sem.at[2], me ^ 1)

    def start(self):
        self.far.start()
        self.near.start()

    def forward(self):
        self.far.wait_recv()
        self.relay.start()

    def finish(self):
        self.near.wait()
        self.far.wait_send()
        self.relay.wait()


class SharedGather:
    def __init__(self, src, dst, send_sem, recv_sem, me):
        group = lax.axis_index('dp')
        half, rest = group, group ^ 1
        self.near = remote(src, dst.at[1], send_sem.at[0], recv_sem.at[0], me ^ 1)
        self.far = remote(src.at[half], dst.at[2, half], send_sem.at[1], recv_sem.at[1], me ^ 2)
        self.side = pltpu.make_async_remote_copy(src_ref=dst.at[2, half], dst_ref=dst.at[2, half], send_sem=send_sem.at[2], recv_sem=recv_sem.at[2], device_id={'dp': rest}, device_id_type=MESH)
        self.relay = Copies([remote(dst.at[2, part], dst.at[3, part], send_sem.at[3 + i], recv_sem.at[3 + i], me ^ 1) for i, part in enumerate((half, rest))])

    def start(self):
        self.far.start()
        self.near.start()

    def forward(self):
        self.far.wait_recv()
        self.side.start()
        self.relay.copies[0].start()

    def forward_rest(self):
        self.side.wait_recv()
        self.relay.copies[1].start()

    def wait_send(self):
        for copy in (self.near, self.far, self.side, self.relay):
            copy.wait_send()


def layer_norm_rows(values, ln_gain, ln_bias):
    centered = values - jnp.mean(values, axis=0, keepdims=True)
    inv_std = lax.rsqrt(jnp.mean(centered * centered, axis=0, keepdims=True) + LN_EPS)
    x_hat = centered * inv_std
    return x_hat * ln_gain + ln_bias, x_hat, inv_std


def layer_norm_rows_grad(d_out, x_hat, inv_std, ln_gain):
    d_hat = d_out * ln_gain
    return inv_std * (d_hat - jnp.mean(d_hat, axis=0, keepdims=True) - x_hat * jnp.mean(d_hat * x_hat, axis=0, keepdims=True))


def dot_tn(lhs, rhs):
    return lax.dot_general(lhs, rhs, (((0,), (0,)), ((), ())), preferred_element_type=F32)


def dot_nt(lhs, rhs):
    return lax.dot_general(lhs, rhs, (((1,), (1,)), ((), ())), preferred_element_type=F32)


def gelu(pre_act):
    half_erf = 0.5 * (1.0 + lax.erf(pre_act * INV_SQRT2))
    act = (pre_act * half_erf).astype(BF16)
    return act, half_erf + pre_act * jnp.exp(-0.5 * pre_act * pre_act) * INV_SQRT_2PI


class Copies:
    def __init__(self, copies):
        self.copies = copies

    def start(self):
        for copy in self.copies:
            copy.start()

    def wait(self):
        for copy in self.copies:
            copy.wait()

    def wait_recv(self):
        for copy in self.copies:
            copy.wait_recv()

    def wait_send(self):
        for copy in self.copies:
            copy.wait_send()


def rows_of(owner, chunk):
    return pl.ds(pl.multiple_of(owner * chunk, chunk), chunk)


def to_sequence(src, dst, send_sem, recv_sem, me, chunk):
    return Copies([remote(src.at[me ^ mask], dst.at[rows_of(me, chunk)], send_sem.at[mask], recv_sem.at[mask], me ^ mask) for mask in (2, 3, 1)])


def from_sequence(src, dst, send_sem, recv_sem, me, chunk):
    return Copies([remote(src.at[rows_of(me ^ mask, chunk)], dst.at[me], send_sem.at[mask], recv_sem.at[mask], me ^ mask) for mask in (2, 3, 1)])


def lane_sum(value):
    return jnp.sum(value, axis=1, keepdims=True)


def forward_kernel(dims, x_ref, wq_ref, bq_ref, mask_ref, vec_ref, cos_ref, sin_ref, wo_ref, wu_ref, wd_ref, dy_ref,
                   x_out, wq_out, h1_out, q_out, k_out, v_out, o_out, wide_out, lse_out, y_out, h2_out, dx1t_out, dx1b_out, do_out, dy_out, h2_all, dy_cross, sums_ref,
                   x_full, wq_all, h1_ref, q_all, k_all, v_all, o_ref, wide_ref, lse_ref, h1t_ref, bq_all, wo_all, wu_all, wd_all, vec_all, dy_full,
                   act_ref, stage_ref, wide_stage, own_sem, once_sem, store_sem, x_send, x_recv, dy_send, dy_recv, send_sem, recv_sem, wide_send, wide_recv):
    chunk, local_heads, head_dim = dims
    me = lax.axis_index('tp')
    half = head_dim // 2
    seq_len, width = x_full.shape
    tp, ff = wu_all.shape[0], wu_ref.shape[2]
    greet(me, True)
    x_move = to_sequence(x_ref, x_full, x_send, x_recv, me, chunk)
    dy_move = to_sequence(dy_ref, dy_full, dy_send, dy_recv, me, chunk)
    dy_far = Copies([remote(dy_ref.at[me ^ i], dy_cross.at[i], dy_send.at[4 + i], dy_recv.at[4 + i], me ^ 2) for i in (0, 1)])
    gathered = ((bq_ref, bq_all), (vec_ref, vec_all))
    moves = [Gather(source, dst, 0, send_sem.at[i], recv_sem.at[i], me) for i, (source, dst) in enumerate(gathered)]
    bq, vec = moves
    weights = ((wq_ref, wq_all), (wo_ref, wo_all), (wu_ref, wu_all), (wd_ref, wd_all))
    shared = [SharedGather(source, dst, wide_send.at[i], wide_recv.at[i], me) for i, (source, dst) in enumerate(weights)]
    wq, wo, wu, wd = shared
    own = [pltpu.make_async_copy(source, dst.at[0], own_sem.at[i]) for i, (source, dst) in enumerate(gathered + weights)]
    x_move.start()
    bq.start()
    wq.start()
    for copy in own:
        copy.start()
    for move in (vec, wo, wu, wd, dy_move, dy_far):
        move.start()
    own_rows = rows_of(me, chunk)
    own_x = pltpu.make_async_copy(x_ref.at[me], x_full.at[own_rows], once_sem.at[0])
    own_dy = pltpu.make_async_copy(dy_ref.at[me], dy_full.at[own_rows], once_sem.at[1])
    own_x.start()
    own_dy.start()
    valid = mask_ref[pl.ds(me, 1)] > 0
    first = lax.broadcasted_iota(jnp.int32, (half, seq_len), 0) == 0
    ones = first.astype(F32).astype(BF16)
    key_bias = jnp.where(first, jnp.where(valid, 0.0, NEG_LARGE), 0.0).astype(BF16)
    for copy in own:
        copy.wait()
    own_x.wait()
    x_move.wait_recv()
    h1, _, _ = layer_norm(x_full[...].astype(F32), vec_all[0, 4:5], vec_all[0, 5:6])
    h1 = h1.astype(BF16)
    h1_ref[...] = h1
    h1t_ref[...] = h1.T
    once = [pltpu.make_async_copy(source, dst, once_sem.at[2 + i]) for i, (source, dst) in enumerate((
        (x_full, x_out), (h1_ref, h1_out), (wq_all, wq_out), (stage_ref.at[0], h2_out), (stage_ref.at[1], y_out), (stage_ref.at[2], dx1b_out), (wide_stage, dx1t_out), (dy_full, dy_out)))]
    once[0].start()
    once[1].start()

    def stores(m):
        heads = pl.ds(m * local_heads, local_heads)
        pairs = ((q_all, q_out), (k_all, k_out), (v_all, v_out), (o_ref, o_out), (wide_ref, wide_out), (lse_ref, lse_out))
        return Copies([pltpu.make_async_copy(source.at[heads], dst.at[heads], store_sem.at[i, m]) for i, (source, dst) in enumerate(pairs)])

    @pl.loop(0, 4)
    def _(m):
        @pl.when(m == 1)
        def _():
            bq.near.wait_recv()
            wq.near.wait_recv()
            bq.forward()
            wq.forward()

        @pl.when(m == 2)
        def _():
            wq.forward_rest()
            vec.forward()
            wo.forward()

        @pl.when(m == 3)
        def _():
            bq.relay.wait_recv()
            wq.relay.wait_recv()
            once[2].start()
            wo.forward_rest()
            wu.forward()
            wd.forward()

        bias = bq_all[m].T[:, :1]
        qkv = dot(wq_all[m].reshape(bias.shape[0], width), h1t_ref[...]) + bias
        cos, sin = cos_ref[...], sin_ref[...]
        group = local_heads * head_dim
        for j in range(local_heads):
            head = m * local_heads + j
            for which, (dst, scale, extra) in enumerate(((q_all, head_dim ** -0.5, ones), (k_all, None, key_bias))):
                rows = qkv[which * group + j * head_dim:which * group + (j + 1) * head_dim]
                rows = rows * scale if scale is not None else rows
                low, high = rows[:half], rows[half:]
                dst[head, :half] = (low * cos - high * sin).astype(BF16)
                dst[head, half:head_dim] = (high * cos + low * sin).astype(BF16)
                dst[head, head_dim:] = extra
            v_all[head] = qkv[2 * group + j * head_dim:2 * group + (j + 1) * head_dim].astype(BF16)

        @pl.loop(0, local_heads)
        def _(j):
            head = m * local_heads + j
            scores = dot(k_all[head].T, q_all[head])
            top = jnp.max(scores, axis=0, keepdims=True)
            weights = jnp.exp(scores - top)
            total = jnp.sum(weights, axis=0, keepdims=True)
            out = dot(v_all[head], weights.astype(BF16)) / total
            o_ref[head] = out.astype(BF16)
            wide_ref[head] = out
            lse_ref[head] = top + jnp.log(total)

        stores(m).start()

    wu.forward_rest()
    wd.forward_rest()
    for move in (vec, wo):
        move.near.wait_recv()
        move.relay.wait_recv()
    rows = tp * local_heads * head_dim
    wo_full = wo_all[...].reshape(rows, width)
    cols = vec_all[0].T
    b_out, gain, bias, b_down = (cols[:, i:i + 1] for i in range(4))
    attn = dot_tn(wo_full, o_ref[...].reshape(rows, seq_len))
    x1 = (x_full[...].T.astype(F32) + (attn + b_out)).astype(BF16).astype(F32)
    h2_f, x_hat, inv_std = layer_norm_rows(x1, gain, bias)
    h2 = h2_f.astype(BF16)
    stage_ref[0] = h2.T
    wu.near.wait_recv()
    wu.relay.wait_recv()
    h2_move = Gather(stage_ref.at[0, :h2_all.shape[1]], h2_all, 1, send_sem.at[2], recv_sem.at[2], me)

    def mlp(slope_ref):
        @pl.loop(0, tp)
        def _(m):
            @pl.when(m == 1)
            def _():
                h2_move.start()
                once[3].start()

            pre_act = dot_tn(wu_all[m].reshape(width, ff), h2) + vec_all[m].T[:, 6:7]
            act, slope = gelu(pre_act)
            act_ref[m] = act
            slope_ref[m] = slope

        wd.near.wait_recv()
        wd.relay.wait_recv()
        out = dot_tn(wd_all[...].reshape(tp * ff, width), act_ref[...].reshape(tp * ff, seq_len))
        stage_ref[1] = (x1 + (out + b_down)).astype(BF16).T
        own_dy.wait()
        dy_move.wait_recv()
        once[7].start()
        dy_t = dy_full[...].T

        @pl.loop(0, tp)
        def _(m):
            @pl.when(m == 1)
            def _():
                once[4].start()

            act_ref[m] = (dot(wd_all[m].reshape(ff, width), dy_t) * slope_ref[m]).astype(BF16)

    pl.run_scoped(mlp, pltpu.VMEM((tp, ff, seq_len), F32))
    d_h2 = dot(wu_all[0].reshape(width, ff), act_ref[0])
    for m in range(1, tp):
        d_h2 = d_h2 + dot(wu_all[m].reshape(width, ff), act_ref[m])
    dy_f = dy_full[...].T.astype(F32)
    d_x1 = dy_f + layer_norm_rows_grad(d_h2, x_hat, inv_std, gain)
    d_x1_b = d_x1.astype(BF16)
    wide_stage[...] = d_x1
    stage_ref[2] = d_x1_b.T
    for m in range(4):
        stores(m).wait()
    o_ref[...] = dot(wo_full, d_x1_b).astype(BF16).reshape(o_ref.shape)
    h2_move.forward()
    once[5].start()
    once[6].start()
    sums = [lane_sum(dy_f), lane_sum(d_h2 * x_hat), lane_sum(d_h2), lane_sum(d_x1)]
    sums_ref[...] = jnp.concatenate(sums + [jnp.zeros((width, 124), F32)], axis=1).T[:8]
    last = pltpu.make_async_copy(o_ref, do_out, once_sem.at[10])
    last.start()
    x_move.wait_send()
    dy_move.wait_send()
    dy_far.wait()
    for move in moves:
        move.near.wait_send()
        move.far.wait_send()
        move.relay.wait_send()
    for move in shared:
        move.wait_send()
    for copy in once:
        copy.wait()
    last.wait()
    h2_move.finish()


def backward_kernel(dims, q_in, k_in, v_in, do_in, wide_in, lse_in, cos_ref, sin_ref, o_in, dx1b_in, h1_in, h2_ref, dy_ref, dy_full, y_ref,
                    wq_in, x_in, dx1t_in, sums_ref, vec_ref, wu_in, wd_in, h2_low, dy_cross,
                    y_out, gwo_ref, gx_ref, gwq_ref, gb_out, sums_out, gwu_ref, gbu_ref, gwd_ref, h2_high, dy_all,
                    dqkv_ref, gb_ref, h1_ref, near_buf, far_buf, near_gwq, far_gwq, near_last, gb_rows, gb_buf, sums_mine, sums_buf, gx_seq,
                    own_sem, load_sem, first_sem, tail_sem, red_send, red_recv, small_send, small_recv, h2_send, h2_recv, dy_send, dy_recv, y_send, y_recv, gx_send, gx_recv):
    local_heads, head_dim = dims
    me = lax.axis_index('tp')
    tp, chunk, width = dy_ref.shape
    half = head_dim // 2
    group = local_heads * head_dim
    rows = 3 * group
    seq_len = tp * chunk
    low_rows = h2_low.shape[1]
    mine, across, partner = rows_of(me, chunk), rows_of(me ^ 2, chunk), me ^ 1
    greet(me)
    h2_move = Gather(h2_ref.at[low_rows:], h2_high, 1, h2_send, h2_recv, me)
    y_move = from_sequence(y_ref, y_out, y_send, y_recv, me, chunk)
    dy_near = Copies([remote(source, dst, dy_send.at[i], dy_recv.at[i], partner) for i, (source, dst) in enumerate((
        (dy_full, dy_all.at[0]), (dy_ref.at[me ^ 2], dy_all.at[2, mine]), (dy_ref.at[me ^ 3], dy_all.at[1, mine])))])
    dy_relay = Copies([remote(dy_cross.at[i], dy_all.at[2 - i, across], dy_send.at[3 + i], dy_recv.at[3 + i], partner) for i in (0, 1)])
    own = Copies([pltpu.make_async_copy(dy_ref.at[me ^ 2], dy_all.at[1, mine], own_sem.at[0]), pltpu.make_async_copy(dy_ref.at[me ^ 3], dy_all.at[2, mine], own_sem.at[1]),
                  pltpu.make_async_copy(y_ref.at[mine], y_out.at[me], own_sem.at[2])]
                 + [pltpu.make_async_copy(dy_cross.at[i], dy_all.at[1 + i, across], own_sem.at[3 + i]) for i in (0, 1)])
    h2_move.start()
    y_move.start()
    dy_near.start()
    dy_relay.start()
    cos, sin = cos_ref[...], sin_ref[...]

    def store(m, j, which, low, high):
        grad = jnp.concatenate([low, high], axis=0)
        at = pl.ds(pl.multiple_of(which * group + j * head_dim, head_dim), head_dim)
        dqkv_ref[m, at] = grad.astype(BF16)
        gb_ref[m, at] = jnp.broadcast_to(lane_sum(grad), (head_dim, 128))

    def back(grad):
        low, high = grad[:half], grad[half:]
        return low * cos + high * sin, high * cos - low * sin

    def attention(q_all, k_all, v_all, do_ref, wide_ref, lse_ref, o_ref, dx1b_ref, part, part_gwq):
        def loads(m):
            heads = pl.ds(m * local_heads, local_heads)
            pairs = ((q_in, q_all), (k_in, k_all), (v_in, v_all), (do_in, do_ref), (wide_in, wide_ref), (lse_in, lse_ref))
            return Copies([pltpu.make_async_copy(source.at[heads], dst.at[heads], load_sem.at[i, m]) for i, (source, dst) in enumerate(pairs)])

        early = Copies([pltpu.make_async_copy(source, dst, first_sem.at[i]) for i, (source, dst) in enumerate(((o_in, o_ref), (dx1b_in, dx1b_ref), (h1_in, h1_ref)))])
        early.start()
        for m in range(tp - 1, -1, -1):
            loads(m).start()
        own.start()
        reduce_near = Copies([remote(part.at[source], near_buf.at[i], red_send.at[i], red_recv.at[i], partner) for i, source in enumerate((1, 3))])
        reduce_far = remote(part.at[2], far_buf, red_send.at[2], red_recv.at[2], me ^ 2)
        gwq_near = remote(part_gwq.at[1], near_gwq, red_send.at[3], red_recv.at[3], partner)
        gwq_far = remote(part_gwq.at[0], far_gwq, red_send.at[4], red_recv.at[4], me ^ 2)
        early.wait()
        part[...] = dot(o_ref[...].reshape(tp * group, seq_len), dx1b_ref[...]).reshape(part.shape)

        @pl.loop(0, tp * local_heads)
        def _(step):
            m = tp - 1 - lax.div(step, local_heads)
            j = lax.rem(step, local_heads)
            head = m * local_heads + j

            @pl.when(j == 0)
            def _():
                loads(m).wait()

            @pl.when(step == 1)
            def _():
                reduce_near.start()

            @pl.when(step == 3)
            def _():
                reduce_near.wait()
                part[0] += near_buf[0]
                part[2] += near_buf[1]

            @pl.when(step == 4)
            def _():
                reduce_far.start()

            @pl.when(step == 6)
            def _():
                h2_move.forward()

            @pl.when(step == 10)
            def _():
                for i in (0, 1):
                    part_gwq[i] = dot(dqkv_ref[2 + i], h1_ref[...])

            @pl.when(step == 11)
            def _():
                gwq_near.start()

            @pl.when(step == 12)
            def _():
                gwq_near.wait()
                part_gwq[0] += near_gwq[...]

            @pl.when(step == 13)
            def _():
                gwq_far.start()

            q, k, v, d_out = q_all[head], k_all[head], v_all[head], do_ref[head]
            delta = jnp.sum(d_out.astype(F32) * wide_ref[head], axis=0, keepdims=True)
            probs = jnp.exp(dot(k.T, q) - lse_ref[head])
            d_probs = dot(v.T, d_out)
            d_scores = (probs * (d_probs - delta)).astype(BF16)
            d_value = dot(probs.astype(BF16), d_out.T).T
            d_key = dot(d_scores, q[:head_dim].T).T
            d_query = dot(k[:head_dim], d_scores)
            low, high = back(d_query)
            scale = head_dim ** -0.5
            store(m, j, 0, low * scale, high * scale)
            low, high = back(d_key)
            store(m, j, 1, low, high)
            store(m, j, 2, d_value[:half], d_value[half:])

        own.wait()
        y_move.wait()
        h2_move.finish()
        dy_near.wait()
        dy_relay.wait()
        reduce_far.wait()
        gwo_ref[...] = part[0] + far_buf[...]
        gwq_far.wait_send()

    heads_all = tp * local_heads

    def vm(array):
        return pltpu.VMEM(array.shape, array.dtype)

    pl.run_scoped(attention, vm(q_in), vm(k_in), vm(v_in), vm(do_in), vm(wide_in), vm(lse_in), vm(o_in), vm(dx1b_in), pltpu.VMEM((tp, group, width), F32), pltpu.VMEM((2, rows, width), F32))

    def tail(wq_ref, x_ref, dx1t_ref, wu_ref, wd_ref, h2_all, dy_full_all, part, acc_up, acc_bias):
        first = [pltpu.make_async_copy(source, dst, tail_sem.at[i]) for i, (source, dst) in enumerate(((wq_in, wq_ref), (x_in, x_ref), (dx1t_in, dx1t_ref), (wu_in, wu_ref), (wd_in, wd_ref)))]
        for m in range(tp):
            if m == 0:
                first.append(pltpu.make_async_copy(h2_ref, h2_all.at[0], tail_sem.at[5]))
                first.append(pltpu.make_async_copy(dy_full, dy_full_all.at[0], tail_sem.at[6]))
            else:
                first.append(pltpu.make_async_copy(h2_low.at[m - 1], h2_all.at[m, :low_rows], tail_sem.at[4 + 3 * m]))
                first.append(pltpu.make_async_copy(h2_high.at[m - 1], h2_all.at[m, low_rows:], tail_sem.at[5 + 3 * m]))
                first.append(pltpu.make_async_copy(dy_all.at[m - 1], dy_full_all.at[m], tail_sem.at[6 + 3 * m]))
        for load in first:
            load.start()
        near = remote(part.at[1], near_last, red_send.at[5], red_recv.at[5], partner)
        part[...] = dot(dqkv_ref[:2].reshape(2 * rows, seq_len), h1_ref[...]).reshape(part.shape)
        cols = vec_ref[...].T
        gain, bias = cols[:, 4:5], cols[:, 5:6]
        first[0].wait()
        near.start()
        d_h1 = dot_tn(wq_ref[...].reshape(tp * rows, width), dqkv_ref[...].reshape(tp * rows, seq_len))
        for load in first[1:]:
            load.wait()
        _, x_hat, inv_std = layer_norm_rows(x_ref[...].T.astype(F32), gain, bias)
        grad_x = (dx1t_ref[...] + layer_norm_rows_grad(d_h1, x_hat, inv_std, gain)).astype(BF16)
        gx_seq[...] = grad_x.T
        sums = [lane_sum(d_h1 * x_hat), lane_sum(d_h1)]
        ln1 = jnp.concatenate(sums + [jnp.zeros((width, 126), F32)], axis=1).T
        sums_mine[...] = jnp.concatenate([sums_ref[:4], ln1[:4]], axis=0)
        gx_ref[me] = gx_seq[mine]
        for m in range(tp):
            gb_rows[m] = gb_ref[m].T[:8]
        small = [remote(gb_rows.at[m], gb_buf.at[m - 1], small_send.at[0, m], small_recv.at[0, m], me ^ m) for m in (1, 2, 3)]
        small += [remote(sums_mine, sums_buf.at[m - 1], small_send.at[1, m], small_recv.at[1, m], me ^ m) for m in (1, 2, 3)]
        for move in small:
            move.start()
        gx_move = from_sequence(gx_seq, gx_ref, gx_send, gx_recv, me, chunk)
        gx_move.start()
        acc_up[...] = jnp.zeros_like(acc_up)
        acc_bias[...] = jnp.zeros_like(acc_bias)
        gwd_ref[...] = jnp.zeros_like(gwd_ref)
        wu_t = wu_ref[...].T
        bu_col = cols[:, 6:7]

        @pl.loop(0, tp)
        def _(m):
            act, slope = gelu(dot_nt(wu_t, h2_all[m]) + bu_col)
            d_pre = dot_nt(wd_ref[...], dy_full_all[m]) * slope
            lanes = d_pre[:, :128]
            for i in range(1, seq_len // 128):
                lanes = lanes + d_pre[:, i * 128:(i + 1) * 128]
            acc_bias[...] += lanes
            gwd_ref[...] += dot(act, dy_full_all[m])
            acc_up[...] += dot(d_pre.astype(BF16), h2_all[m])

        gwu_ref[...] = acc_up[...].T
        gbu_ref[...] = jnp.broadcast_to(lane_sum(acc_bias[...]), acc_bias.shape).T[:8]
        near.wait()
        remote(part.at[0], far_gwq, red_send.at[4], red_recv.at[4], me ^ 2).wait_recv()
        gwq_ref[...] = part[0] + near_last[...] + far_gwq[...]
        for move in small:
            move.wait()
        gb_out[...] = gb_rows[0] + gb_buf[0] + (gb_buf[1] + gb_buf[2])
        sums_out[...] = sums_mine[...] + sums_buf[0] + (sums_buf[1] + sums_buf[2])
        gx_move.wait()

    pl.run_scoped(tail, vm(wq_in), vm(x_in), vm(dx1t_in), vm(wu_in), vm(wd_in), pltpu.VMEM((tp, seq_len, width), BF16), pltpu.VMEM((tp, seq_len, width), BF16),
                  pltpu.VMEM((2, rows, width), F32), pltpu.VMEM((wd_in.shape[0], width), F32), pltpu.VMEM((wd_in.shape[0], 128), F32))


VMEM_SPEC = pl.BlockSpec(memory_space=pltpu.VMEM)
ANY_SPEC = pl.BlockSpec(memory_space=pl.ANY)


def shape(dims, dtype=BF16):
    return jax.ShapeDtypeStruct(dims, dtype)


def single_call(kernel, name, collective_id, ins, in_any, outs, out_any, scratch):
    dma = pltpu.SemaphoreType.DMA
    return pl.pallas_call(
        kernel,
        out_shape=outs,
        in_specs=[ANY_SPEC if i in in_any else VMEM_SPEC for i in range(len(ins))],
        out_specs=[ANY_SPEC if i in out_any else VMEM_SPEC for i in range(len(outs))],
        scratch_shapes=[dma(s) if isinstance(s, tuple) else pltpu.VMEM(s.shape, s.dtype) for s in scratch],
        compiler_params=pltpu.CompilerParams(collective_id=collective_id, has_side_effects=True, vmem_limit_bytes=67043328),
        name=name,
    )(*ins)


def solution(mesh):
    tp = mesh.shape['tp']
    act_spec = P('dp', 'tp', None)
    rep_vec = P(None)
    part_vec = P('dp')
    in_specs = (act_spec, act_spec, P('dp', None), rep_vec, rep_vec, P(None, None, 'tp', None), P(None, 'tp', None),
                P('tp', None, None), rep_vec, rep_vec, rep_vec, P(None, 'tp'), P('tp'), P('tp', None), rep_vec)
    out_specs = (act_spec, act_spec, part_vec, part_vec, P('dp', None, 'tp', None), P('dp', 'tp', None),
                 P(('dp', 'tp'), None, None), part_vec, part_vec, part_vec, P('dp', 'tp'), P(('dp', 'tp')),
                 P(('dp', 'tp'), None), part_vec)

    def device_step(x_in, grad_y, pad_mask, ln1_gain, ln1_bias, w_qkv, b_qkv, w_out, b_out, ln2_gain, ln2_bias, w_up, b_up, w_down, b_down):
        seq_len = pad_mask.shape[1]
        local_heads, head_dim = w_qkv.shape[2:]
        chunk, width = x_in.shape[1:]
        ff = w_up.shape[1]
        heads = local_heads * tp
        group = local_heads * head_dim
        qkv_rows = 3 * group
        ext = head_dim + head_dim // 2
        low_rows = seq_len // 2
        dims = (local_heads, head_dim)
        cos_tab, sin_tab = (jnp.asarray(table) for table in rope_tables(seq_len, head_dim))
        wq_own = w_qkv.transpose(0, 2, 3, 1).reshape(2, qkv_rows // 2, width)
        bq_own = jnp.broadcast_to(b_qkv.reshape(1, qkv_rows), (8, qkv_rows))
        wo_own = w_out.reshape(2, group // 2, width)
        wu_own = w_up.reshape(2, width // 2, ff)
        wd_own = w_down.reshape(2, ff // 2, width)
        vec = jnp.stack([b_out, ln2_gain, ln2_bias, b_down, ln1_gain, ln1_bias, b_up, b_up])
        act = shape((seq_len, width))
        by_head = shape((heads, head_dim, seq_len))
        ext_head = shape((heads, ext, seq_len))
        held = [act, shape((tp,) + wq_own.shape), act, ext_head, ext_head, by_head, by_head, shape(by_head.shape, F32), shape((heads, 1, seq_len), F32)]
        d_x1_t = shape((width, seq_len), F32)
        rows8 = shape((8, width), F32)
        ins = (x_in, wq_own, bq_own, pad_mask, vec, cos_tab, sin_tab, wo_own, wu_own, wd_own, grad_y)
        outs = held + [act, act, d_x1_t, act, by_head, act, shape((tp - 1, low_rows, width)), shape((2, chunk, width)), rows8]
        scratch = held + [shape((width, seq_len)), shape((tp,) + bq_own.shape, F32), shape((tp,) + wo_own.shape), shape((tp,) + wu_own.shape), shape((tp,) + wd_own.shape), shape((tp,) + vec.shape, F32), act,
                          shape((tp, ff, seq_len)), shape((3, seq_len, width)), d_x1_t, (6,), (11,), (6, 4), (4,), (4,), (6,), (6,), (3, 3), (3, 3), (4, 5), (4, 5)]
        (x_full, wq_all, h1, q_ext, k_ext, v_heads, attn_o, attn_wide, lse, y_seq, h2, dx1_t, dx1_b, d_o, dy_full, h2_low, dy_cross, mid_sums) = single_call(
            functools.partial(forward_kernel, (chunk,) + dims), 'forward', 0, ins, (0, 1, 2, 4, 7, 8, 9, 10), outs, range(17), scratch)
        ins = (q_ext, k_ext, v_heads, d_o, attn_wide, lse, cos_tab, sin_tab, attn_o, dx1_b, h1, h2, grad_y, dy_full, y_seq, wq_all.reshape(tp, qkv_rows, width), x_full, dx1_t, mid_sums, vec, w_up, w_down, h2_low, dy_cross)
        gwq = shape((qkv_rows, width), F32)
        gwo = shape((group, width), F32)
        outs = [shape((tp, chunk, width)), gwo, shape((tp, chunk, width)), gwq, shape((8, qkv_rows), F32), rows8, shape(w_up.shape, F32), shape((8, ff), F32), shape(w_down.shape, F32),
                shape((tp - 1, seq_len - low_rows, width)), shape((tp - 1, seq_len, width))]
        scratch = [shape((tp, qkv_rows, seq_len)), shape((tp, qkv_rows, 128), F32), act, shape((2, group, width), F32), gwo, gwq, gwq, gwq, shape((tp, 8, qkv_rows), F32), shape((3, 8, qkv_rows), F32), rows8, shape((3, 8, width), F32), act,
                   (5,), (6, 4), (3,), (16,), (6,), (6,), (2, 4), (2, 4), (3,), (3,), (5,), (5,), (4,), (4,), (4,), (4,)]
        y_out, grad_w_out, grad_x, grad_w_qkv, grad_b_qkv, sums, grad_w_up, grad_b_up, grad_w_down, _, _ = single_call(
            functools.partial(backward_kernel, dims), 'backward', 1, ins, (0, 1, 2, 3, 4, 5, 8, 9, 10, 11, 12, 13, 14, 15, 16, 17, 20, 21, 22, 23), outs, (0, 9, 10), scratch)
        grad_w_qkv = grad_w_qkv.reshape(3, local_heads, head_dim, width).transpose(0, 3, 1, 2)
        grad_b_qkv = grad_b_qkv[0].reshape(3, local_heads, head_dim)
        grad_w_out = grad_w_out.reshape(local_heads, head_dim, width)
        return (y_out, grad_x, sums[4], sums[5], grad_w_qkv, grad_b_qkv, grad_w_out, sums[3],
                sums[1], sums[2], grad_w_up, grad_b_up[0], grad_w_down, sums[0])

    return jax.shard_map(device_step, mesh=mesh, in_specs=in_specs, out_specs=out_specs, check_vma=False)
```

```python
import functools

import jax
import jax.numpy as jnp
import numpy as np
from jax import lax
from jax.experimental import pallas as pl
from jax.experimental.pallas import tpu as pltpu
from jax.sharding import PartitionSpec as P

LN_EPS = 1e-5
ROPE_BASE = 10000.0
INV_SQRT2 = 0.7071067811865476
INV_SQRT_2PI = 0.3989422804014327
NEG_LARGE = -1e30
F32 = jnp.float32
BF16 = jnp.bfloat16
MESH = pl.DeviceIdType.MESH


def dot(lhs, rhs):
    return jnp.dot(lhs, rhs, preferred_element_type=F32)


def layer_norm(values, ln_gain, ln_bias):
    centered = values - jnp.mean(values, axis=-1, keepdims=True)
    inv_std = lax.rsqrt(jnp.mean(centered * centered, axis=-1, keepdims=True) + LN_EPS)
    x_hat = centered * inv_std
    return x_hat * ln_gain + ln_bias, x_hat, inv_std


def rope_tables(seq_len, head_dim):
    half_dim = head_dim // 2
    inv_freq = np.float32(ROPE_BASE) ** (np.float32(-2.0) * np.arange(half_dim, dtype=np.float32) / np.float32(head_dim))
    angles = inv_freq[:, None] * np.arange(seq_len, dtype=np.float32)[None, :]
    return np.cos(angles), np.sin(angles)


def remote(src, dst, send_sem, recv_sem, device):
    return pltpu.make_async_remote_copy(src_ref=src, dst_ref=dst, send_sem=send_sem, recv_sem=recv_sem, device_id={'tp': device}, device_id_type=MESH)


def greet(me, groups=False):
    barrier = pltpu.get_barrier_semaphore()
    for mask in (1, 2, 3):
        pl.semaphore_signal(barrier, inc=1, device_id={'tp': me ^ mask}, device_id_type=MESH)
    if groups:
        pl.semaphore_signal(barrier, inc=1, device_id={'dp': lax.axis_index('dp') ^ 1}, device_id_type=MESH)
    pl.semaphore_wait(barrier, 4 if groups else 3)


class Gather:
    def __init__(self, src, dst, base, send_sem, recv_sem, me):
        self.near = remote(src, dst.at[1 - base], send_sem.at[0], recv_sem.at[0], me ^ 1)
        self.far = remote(src, dst.at[2 - base], send_sem.at[1], recv_sem.at[1], me ^ 2)
        self.relay = remote(dst.at[2 - base], dst.at[3 - base], send_sem.at[2], recv_sem.at[2], me ^ 1)

    def start(self):
        self.far.start()
        self.near.start()

    def forward(self):
        self.far.wait_recv()
        self.relay.start()

    def finish(self):
        self.near.wait()
        self.far.wait_send()
        self.relay.wait()


class SharedGather:
    def __init__(self, src, dst, send_sem, recv_sem, me):
        group = lax.axis_index('dp')
        half, rest = group, group ^ 1
        self.near = remote(src, dst.at[1], send_sem.at[0], recv_sem.at[0], me ^ 1)
        self.far = remote(src.at[half], dst.at[2, half], send_sem.at[1], recv_sem.at[1], me ^ 2)
        self.side = pltpu.make_async_remote_copy(src_ref=dst.at[2, half], dst_ref=dst.at[2, half], send_sem=send_sem.at[2], recv_sem=recv_sem.at[2], device_id={'dp': rest}, device_id_type=MESH)
        self.relay = Copies([remote(dst.at[2, part], dst.at[3, part], send_sem.at[3 + i], recv_sem.at[3 + i], me ^ 1) for i, part in enumerate((half, rest))])

    def start(self):
        self.far.start()
        self.near.start()

    def forward(self):
        self.far.wait_recv()
        self.side.start()
        self.relay.copies[0].start()

    def forward_rest(self):
        self.side.wait_recv()
        self.relay.copies[1].start()

    def wait_send(self):
        for copy in (self.near, self.far, self.side, self.relay):
            copy.wait_send()


def layer_norm_rows(values, ln_gain, ln_bias):
    centered = values - jnp.mean(values, axis=0, keepdims=True)
    inv_std = lax.rsqrt(jnp.mean(centered * centered, axis=0, keepdims=True) + LN_EPS)
    x_hat = centered * inv_std
    return x_hat * ln_gain + ln_bias, x_hat, inv_std


def layer_norm_rows_grad(d_out, x_hat, inv_std, ln_gain):
    d_hat = d_out * ln_gain
    return inv_std * (d_hat - jnp.mean(d_hat, axis=0, keepdims=True) - x_hat * jnp.mean(d_hat * x_hat, axis=0, keepdims=True))


def dot_tn(lhs, rhs):
    return lax.dot_general(lhs, rhs, (((0,), (0,)), ((), ())), preferred_element_type=F32)


def dot_nt(lhs, rhs):
    return lax.dot_general(lhs, rhs, (((1,), (1,)), ((), ())), preferred_element_type=F32)


def gelu(pre_act):
    half_erf = 0.5 * (1.0 + lax.erf(pre_act * INV_SQRT2))
    act = (pre_act * half_erf).astype(BF16)
    return act, half_erf + pre_act * jnp.exp(-0.5 * pre_act * pre_act) * INV_SQRT_2PI


class Copies:
    def __init__(self, copies):
        self.copies = copies

    def start(self):
        for copy in self.copies:
            copy.start()

    def wait(self):
        for copy in self.copies:
            copy.wait()

    def wait_recv(self):
        for copy in self.copies:
            copy.wait_recv()

    def wait_send(self):
        for copy in self.copies:
            copy.wait_send()


def rows_of(owner, chunk):
    return pl.ds(pl.multiple_of(owner * chunk, chunk), chunk)


def to_sequence(src, dst, send_sem, recv_sem, me, chunk):
    return Copies([remote(src.at[me ^ mask], dst.at[rows_of(me, chunk)], send_sem.at[mask], recv_sem.at[mask], me ^ mask) for mask in (2, 3, 1)])


def from_sequence(src, dst, send_sem, recv_sem, me, chunk):
    return Copies([remote(src.at[rows_of(me ^ mask, chunk)], dst.at[me], send_sem.at[mask], recv_sem.at[mask], me ^ mask) for mask in (2, 3, 1)])


def lane_sum(value):
    return jnp.sum(value, axis=1, keepdims=True)


def forward_kernel(dims, x_ref, wq_ref, bq_ref, mask_ref, b_out_ref, gain2_ref, bias2_ref, b_down_ref, gain1_ref, bias1_ref, b_up_ref, cos_ref, sin_ref, wo_ref, wu_ref, wd_ref, dy_ref,
                   x_out, wq_out, h1_out, q_out, k_out, v_out, o_out, wide_out, lse_out, y_out, h2_out, dx1t_out, dx1b_out, do_out, dy_out, h2_all, dy_cross, sums_ref, vec_ref,
                   x_full, wq_all, h1_ref, q_all, k_all, v_all, o_ref, wide_ref, lse_ref, h1t_ref, bq_all, wo_all, wu_all, wd_all, vec_all, dy_full,
                   act_ref, stage_ref, wide_stage, own_sem, once_sem, store_sem, x_send, x_recv, dy_send, dy_recv, send_sem, recv_sem, wide_send, wide_recv):
    chunk, local_heads, head_dim = dims
    me = lax.axis_index('tp')
    half = head_dim // 2
    seq_len, width = x_full.shape
    tp, ff = wu_all.shape[0], wu_ref.shape[2]
    for i, row in enumerate((b_out_ref, gain2_ref, bias2_ref, b_down_ref, gain1_ref, bias1_ref, b_up_ref, b_up_ref)):
        vec_ref[i:i + 1] = row[...].reshape(1, width)
    greet(me, True)
    x_move = to_sequence(x_ref, x_full, x_send, x_recv, me, chunk)
    dy_move = to_sequence(dy_ref, dy_full, dy_send, dy_recv, me, chunk)
    dy_far = Copies([remote(dy_ref.at[me ^ i], dy_cross.at[i], dy_send.at[4 + i], dy_recv.at[4 + i], me ^ 2) for i in (0, 1)])
    vec_all[0] = vec_ref[...]
    gathered = ((bq_ref, bq_all), (vec_ref, vec_all))
    moves = [Gather(source, dst, 0, send_sem.at[i], recv_sem.at[i], me) for i, (source, dst) in enumerate(gathered)]
    bq, vec = moves
    weights = ((wq_ref, wq_all), (wo_ref, wo_all), (wu_ref, wu_all), (wd_ref, wd_all))
    shared = [SharedGather(source, dst, wide_send.at[i], wide_recv.at[i], me) for i, (source, dst) in enumerate(weights)]
    wq, wo, wu, wd = shared
    own = [pltpu.make_async_copy(source, dst.at[0], own_sem.at[i]) for i, (source, dst) in enumerate(gathered[:1] + weights)]
    x_move.start()
    bq.start()
    wq.start()
    for copy in own:
        copy.start()
    for move in (vec, wo, wu, wd, dy_move, dy_far):
        move.start()
    own_rows = rows_of(me, chunk)
    own_x = pltpu.make_async_copy(x_ref.at[me], x_full.at[own_rows], once_sem.at[0])
    own_dy = pltpu.make_async_copy(dy_ref.at[me], dy_full.at[own_rows], once_sem.at[1])
    own_x.start()
    own_dy.start()
    valid = mask_ref[pl.ds(me, 1)] > 0
    first = lax.broadcasted_iota(jnp.int32, (half, seq_len), 0) == 0
    ones = first.astype(F32).astype(BF16)
    key_bias = jnp.where(first, jnp.where(valid, 0.0, NEG_LARGE), 0.0).astype(BF16)
    for copy in own:
        copy.wait()
    own_x.wait()
    x_move.wait_recv()
    h1, _, _ = layer_norm(x_full[...].astype(F32), vec_all[0, 4:5], vec_all[0, 5:6])
    h1 = h1.astype(BF16)
    h1_ref[...] = h1
    h1t_ref[...] = h1.T
    once = [pltpu.make_async_copy(source, dst, once_sem.at[2 + i]) for i, (source, dst) in enumerate((
        (x_full, x_out), (h1_ref, h1_out), (wq_all, wq_out), (stage_ref.at[0], h2_out), (stage_ref.at[1], y_out), (stage_ref.at[2], dx1b_out), (wide_stage, dx1t_out), (dy_full, dy_out)))]
    once[0].start()
    once[1].start()

    def stores(m):
        heads = pl.ds(m * local_heads, local_heads)
        pairs = ((q_all, q_out), (k_all, k_out), (v_all, v_out), (o_ref, o_out), (wide_ref, wide_out), (lse_ref, lse_out))
        return Copies([pltpu.make_async_copy(source.at[heads], dst.at[heads], store_sem.at[i, m]) for i, (source, dst) in enumerate(pairs)])

    @pl.loop(0, 4)
    def _(m):
        @pl.when(m == 1)
        def _():
            bq.near.wait_recv()
            wq.near.wait_recv()
            bq.forward()
            wq.forward()

        @pl.when(m == 2)
        def _():
            wq.forward_rest()
            vec.forward()
            wo.forward()

        @pl.when(m == 3)
        def _():
            bq.relay.wait_recv()
            wq.relay.wait_recv()
            once[2].start()
            wo.forward_rest()
            wu.forward()
            wd.forward()

        biases = [bq_all[m, j].T for j in range(local_heads)]
        qkv = dot(wq_all[m].reshape(3 * local_heads * head_dim, width), h1t_ref[...])
        cos, sin = cos_ref[...], sin_ref[...]
        group = local_heads * head_dim
        for j in range(local_heads):
            head = m * local_heads + j
            for which, (dst, scale, extra) in enumerate(((q_all, head_dim ** -0.5, ones), (k_all, None, key_bias))):
                rows = qkv[which * group + j * head_dim:which * group + (j + 1) * head_dim] + biases[j][:, which:which + 1]
                rows = rows * scale if scale is not None else rows
                low, high = rows[:half], rows[half:]
                dst[head, :half] = (low * cos - high * sin).astype(BF16)
                dst[head, half:head_dim] = (high * cos + low * sin).astype(BF16)
                dst[head, head_dim:] = extra
            v_all[head] = (qkv[2 * group + j * head_dim:2 * group + (j + 1) * head_dim] + biases[j][:, 2:3]).astype(BF16)

        coming = dot(k_all[m * local_heads].T, q_all[m * local_heads])
        for j in range(local_heads):
            head, scores = m * local_heads + j, coming
            top = jnp.max(scores, axis=0, keepdims=True)
            if j + 1 < local_heads:
                coming = dot(k_all[head + 1].T, q_all[head + 1])
            weights = jnp.exp(scores - top)
            total = jnp.sum(weights, axis=0, keepdims=True)
            out = dot(v_all[head], weights.astype(BF16)) / total
            o_ref[head] = out.astype(BF16)
            wide_ref[head] = out
            lse_ref[head] = top + jnp.log(total)

        stores(m).start()

    wu.forward_rest()
    wd.forward_rest()
    for move in (vec, wo):
        move.near.wait_recv()
        move.relay.wait_recv()
    rows = tp * local_heads * head_dim
    wo_full = wo_all[...].reshape(rows, width)
    cols = vec_all[0].T
    b_out, gain, bias, b_down = (cols[:, i:i + 1] for i in range(4))
    attn = dot_tn(wo_full, o_ref[...].reshape(rows, seq_len))
    x1 = (x_full[...].T.astype(F32) + (attn + b_out)).astype(BF16).astype(F32)
    h2_f, x_hat, inv_std = layer_norm_rows(x1, gain, bias)
    h2 = h2_f.astype(BF16)
    stage_ref[0] = h2.T
    wu.near.wait_recv()
    wu.relay.wait_recv()
    h2_move = Gather(stage_ref.at[0, :h2_all.shape[1]], h2_all, 1, send_sem.at[2], recv_sem.at[2], me)

    def mlp(slope_ref):
        @pl.loop(0, tp)
        def _(m):
            @pl.when(m == 1)
            def _():
                h2_move.start()
                once[3].start()

            pre_act = dot_tn(wu_all[m].reshape(width, ff), h2) + vec_all[m].T[:, 6:7]
            act, slope = gelu(pre_act)
            act_ref[m] = act
            slope_ref[m] = slope

        wd.near.wait_recv()
        wd.relay.wait_recv()
        out = dot_tn(wd_all[...].reshape(tp * ff, width), act_ref[...].reshape(tp * ff, seq_len))
        stage_ref[1] = (x1 + (out + b_down)).astype(BF16).T
        own_dy.wait()
        dy_move.wait_recv()
        once[7].start()
        dy_t = dy_full[...].T
        wide_stage[...] = jnp.zeros_like(wide_stage)

        @pl.loop(0, tp)
        def _(m):
            @pl.when(m == 1)
            def _():
                once[4].start()

            d_pre = (dot(wd_all[m].reshape(ff, width), dy_t) * slope_ref[m]).astype(BF16)
            wide_stage[...] += dot(wu_all[m].reshape(width, ff), d_pre)

    pl.run_scoped(mlp, pltpu.VMEM((tp, ff, seq_len), F32))
    d_h2 = wide_stage[...]
    dy_f = dy_full[...].T.astype(F32)
    d_x1 = dy_f + layer_norm_rows_grad(d_h2, x_hat, inv_std, gain)
    d_x1_b = d_x1.astype(BF16)
    wide_stage[...] = d_x1
    stage_ref[2] = d_x1_b.T
    for m in range(4):
        stores(m).wait()
    o_ref[...] = dot(wo_full, d_x1_b).astype(BF16).reshape(o_ref.shape)
    h2_move.forward()
    once[5].start()
    once[6].start()
    sums = [lane_sum(dy_f), lane_sum(d_h2 * x_hat), lane_sum(d_h2), lane_sum(d_x1)]
    sums_ref[...] = jnp.concatenate(sums + [jnp.zeros((width, 124), F32)], axis=1).T[:8]
    last = pltpu.make_async_copy(o_ref, do_out, once_sem.at[10])
    last.start()
    x_move.wait_send()
    dy_move.wait_send()
    dy_far.wait()
    for move in moves:
        move.near.wait_send()
        move.far.wait_send()
        move.relay.wait_send()
    for move in shared:
        move.wait_send()
    for copy in once:
        copy.wait()
    last.wait()
    h2_move.finish()


def backward_kernel(dims, q_in, k_in, v_in, do_in, wide_in, lse_in, cos_ref, sin_ref, o_in, dx1b_in, h1_in, h2_ref, dy_ref, dy_full, y_ref,
                    wq_in, x_in, dx1t_in, sums_ref, vec_ref, wu_in, wd_in, h2_low, dy_cross,
                    y_out, gwo_ref, gx_ref, gwq_ref, gb_out, sums_out, gwu_ref, gbu_ref, gwd_ref, h2_high, dy_all,
                    dqkv_ref, gb_ref, h1_ref, near_buf, far_buf, near_gwq, far_gwq, near_last, gb_rows, gb_buf, sums_mine, sums_buf, gx_seq,
                    own_sem, load_sem, first_sem, tail_sem, red_send, red_recv, small_send, small_recv, h2_send, h2_recv, dy_send, dy_recv, y_send, y_recv, gx_send, gx_recv):
    local_heads, head_dim = dims
    me = lax.axis_index('tp')
    tp, chunk, width = dy_ref.shape
    half = head_dim // 2
    group = local_heads * head_dim
    rows = 3 * group
    seq_len = tp * chunk
    low_rows = h2_low.shape[1]
    mine, across, partner = rows_of(me, chunk), rows_of(me ^ 2, chunk), me ^ 1
    greet(me)
    h2_move = Gather(h2_ref.at[low_rows:], h2_high, 1, h2_send, h2_recv, me)
    y_move = from_sequence(y_ref, y_out, y_send, y_recv, me, chunk)
    dy_near = Copies([remote(source, dst, dy_send.at[i], dy_recv.at[i], partner) for i, (source, dst) in enumerate((
        (dy_full, dy_all.at[0]), (dy_ref.at[me ^ 2], dy_all.at[2, mine]), (dy_ref.at[me ^ 3], dy_all.at[1, mine])))])
    dy_relay = Copies([remote(dy_cross.at[i], dy_all.at[2 - i, across], dy_send.at[3 + i], dy_recv.at[3 + i], partner) for i in (0, 1)])
    own = Copies([pltpu.make_async_copy(dy_ref.at[me ^ 2], dy_all.at[1, mine], own_sem.at[0]), pltpu.make_async_copy(dy_ref.at[me ^ 3], dy_all.at[2, mine], own_sem.at[1]),
                  pltpu.make_async_copy(y_ref.at[mine], y_out.at[me], own_sem.at[2])]
                 + [pltpu.make_async_copy(dy_cross.at[i], dy_all.at[1 + i, across], own_sem.at[3 + i]) for i in (0, 1)])
    h2_move.start()
    y_move.start()
    dy_near.start()
    dy_relay.start()
    cos, sin = cos_ref[...], sin_ref[...]

    def store(m, j, which, low, high):
        grad = jnp.concatenate([low, high], axis=0)
        at = pl.ds(pl.multiple_of(which * group + j * head_dim, head_dim), head_dim)
        dqkv_ref[m, at] = grad.astype(BF16)
        gb_ref[m, at] = jnp.broadcast_to(lane_sum(grad), (head_dim, 128))

    def back(grad):
        low, high = grad[:half], grad[half:]
        return low * cos + high * sin, high * cos - low * sin

    def attention(q_all, k_all, v_all, do_ref, wide_ref, lse_ref, o_ref, dx1b_ref, part, part_gwq):
        def loads(m):
            heads = pl.ds(m * local_heads, local_heads)
            pairs = ((q_in, q_all), (k_in, k_all), (v_in, v_all), (do_in, do_ref), (wide_in, wide_ref), (lse_in, lse_ref))
            return Copies([pltpu.make_async_copy(source.at[heads], dst.at[heads], load_sem.at[i, m]) for i, (source, dst) in enumerate(pairs)])

        early = Copies([pltpu.make_async_copy(source, dst, first_sem.at[i]) for i, (source, dst) in enumerate(((o_in, o_ref), (dx1b_in, dx1b_ref), (h1_in, h1_ref)))])
        early.start()
        for m in range(tp - 1, -1, -1):
            loads(m).start()
        own.start()
        reduce_near = Copies([remote(part.at[source], near_buf.at[i], red_send.at[i], red_recv.at[i], partner) for i, source in enumerate((1, 3))])
        reduce_far = remote(part.at[2], far_buf, red_send.at[2], red_recv.at[2], me ^ 2)
        gwq_near = remote(part_gwq.at[1], near_gwq, red_send.at[3], red_recv.at[3], partner)
        gwq_far = remote(part_gwq.at[0], far_gwq, red_send.at[4], red_recv.at[4], me ^ 2)
        early.wait()

        @pl.loop(0, tp)
        def _(m):
            heads = pl.ds(m * local_heads, local_heads)
            part[m] = dot(o_ref[heads].reshape(group, seq_len), dx1b_ref[...])

        @pl.loop(0, tp * local_heads)
        def _(step):
            m = tp - 1 - lax.div(step, local_heads)
            j = lax.rem(step, local_heads)
            head = m * local_heads + j

            @pl.when(j == 0)
            def _():
                loads(m).wait()

            @pl.when(step == 1)
            def _():
                reduce_near.start()

            @pl.when(step == 3)
            def _():
                reduce_near.wait()
                part[0] += near_buf[0]
                part[2] += near_buf[1]

            @pl.when(step == 4)
            def _():
                reduce_far.start()

            @pl.when(step == 6)
            def _():
                h2_move.forward()

            @pl.when(step == 10)
            def _():
                @pl.loop(0, 2)
                def _(i):
                    part_gwq[i] = dot(dqkv_ref[2 + i], h1_ref[...])

            @pl.when(step == 11)
            def _():
                gwq_near.start()

            @pl.when(step == 12)
            def _():
                gwq_near.wait()
                part_gwq[0] += near_gwq[...]

            @pl.when(step == 13)
            def _():
                gwq_far.start()

            q, k, v, d_out = q_all[head], k_all[head], v_all[head], do_ref[head]
            delta = jnp.sum(d_out.astype(F32) * wide_ref[head], axis=0, keepdims=True)
            probs = jnp.exp(dot(k.T, q) - lse_ref[head])
            d_probs = dot(v.T, d_out)
            d_scores = (probs * (d_probs - delta)).astype(BF16)
            d_value = dot(probs.astype(BF16), d_out.T).T
            d_key = dot(d_scores, q[:head_dim].T).T
            d_query = dot(k[:head_dim], d_scores)
            low, high = back(d_query)
            scale = head_dim ** -0.5
            store(m, j, 0, low * scale, high * scale)
            low, high = back(d_key)
            store(m, j, 1, low, high)
            store(m, j, 2, d_value[:half], d_value[half:])

        own.wait()
        y_move.wait()
        h2_move.finish()
        dy_near.wait()
        dy_relay.wait()
        reduce_far.wait()
        gwo_ref[...] = part[0] + far_buf[...]
        gwq_far.wait_send()

    heads_all = tp * local_heads

    def vm(array):
        return pltpu.VMEM(array.shape, array.dtype)

    pl.run_scoped(attention, vm(q_in), vm(k_in), vm(v_in), vm(do_in), vm(wide_in), vm(lse_in), vm(o_in), vm(dx1b_in), pltpu.VMEM((tp, group, width), F32), pltpu.VMEM((2, rows, width), F32))

    def tail(wq_ref, x_ref, dx1t_ref, wu_ref, wd_ref, h2_all, dy_full_all, part, acc_up, acc_bias):
        first = [pltpu.make_async_copy(source, dst, tail_sem.at[i]) for i, (source, dst) in enumerate(((wq_in, wq_ref), (x_in, x_ref), (dx1t_in, dx1t_ref), (wu_in, wu_ref), (wd_in, wd_ref)))]
        for m in range(tp):
            if m == 0:
                first.append(pltpu.make_async_copy(h2_ref, h2_all.at[0], tail_sem.at[5]))
                first.append(pltpu.make_async_copy(dy_full, dy_full_all.at[0], tail_sem.at[6]))
            else:
                first.append(pltpu.make_async_copy(h2_low.at[m - 1], h2_all.at[m, :low_rows], tail_sem.at[4 + 3 * m]))
                first.append(pltpu.make_async_copy(h2_high.at[m - 1], h2_all.at[m, low_rows:], tail_sem.at[5 + 3 * m]))
                first.append(pltpu.make_async_copy(dy_all.at[m - 1], dy_full_all.at[m], tail_sem.at[6 + 3 * m]))
        for load in first:
            load.start()
        near = remote(part.at[1], near_last, red_send.at[5], red_recv.at[5], partner)

        @pl.loop(0, 2)
        def _(i):
            part[i] = dot(dqkv_ref[i], h1_ref[...])

        cols = vec_ref[...].T
        gain, bias = cols[:, 4:5], cols[:, 5:6]
        first[0].wait()
        near.start()
        d_h1 = dot_tn(wq_ref[...].reshape(tp * rows, width), dqkv_ref[...].reshape(tp * rows, seq_len))
        for load in first[1:]:
            load.wait()
        _, x_hat, inv_std = layer_norm_rows(x_ref[...].T.astype(F32), gain, bias)
        grad_x = (dx1t_ref[...] + layer_norm_rows_grad(d_h1, x_hat, inv_std, gain)).astype(BF16)
        gx_seq[...] = grad_x.T
        sums = [lane_sum(d_h1 * x_hat), lane_sum(d_h1)]
        ln1 = jnp.concatenate(sums + [jnp.zeros((width, 126), F32)], axis=1).T
        sums_mine[...] = jnp.concatenate([sums_ref[:4], ln1[:4]], axis=0)
        gx_ref[me] = gx_seq[mine]
        for m in range(tp):
            gb_rows[m] = gb_ref[m].T[:8]
        small = [remote(gb_rows.at[m], gb_buf.at[m - 1], small_send.at[0, m], small_recv.at[0, m], me ^ m) for m in (1, 2, 3)]
        small += [remote(sums_mine, sums_buf.at[m - 1], small_send.at[1, m], small_recv.at[1, m], me ^ m) for m in (1, 2, 3)]
        for move in small:
            move.start()
        gx_move = from_sequence(gx_seq, gx_ref, gx_send, gx_recv, me, chunk)
        gx_move.start()
        acc_up[...] = jnp.zeros_like(acc_up)
        acc_bias[...] = jnp.zeros_like(acc_bias)
        gwd_ref[...] = jnp.zeros_like(gwd_ref)
        wu_t = wu_ref[...].T
        bu_col = cols[:, 6:7]

        @pl.loop(0, tp)
        def _(m):
            act, slope = gelu(dot_nt(wu_t, h2_all[m]) + bu_col)
            d_pre = dot_nt(wd_ref[...], dy_full_all[m]) * slope
            lanes = d_pre[:, :128]
            for i in range(1, seq_len // 128):
                lanes = lanes + d_pre[:, i * 128:(i + 1) * 128]
            acc_bias[...] += lanes
            gwd_ref[...] += dot(act, dy_full_all[m])
            acc_up[...] += dot(d_pre.astype(BF16), h2_all[m])

        gwu_ref[...] = acc_up[...].T
        gbu_ref[...] = jnp.broadcast_to(lane_sum(acc_bias[...]), acc_bias.shape).T[:8]
        near.wait()
        remote(part.at[0], far_gwq, red_send.at[4], red_recv.at[4], me ^ 2).wait_recv()
        gwq_ref[...] = part[0] + near_last[...] + far_gwq[...]
        for move in small:
            move.wait()
        gb_out[...] = gb_rows[0] + gb_buf[0] + (gb_buf[1] + gb_buf[2])
        sums_out[...] = sums_mine[...] + sums_buf[0] + (sums_buf[1] + sums_buf[2])
        gx_move.wait()

    pl.run_scoped(tail, vm(wq_in), vm(x_in), vm(dx1t_in), vm(wu_in), vm(wd_in), pltpu.VMEM((tp, seq_len, width), BF16), pltpu.VMEM((tp, seq_len, width), BF16),
                  pltpu.VMEM((2, rows, width), F32), pltpu.VMEM((wd_in.shape[0], width), F32), pltpu.VMEM((wd_in.shape[0], 128), F32))


def finish_kernel(*refs):
    moved, small = refs[:6], refs[6:9]
    outs, vectors, bias_up, bias_qkv = refs[9:15], refs[15:21], refs[21], refs[22]
    bufs, load_sem, store_sem = refs[23:29], refs[29], refs[30]
    loads = [pltpu.make_async_copy(source, buf, load_sem.at[i]) for i, (source, buf) in enumerate(zip(moved, bufs))]
    stores = [pltpu.make_async_copy(buf, dst, store_sem.at[i]) for i, (buf, dst) in enumerate(zip(bufs, outs))]
    for load in loads:
        load.start()
    for load, store in zip(loads, stores):
        load.wait()
        store.start()
    sums, grad_up, grad_qkv = small
    for i, vector in enumerate(vectors):
        vector[...] = sums[i]
    bias_up[...] = grad_up[0]
    heads, kinds, head_dim = bias_qkv.shape
    row = grad_qkv[:1]
    for j in range(heads):
        for which in range(kinds):
            at = (which * heads + j) * head_dim
            bias_qkv[j, which:which + 1] = row[:, at:at + head_dim]
    for store in stores:
        store.wait()


VMEM_SPEC = pl.BlockSpec(memory_space=pltpu.VMEM)
ANY_SPEC = pl.BlockSpec(memory_space=pl.ANY)


def shape(dims, dtype=BF16):
    return jax.ShapeDtypeStruct(dims, dtype)


def single_call(kernel, name, collective_id, ins, in_any, outs, out_any, scratch, limit=67043328):
    dma = pltpu.SemaphoreType.DMA
    return pl.pallas_call(
        kernel,
        out_shape=outs,
        in_specs=[ANY_SPEC if i in in_any else VMEM_SPEC for i in range(len(ins))],
        out_specs=[ANY_SPEC if i in out_any else VMEM_SPEC for i in range(len(outs))],
        scratch_shapes=[dma(s) if isinstance(s, tuple) else pltpu.VMEM(s.shape, s.dtype) for s in scratch],
        compiler_params=pltpu.CompilerParams(collective_id=collective_id, has_side_effects=collective_id is not None, vmem_limit_bytes=limit),
        name=name,
    )(*ins)


def solution(mesh):
    tp = mesh.shape['tp']
    act_spec = P('dp', 'tp', None)
    rep_vec = P(None)
    part_vec = P('dp')
    in_specs = (act_spec, act_spec, P('dp', None), rep_vec, rep_vec, P(None, None, 'tp', None), P(None, 'tp', None),
                P('tp', None, None), rep_vec, rep_vec, rep_vec, P(None, 'tp'), P('tp'), P('tp', None), rep_vec)
    out_specs = (act_spec, act_spec, part_vec, part_vec, P('dp', None, 'tp', None), P('dp', 'tp', None),
                 P(('dp', 'tp'), None, None), part_vec, part_vec, part_vec, P('dp', 'tp'), P(('dp', 'tp')),
                 P(('dp', 'tp'), None), part_vec)

    def device_step(x_in, grad_y, pad_mask, ln1_gain, ln1_bias, w_qkv, b_qkv, w_out, b_out, ln2_gain, ln2_bias, w_up, b_up, w_down, b_down):
        seq_len = pad_mask.shape[1]
        local_heads, head_dim = w_qkv.shape[2:]
        chunk, width = x_in.shape[1:]
        ff = w_up.shape[1]
        heads = local_heads * tp
        group = local_heads * head_dim
        qkv_rows = 3 * group
        ext = head_dim + head_dim // 2
        low_rows = seq_len // 4
        dims = (local_heads, head_dim)
        cos_tab, sin_tab = (jnp.asarray(table) for table in rope_tables(seq_len, head_dim))
        wq_own = w_qkv.transpose(0, 2, 3, 1).reshape(2, qkv_rows // 2, width)
        bq_own = b_qkv.transpose(1, 0, 2)
        wo_own = w_out.reshape(2, group // 2, width)
        wu_own = w_up.reshape(2, width // 2, ff)
        wd_own = w_down.reshape(2, ff // 2, width)
        act = shape((seq_len, width))
        by_head = shape((heads, head_dim, seq_len))
        ext_head = shape((heads, ext, seq_len))
        held = [act, shape((tp,) + wq_own.shape), act, ext_head, ext_head, by_head, by_head, shape(by_head.shape, F32), shape((heads, 1, seq_len), F32)]
        d_x1_t = shape((width, seq_len), F32)
        rows8 = shape((8, width), F32)
        ins = (x_in, wq_own, bq_own, pad_mask, b_out, ln2_gain, ln2_bias, b_down, ln1_gain, ln1_bias, b_up, cos_tab, sin_tab, wo_own, wu_own, wd_own, grad_y)
        outs = held + [act, act, d_x1_t, act, by_head, act, shape((tp - 1, low_rows, width)), shape((2, chunk, width)), rows8, rows8]
        scratch = held + [shape((width, seq_len)), shape((tp,) + bq_own.shape, F32), shape((tp,) + wo_own.shape), shape((tp,) + wu_own.shape), shape((tp,) + wd_own.shape), shape((tp,) + rows8.shape, F32), act,
                          shape((tp, ff, seq_len)), shape((3, seq_len, width)), d_x1_t, (5,), (11,), (6, 4), (4,), (4,), (6,), (6,), (3, 3), (3, 3), (4, 5), (4, 5)]
        (x_full, wq_all, h1, q_ext, k_ext, v_heads, attn_o, attn_wide, lse, y_seq, h2, dx1_t, dx1_b, d_o, dy_full, h2_low, dy_cross, mid_sums, vec) = single_call(
            functools.partial(forward_kernel, (chunk,) + dims), 'forward', 0, ins, (0, 1, 2, 13, 14, 15, 16), outs, range(17), scratch)
        ins = (q_ext, k_ext, v_heads, d_o, attn_wide, lse, cos_tab, sin_tab, attn_o, dx1_b, h1, h2, grad_y, dy_full, y_seq, wq_all.reshape(tp, qkv_rows, width), x_full, dx1_t, mid_sums, vec, w_up, w_down, h2_low, dy_cross)
        gwq = shape((qkv_rows, width), F32)
        gwo = shape((group, width), F32)
        outs = [shape((tp, chunk, width)), gwo, shape((tp, chunk, width)), gwq, shape((8, qkv_rows), F32), rows8, shape(w_up.shape, F32), shape((8, ff), F32), shape(w_down.shape, F32),
                shape((tp - 1, seq_len - low_rows, width)), shape((tp - 1, seq_len, width))]
        scratch = [shape((tp, qkv_rows, seq_len)), shape((tp, qkv_rows, 128), F32), act, shape((2, group, width), F32), gwo, gwq, gwq, gwq, shape((tp, 8, qkv_rows), F32), shape((3, 8, qkv_rows), F32), rows8, shape((3, 8, width), F32), act,
                   (5,), (6, 4), (3,), (16,), (6,), (6,), (2, 4), (2, 4), (3,), (3,), (5,), (5,), (4,), (4,), (4,), (4,)]
        y_out, grad_w_out, grad_x, grad_w_qkv, grad_b_qkv, sums, grad_w_up, grad_b_up, grad_w_down, _, _ = single_call(
            functools.partial(backward_kernel, dims), 'backward', 1, ins, (0, 1, 2, 3, 4, 5, 8, 9, 10, 11, 12, 13, 14, 15, 16, 17, 20, 21, 22, 23), outs, (0, 9, 10), scratch)
        moved = (y_out, grad_x, grad_w_qkv, grad_w_out, grad_w_up, grad_w_down)
        ins = moved + (sums, grad_b_up, grad_b_qkv)
        vector = shape((width,), F32)
        moved_shapes = [shape(a.shape, a.dtype) for a in moved]
        outs = moved_shapes + [vector] * 6 + [shape((ff,), F32), shape((local_heads, 3, head_dim), F32)]
        y_out, grad_x, grad_w_qkv, grad_w_out, grad_w_up, grad_w_down, *vectors, grad_b_up, grad_b_qkv = single_call(
            finish_kernel, 'finish', None, ins, range(6), outs, range(6), moved_shapes + [(6,), (6,)])
        grad_w_qkv = grad_w_qkv.reshape(3, local_heads, head_dim, width).transpose(0, 3, 1, 2)
        grad_b_qkv = grad_b_qkv.transpose(1, 0, 2)
        grad_w_out = grad_w_out.reshape(local_heads, head_dim, width)
        return (y_out, grad_x, vectors[4], vectors[5], grad_w_qkv, grad_b_qkv, grad_w_out, vectors[3],
                vectors[1], vectors[2], grad_w_up, grad_b_up, grad_w_down, vectors[0])

    return jax.shard_map(device_step, mesh=mesh, in_specs=in_specs, out_specs=out_specs, check_vma=False)
```

```python
import functools

import jax
import jax.numpy as jnp
import numpy as np
from jax import lax
from jax.experimental import pallas as pl
from jax.experimental.pallas import tpu as pltpu
from jax.sharding import PartitionSpec as P

LN_EPS = 1e-5
ROPE_BASE = 10000.0
INV_SQRT2 = 0.7071067811865476
INV_SQRT_2PI = 0.3989422804014327
NEG_LARGE = -1e30
F32 = jnp.float32
BF16 = jnp.bfloat16
MESH = pl.DeviceIdType.MESH


def dot(lhs, rhs):
    return jnp.dot(lhs, rhs, preferred_element_type=F32)


def layer_norm(values, ln_gain, ln_bias):
    centered = values - jnp.mean(values, axis=-1, keepdims=True)
    inv_std = lax.rsqrt(jnp.mean(centered * centered, axis=-1, keepdims=True) + LN_EPS)
    x_hat = centered * inv_std
    return x_hat * ln_gain + ln_bias, x_hat, inv_std


def rope_tables(seq_len, head_dim):
    half_dim = head_dim // 2
    inv_freq = np.float32(ROPE_BASE) ** (np.float32(-2.0) * np.arange(half_dim, dtype=np.float32) / np.float32(head_dim))
    angles = inv_freq[:, None] * np.arange(seq_len, dtype=np.float32)[None, :]
    return np.cos(angles), np.sin(angles)


def remote(src, dst, send_sem, recv_sem, device):
    return pltpu.make_async_remote_copy(src_ref=src, dst_ref=dst, send_sem=send_sem, recv_sem=recv_sem, device_id={'tp': device}, device_id_type=MESH)


def greet(me, groups=False):
    barrier = pltpu.get_barrier_semaphore()
    for mask in (1, 2, 3):
        pl.semaphore_signal(barrier, inc=1, device_id={'tp': me ^ mask}, device_id_type=MESH)
    if groups:
        pl.semaphore_signal(barrier, inc=1, device_id={'dp': lax.axis_index('dp') ^ 1}, device_id_type=MESH)
    pl.semaphore_wait(barrier, 4 if groups else 3)


class Gather:
    def __init__(self, src, dst, base, send_sem, recv_sem, me):
        self.near = remote(src, dst.at[1 - base], send_sem.at[0], recv_sem.at[0], me ^ 1)
        self.far = remote(src, dst.at[2 - base], send_sem.at[1], recv_sem.at[1], me ^ 2)
        self.relay = remote(dst.at[2 - base], dst.at[3 - base], send_sem.at[2], recv_sem.at[2], me ^ 1)

    def start(self):
        self.far.start()
        self.near.start()

    def forward(self):
        self.far.wait_recv()
        self.relay.start()

    def finish(self):
        self.near.wait()
        self.far.wait_send()
        self.relay.wait()


class SharedGather:
    def __init__(self, src, dst, send_sem, recv_sem, me):
        group = lax.axis_index('dp')
        half, rest = group, group ^ 1
        self.near = remote(src, dst.at[1], send_sem.at[0], recv_sem.at[0], me ^ 1)
        self.far = remote(src.at[half], dst.at[2, half], send_sem.at[1], recv_sem.at[1], me ^ 2)
        self.side = pltpu.make_async_remote_copy(src_ref=dst.at[2, half], dst_ref=dst.at[2, half], send_sem=send_sem.at[2], recv_sem=recv_sem.at[2], device_id={'dp': rest}, device_id_type=MESH)
        self.relay = Copies([remote(dst.at[2, part], dst.at[3, part], send_sem.at[3 + i], recv_sem.at[3 + i], me ^ 1) for i, part in enumerate((half, rest))])

    def start(self):
        self.far.start()
        self.near.start()

    def forward(self):
        self.far.wait_recv()
        self.side.start()
        self.relay.copies[0].start()

    def forward_rest(self):
        self.side.wait_recv()
        self.relay.copies[1].start()

    def wait_send(self):
        for copy in (self.near, self.far, self.side, self.relay):
            copy.wait_send()


def layer_norm_rows(values, ln_gain, ln_bias):
    centered = values - jnp.mean(values, axis=0, keepdims=True)
    inv_std = lax.rsqrt(jnp.mean(centered * centered, axis=0, keepdims=True) + LN_EPS)
    x_hat = centered * inv_std
    return x_hat * ln_gain + ln_bias, x_hat, inv_std


def layer_norm_rows_grad(d_out, x_hat, inv_std, ln_gain):
    d_hat = d_out * ln_gain
    return inv_std * (d_hat - jnp.mean(d_hat, axis=0, keepdims=True) - x_hat * jnp.mean(d_hat * x_hat, axis=0, keepdims=True))


def dot_tn(lhs, rhs):
    return lax.dot_general(lhs, rhs, (((0,), (0,)), ((), ())), preferred_element_type=F32)


def dot_nt(lhs, rhs):
    return lax.dot_general(lhs, rhs, (((1,), (1,)), ((), ())), preferred_element_type=F32)


def gelu(pre_act):
    half_erf = 0.5 * (1.0 + lax.erf(pre_act * INV_SQRT2))
    act = (pre_act * half_erf).astype(BF16)
    return act, half_erf + pre_act * jnp.exp(-0.5 * pre_act * pre_act) * INV_SQRT_2PI


class Copies:
    def __init__(self, copies):
        self.copies = copies

    def start(self):
        for copy in self.copies:
            copy.start()

    def wait(self):
        for copy in self.copies:
            copy.wait()

    def wait_recv(self):
        for copy in self.copies:
            copy.wait_recv()

    def wait_send(self):
        for copy in self.copies:
            copy.wait_send()


def rows_of(owner, chunk):
    return pl.ds(pl.multiple_of(owner * chunk, chunk), chunk)


def to_sequence(src, dst, send_sem, recv_sem, me, chunk):
    return Copies([remote(src.at[me ^ mask], dst.at[rows_of(me, chunk)], send_sem.at[mask], recv_sem.at[mask], me ^ mask) for mask in (2, 3, 1)])


def from_sequence(src, dst, send_sem, recv_sem, me, chunk):
    return Copies([remote(src.at[rows_of(me ^ mask, chunk)], dst.at[me], send_sem.at[mask], recv_sem.at[mask], me ^ mask) for mask in (2, 3, 1)])


def lane_sum(value):
    return jnp.sum(value, axis=1, keepdims=True)


def forward_kernel(dims, x_ref, wq_ref, bq_ref, mask_ref, b_out_ref, gain2_ref, bias2_ref, b_down_ref, gain1_ref, bias1_ref, b_up_ref, cos_ref, sin_ref, wo_ref, wu_ref, wd_ref, dy_ref,
                   x_out, wq_out, h1_out, q_out, k_out, v_out, o_out, wide_out, lse_out, y_out, h2_out, dx1t_out, dx1b_out, do_out, dy_out, h2_all, dy_cross, sums_ref, vec_ref,
                   x_full, wq_all, h1_ref, q_all, k_all, v_all, o_ref, wide_ref, lse_ref, h1t_ref, bq_all, wo_all, wu_all, wd_all, vec_all, dy_full,
                   act_ref, stage_ref, wide_stage, own_sem, once_sem, store_sem, x_send, x_recv, dy_send, dy_recv, send_sem, recv_sem, wide_send, wide_recv):
    chunk, local_heads, head_dim = dims
    me = lax.axis_index('tp')
    half = head_dim // 2
    seq_len, width = x_full.shape
    tp, ff = wu_all.shape[0], wu_ref.shape[2]
    for i, row in enumerate((b_out_ref, gain2_ref, bias2_ref, b_down_ref, gain1_ref, bias1_ref, b_up_ref, b_up_ref)):
        vec_ref[i:i + 1] = row[...].reshape(1, width)
    greet(me, True)
    x_move = to_sequence(x_ref, x_full, x_send, x_recv, me, chunk)
    dy_move = to_sequence(dy_ref, dy_full, dy_send, dy_recv, me, chunk)
    dy_far = Copies([remote(dy_ref.at[me ^ i], dy_cross.at[i], dy_send.at[4 + i], dy_recv.at[4 + i], me ^ 2) for i in (0, 1)])
    vec_all[0] = vec_ref[...]
    gathered = ((bq_ref, bq_all), (vec_ref, vec_all))
    moves = [Gather(source, dst, 0, send_sem.at[i], recv_sem.at[i], me) for i, (source, dst) in enumerate(gathered)]
    bq, vec = moves
    weights = ((wq_ref, wq_all), (wo_ref, wo_all), (wu_ref, wu_all), (wd_ref, wd_all))
    shared = [SharedGather(source, dst, wide_send.at[i], wide_recv.at[i], me) for i, (source, dst) in enumerate(weights)]
    wq, wo, wu, wd = shared
    own = [pltpu.make_async_copy(source, dst.at[0], own_sem.at[i]) for i, (source, dst) in enumerate(gathered[:1] + weights)]
    x_move.start()
    bq.start()
    wq.start()
    for copy in own:
        copy.start()
    vec.start()
    wo.start()
    own_rows = rows_of(me, chunk)
    own_x = pltpu.make_async_copy(x_ref.at[me], x_full.at[own_rows], once_sem.at[0])
    own_dy = pltpu.make_async_copy(dy_ref.at[me], dy_full.at[own_rows], once_sem.at[1])
    own_x.start()
    own_dy.start()
    valid = mask_ref[pl.ds(me, 1)] > 0
    first = lax.broadcasted_iota(jnp.int32, (half, seq_len), 0) == 0
    ones = first.astype(F32).astype(BF16)
    key_bias = jnp.where(first, jnp.where(valid, 0.0, NEG_LARGE), 0.0).astype(BF16)
    for copy in own:
        copy.wait()
    own_x.wait()
    x_move.wait_recv()
    for move in (wu, wd, dy_move, dy_far):
        move.start()
    h1, _, _ = layer_norm(x_full[...].astype(F32), vec_all[0, 4:5], vec_all[0, 5:6])
    h1 = h1.astype(BF16)
    h1_ref[...] = h1
    h1t_ref[...] = h1.T
    once = [pltpu.make_async_copy(source, dst, once_sem.at[2 + i]) for i, (source, dst) in enumerate((
        (x_full, x_out), (h1_ref, h1_out), (wq_all, wq_out), (stage_ref.at[0], h2_out), (stage_ref.at[1], y_out), (stage_ref.at[2], dx1b_out), (wide_stage, dx1t_out), (dy_full, dy_out)))]
    once[0].start()
    once[1].start()

    def stores(m):
        heads = pl.ds(m * local_heads, local_heads)
        pairs = ((q_all, q_out), (k_all, k_out), (v_all, v_out), (o_ref, o_out), (wide_ref, wide_out), (lse_ref, lse_out))
        return Copies([pltpu.make_async_copy(source.at[heads], dst.at[heads], store_sem.at[i, m]) for i, (source, dst) in enumerate(pairs)])

    @pl.loop(0, 4)
    def _(m):
        @pl.when(m == 1)
        def _():
            bq.near.wait_recv()
            wq.near.wait_recv()
            bq.forward()
            wq.forward()

        @pl.when(m == 2)
        def _():
            wq.forward_rest()
            vec.forward()
            wo.forward()
            wu.forward()

        @pl.when(m == 3)
        def _():
            bq.relay.wait_recv()
            wq.relay.wait_recv()
            once[2].start()
            wo.forward_rest()
            wd.forward()

        biases = [bq_all[m, j].T for j in range(local_heads)]
        qkv = dot(wq_all[m].reshape(3 * local_heads * head_dim, width), h1t_ref[...])
        cos, sin = cos_ref[...], sin_ref[...]
        group = local_heads * head_dim
        for j in range(local_heads):
            head = m * local_heads + j
            for which, (dst, scale, extra) in enumerate(((q_all, head_dim ** -0.5, ones), (k_all, None, key_bias))):
                rows = qkv[which * group + j * head_dim:which * group + (j + 1) * head_dim] + biases[j][:, which:which + 1]
                rows = rows * scale if scale is not None else rows
                low, high = rows[:half], rows[half:]
                dst[head, :half] = (low * cos - high * sin).astype(BF16)
                dst[head, half:head_dim] = (high * cos + low * sin).astype(BF16)
                dst[head, head_dim:] = extra
            v_all[head] = (qkv[2 * group + j * head_dim:2 * group + (j + 1) * head_dim] + biases[j][:, 2:3]).astype(BF16)

        coming = dot(k_all[m * local_heads].T, q_all[m * local_heads])
        for j in range(local_heads):
            head, scores = m * local_heads + j, coming
            top = jnp.max(scores, axis=0, keepdims=True)
            if j + 1 < local_heads:
                coming = dot(k_all[head + 1].T, q_all[head + 1])
            weights = jnp.exp(scores - top)
            total = jnp.sum(weights, axis=0, keepdims=True)
            out = dot(v_all[head], weights.astype(BF16)) / total
            o_ref[head] = out.astype(BF16)
            wide_ref[head] = out
            lse_ref[head] = top + jnp.log(total)

        stores(m).start()

    wu.forward_rest()
    for move in (vec, wo):
        move.near.wait_recv()
        move.relay.wait_recv()
    rows = tp * local_heads * head_dim
    wo_full = wo_all[...].reshape(rows, width)
    cols = vec_all[0].T
    b_out, gain, bias, b_down = (cols[:, i:i + 1] for i in range(4))
    attn = dot_tn(wo_full, o_ref[...].reshape(rows, seq_len))
    x1 = (x_full[...].T.astype(F32) + (attn + b_out)).astype(BF16).astype(F32)
    h2_f, x_hat, inv_std = layer_norm_rows(x1, gain, bias)
    h2 = h2_f.astype(BF16)
    stage_ref[0] = h2.T
    wu.near.wait_recv()
    wu.relay.wait_recv()
    h2_move = Gather(stage_ref.at[0, :h2_all.shape[1]], h2_all, 1, send_sem.at[2], recv_sem.at[2], me)

    def mlp(slope_ref):
        @pl.loop(0, tp)
        def _(m):
            @pl.when(m == 1)
            def _():
                wd.forward_rest()
                h2_move.start()
                once[3].start()

            pre_act = dot_tn(wu_all[m].reshape(width, ff), h2) + vec_all[m].T[:, 6:7]
            act, slope = gelu(pre_act)
            act_ref[m] = act
            slope_ref[m] = slope

        wd.near.wait_recv()
        wd.relay.wait_recv()
        out = dot_tn(wd_all[...].reshape(tp * ff, width), act_ref[...].reshape(tp * ff, seq_len))
        stage_ref[1] = (x1 + (out + b_down)).astype(BF16).T
        own_dy.wait()
        dy_move.wait_recv()
        once[7].start()
        dy_t = dy_full[...].T
        wide_stage[...] = jnp.zeros_like(wide_stage)

        @pl.loop(0, tp)
        def _(m):
            @pl.when(m == 1)
            def _():
                once[4].start()

            d_pre = (dot(wd_all[m].reshape(ff, width), dy_t) * slope_ref[m]).astype(BF16)
            wide_stage[...] += dot(wu_all[m].reshape(width, ff), d_pre)

    pl.run_scoped(mlp, pltpu.VMEM((tp, ff, seq_len), F32))
    d_h2 = wide_stage[...]
    dy_f = dy_full[...].T.astype(F32)
    d_x1 = dy_f + layer_norm_rows_grad(d_h2, x_hat, inv_std, gain)
    d_x1_b = d_x1.astype(BF16)
    wide_stage[...] = d_x1
    stage_ref[2] = d_x1_b.T
    for m in range(4):
        stores(m).wait()
    o_ref[...] = dot(wo_full, d_x1_b).astype(BF16).reshape(o_ref.shape)
    h2_move.forward()
    once[5].start()
    once[6].start()
    sums = [lane_sum(dy_f), lane_sum(d_h2 * x_hat), lane_sum(d_h2), lane_sum(d_x1)]
    sums_ref[...] = jnp.concatenate(sums + [jnp.zeros((width, 124), F32)], axis=1).T[:8]
    last = pltpu.make_async_copy(o_ref, do_out, once_sem.at[10])
    last.start()
    x_move.wait_send()
    dy_move.wait_send()
    dy_far.wait()
    for move in moves:
        move.near.wait_send()
        move.far.wait_send()
        move.relay.wait_send()
    for move in shared:
        move.wait_send()
    for copy in once:
        copy.wait()
    last.wait()
    h2_move.finish()


def backward_kernel(dims, q_in, k_in, v_in, do_in, wide_in, lse_in, cos_ref, sin_ref, o_in, dx1b_in, h1_in, h2_ref, dy_ref, dy_full, y_ref,
                    wq_in, x_in, dx1t_in, sums_ref, vec_ref, wu_in, wd_in, h2_low, dy_cross,
                    y_out, gwo_ref, gx_ref, gwq_ref, gb_out, sums_out, gwu_ref, gbu_ref, gwd_ref, h2_high, dy_all,
                    dqkv_ref, gb_ref, h1_ref, near_buf, far_buf, near_gwq, far_gwq, near_last, part_gwq, gb_rows, gb_buf, sums_mine, sums_buf, gx_seq,
                    own_sem, load_sem, first_sem, tail_sem, red_send, red_recv, small_send, small_recv, h2_send, h2_recv, dy_send, dy_recv, y_send, y_recv, gx_send, gx_recv):
    local_heads, head_dim = dims
    me = lax.axis_index('tp')
    tp, chunk, width = dy_ref.shape
    half = head_dim // 2
    group = local_heads * head_dim
    rows = 3 * group
    seq_len = tp * chunk
    low_rows = h2_low.shape[1]
    mine, across, partner = rows_of(me, chunk), rows_of(me ^ 2, chunk), me ^ 1
    greet(me)
    h2_move = Gather(h2_ref.at[low_rows:], h2_high, 1, h2_send, h2_recv, me)
    y_move = from_sequence(y_ref, y_out, y_send, y_recv, me, chunk)
    dy_near = Copies([remote(source, dst, dy_send.at[i], dy_recv.at[i], partner) for i, (source, dst) in enumerate((
        (dy_full, dy_all.at[0]), (dy_ref.at[me ^ 2], dy_all.at[2, mine]), (dy_ref.at[me ^ 3], dy_all.at[1, mine])))])
    dy_relay = Copies([remote(dy_cross.at[i], dy_all.at[2 - i, across], dy_send.at[3 + i], dy_recv.at[3 + i], partner) for i in (0, 1)])
    own = Copies([pltpu.make_async_copy(dy_ref.at[me ^ 2], dy_all.at[1, mine], own_sem.at[0]), pltpu.make_async_copy(dy_ref.at[me ^ 3], dy_all.at[2, mine], own_sem.at[1]),
                  pltpu.make_async_copy(y_ref.at[mine], y_out.at[me], own_sem.at[2])]
                 + [pltpu.make_async_copy(dy_cross.at[i], dy_all.at[1 + i, across], own_sem.at[3 + i]) for i in (0, 1)])
    h2_move.start()
    y_move.start()
    dy_near.start()
    dy_relay.start()
    cos, sin = cos_ref[...], sin_ref[...]

    def store(m, j, which, low, high):
        grad = jnp.concatenate([low, high], axis=0)
        at = pl.ds(pl.multiple_of(which * group + j * head_dim, head_dim), head_dim)
        dqkv_ref[m, at] = grad.astype(BF16)
        gb_ref[m, at] = jnp.broadcast_to(lane_sum(grad), (head_dim, 128))

    def back(grad):
        low, high = grad[:half], grad[half:]
        return low * cos + high * sin, high * cos - low * sin

    def attention(q_all, k_all, v_all, do_ref, wide_ref, lse_ref, o_ref, dx1b_ref, part):
        def loads(m):
            heads = pl.ds(m * local_heads, local_heads)
            pairs = ((q_in, q_all), (k_in, k_all), (v_in, v_all), (do_in, do_ref), (wide_in, wide_ref), (lse_in, lse_ref))
            return Copies([pltpu.make_async_copy(source.at[heads], dst.at[heads], load_sem.at[i, m]) for i, (source, dst) in enumerate(pairs)])

        early = Copies([pltpu.make_async_copy(source, dst, first_sem.at[i]) for i, (source, dst) in enumerate(((o_in, o_ref), (dx1b_in, dx1b_ref), (h1_in, h1_ref)))])
        early.start()
        for m in range(tp - 1, -1, -1):
            loads(m).start()
        own.start()
        reduce_near = Copies([remote(part.at[source], near_buf.at[i], red_send.at[i], red_recv.at[i], partner) for i, source in enumerate((1, 3))])
        reduce_far = remote(part.at[2], far_buf, red_send.at[2], red_recv.at[2], me ^ 2)
        gwq_near = remote(part_gwq.at[1], near_gwq, red_send.at[3], red_recv.at[3], partner)
        gwq_far = remote(part_gwq.at[0], far_gwq, red_send.at[4], red_recv.at[4], me ^ 2)
        early.wait()

        @pl.loop(0, tp)
        def _(m):
            heads = pl.ds(m * local_heads, local_heads)
            part[m] = dot(o_ref[heads].reshape(group, seq_len), dx1b_ref[...])

        @pl.loop(0, tp * local_heads)
        def _(step):
            m = tp - 1 - lax.div(step, local_heads)
            j = lax.rem(step, local_heads)
            head = m * local_heads + j

            @pl.when(j == 0)
            def _():
                loads(m).wait()

            @pl.when(step == 1)
            def _():
                reduce_near.start()

            @pl.when(step == 3)
            def _():
                reduce_near.wait()
                part[0] += near_buf[0]
                part[2] += near_buf[1]

            @pl.when(step == 4)
            def _():
                reduce_far.start()

            @pl.when(step == 9)
            def _():
                h2_move.forward()

            @pl.when(step == 10)
            def _():
                @pl.loop(0, 2)
                def _(i):
                    part_gwq[i] = dot(dqkv_ref[2 + i], h1_ref[...])

            @pl.when(step == 11)
            def _():
                gwq_near.start()

            @pl.when(step == 12)
            def _():
                gwq_near.wait()
                part_gwq[0] += near_gwq[...]

            @pl.when(step == 13)
            def _():
                gwq_far.start()

            q, k, v, d_out = q_all[head], k_all[head], v_all[head], do_ref[head]
            delta = jnp.sum(d_out.astype(F32) * wide_ref[head], axis=0, keepdims=True)
            probs = jnp.exp(dot(k.T, q) - lse_ref[head])
            d_probs = dot(v.T, d_out)
            d_scores = (probs * (d_probs - delta)).astype(BF16)
            d_value = dot(probs.astype(BF16), d_out.T).T
            d_key = dot(d_scores, q[:head_dim].T).T
            d_query = dot(k[:head_dim], d_scores)
            low, high = back(d_query)
            scale = head_dim ** -0.5
            store(m, j, 0, low * scale, high * scale)
            low, high = back(d_key)
            store(m, j, 1, low, high)
            store(m, j, 2, d_value[:half], d_value[half:])

        own.wait()
        y_move.wait()
        h2_move.finish()
        dy_near.wait()
        dy_relay.wait()
        reduce_far.wait()
        gwo_ref[...] = part[0] + far_buf[...]

    heads_all = tp * local_heads

    def vm(array):
        return pltpu.VMEM(array.shape, array.dtype)

    pl.run_scoped(attention, vm(q_in), vm(k_in), vm(v_in), vm(do_in), vm(wide_in), vm(lse_in), vm(o_in), vm(dx1b_in), pltpu.VMEM((tp, group, width), F32))

    def tail(wq_ref, x_ref, dx1t_ref, wu_ref, wd_ref, h2_all, dy_full_all, part, acc_up, acc_bias):
        first = [pltpu.make_async_copy(source, dst, tail_sem.at[i]) for i, (source, dst) in enumerate(((wq_in, wq_ref), (x_in, x_ref), (dx1t_in, dx1t_ref), (wu_in, wu_ref), (wd_in, wd_ref)))]
        for m in range(tp):
            if m == 0:
                first.append(pltpu.make_async_copy(h2_ref, h2_all.at[0], tail_sem.at[5]))
                first.append(pltpu.make_async_copy(dy_full, dy_full_all.at[0], tail_sem.at[6]))
            else:
                first.append(pltpu.make_async_copy(h2_low.at[m - 1], h2_all.at[m, :low_rows], tail_sem.at[4 + 3 * m]))
                first.append(pltpu.make_async_copy(h2_high.at[m - 1], h2_all.at[m, low_rows:], tail_sem.at[5 + 3 * m]))
                first.append(pltpu.make_async_copy(dy_all.at[m - 1], dy_full_all.at[m], tail_sem.at[6 + 3 * m]))
        for load in first:
            load.start()
        near = remote(part.at[1], near_last, red_send.at[5], red_recv.at[5], partner)

        @pl.loop(0, 2)
        def _(i):
            part[i] = dot(dqkv_ref[i], h1_ref[...])

        cols = vec_ref[...].T
        gain, bias = cols[:, 4:5], cols[:, 5:6]
        first[0].wait()
        near.start()
        d_h1 = dot_tn(wq_ref[...].reshape(tp * rows, width), dqkv_ref[...].reshape(tp * rows, seq_len))
        for load in first[1:]:
            load.wait()
        _, x_hat, inv_std = layer_norm_rows(x_ref[...].T.astype(F32), gain, bias)
        grad_x = (dx1t_ref[...] + layer_norm_rows_grad(d_h1, x_hat, inv_std, gain)).astype(BF16)
        gx_seq[...] = grad_x.T
        sums = [lane_sum(d_h1 * x_hat), lane_sum(d_h1)]
        ln1 = jnp.concatenate(sums + [jnp.zeros((width, 126), F32)], axis=1).T
        sums_mine[...] = jnp.concatenate([sums_ref[:4], ln1[:4]], axis=0)
        gx_ref[me] = gx_seq[mine]
        for m in range(tp):
            gb_rows[m] = gb_ref[m].T[:8]
        small = [remote(gb_rows.at[m], gb_buf.at[m - 1], small_send.at[0, m], small_recv.at[0, m], me ^ m) for m in (1, 2, 3)]
        small += [remote(sums_mine, sums_buf.at[m - 1], small_send.at[1, m], small_recv.at[1, m], me ^ m) for m in (1, 2, 3)]
        for move in small:
            move.start()
        gx_move = from_sequence(gx_seq, gx_ref, gx_send, gx_recv, me, chunk)
        gx_move.start()
        acc_up[...] = jnp.zeros_like(acc_up)
        acc_bias[...] = jnp.zeros_like(acc_bias)
        gwd_ref[...] = jnp.zeros_like(gwd_ref)
        wu_t = wu_ref[...].T
        bu_col = cols[:, 6:7]

        @pl.loop(0, tp)
        def _(m):
            act, slope = gelu(dot_nt(wu_t, h2_all[m]) + bu_col)
            d_pre = dot_nt(wd_ref[...], dy_full_all[m]) * slope
            lanes = d_pre[:, :128]
            for i in range(1, seq_len // 128):
                lanes = lanes + d_pre[:, i * 128:(i + 1) * 128]
            acc_bias[...] += lanes
            gwd_ref[...] += dot(act, dy_full_all[m])
            acc_up[...] += dot(d_pre.astype(BF16), h2_all[m])

        gwu_ref[...] = acc_up[...].T
        gbu_ref[...] = jnp.broadcast_to(lane_sum(acc_bias[...]), acc_bias.shape).T[:8]
        near.wait()
        remote(part_gwq.at[0], far_gwq, red_send.at[4], red_recv.at[4], me ^ 2).wait()
        gwq_ref[...] = part[0] + near_last[...] + far_gwq[...]
        for move in small:
            move.wait()
        gb_out[...] = gb_rows[0] + gb_buf[0] + (gb_buf[1] + gb_buf[2])
        sums_out[...] = sums_mine[...] + sums_buf[0] + (sums_buf[1] + sums_buf[2])
        gx_move.wait()

    pl.run_scoped(tail, vm(wq_in), vm(x_in), vm(dx1t_in), vm(wu_in), vm(wd_in), pltpu.VMEM((tp, seq_len, width), BF16), pltpu.VMEM((tp, seq_len, width), BF16),
                  pltpu.VMEM((2, rows, width), F32), pltpu.VMEM((wd_in.shape[0], width), F32), pltpu.VMEM((wd_in.shape[0], 128), F32))


def finish_kernel(*refs):
    moved, small = refs[:6], refs[6:9]
    outs, vectors, bias_up, bias_qkv = refs[9:15], refs[15:21], refs[21], refs[22]
    bufs, load_sem, store_sem = refs[23:29], refs[29], refs[30]
    loads = [pltpu.make_async_copy(source, buf, load_sem.at[i]) for i, (source, buf) in enumerate(zip(moved, bufs))]
    stores = [pltpu.make_async_copy(buf, dst, store_sem.at[i]) for i, (buf, dst) in enumerate(zip(bufs, outs))]
    for load in loads:
        load.start()
    for load, store in zip(loads, stores):
        load.wait()
        store.start()
    sums, grad_up, grad_qkv = small
    for i, vector in enumerate(vectors):
        vector[...] = sums[i]
    bias_up[...] = grad_up[0]
    heads, kinds, head_dim = bias_qkv.shape
    row = grad_qkv[:1]
    for j in range(heads):
        for which in range(kinds):
            at = (which * heads + j) * head_dim
            bias_qkv[j, which:which + 1] = row[:, at:at + head_dim]
    for store in stores:
        store.wait()


VMEM_SPEC = pl.BlockSpec(memory_space=pltpu.VMEM)
ANY_SPEC = pl.BlockSpec(memory_space=pl.ANY)


def shape(dims, dtype=BF16):
    return jax.ShapeDtypeStruct(dims, dtype)


def single_call(kernel, name, collective_id, ins, in_any, outs, out_any, scratch, limit=67043328):
    dma = pltpu.SemaphoreType.DMA
    return pl.pallas_call(
        kernel,
        out_shape=outs,
        in_specs=[ANY_SPEC if i in in_any else VMEM_SPEC for i in range(len(ins))],
        out_specs=[ANY_SPEC if i in out_any else VMEM_SPEC for i in range(len(outs))],
        scratch_shapes=[dma(s) if isinstance(s, tuple) else pltpu.VMEM(s.shape, s.dtype) for s in scratch],
        compiler_params=pltpu.CompilerParams(collective_id=collective_id, has_side_effects=collective_id is not None, vmem_limit_bytes=limit),
        name=name,
    )(*ins)


def solution(mesh):
    tp = mesh.shape['tp']
    act_spec = P('dp', 'tp', None)
    rep_vec = P(None)
    part_vec = P('dp')
    in_specs = (act_spec, act_spec, P('dp', None), rep_vec, rep_vec, P(None, None, 'tp', None), P(None, 'tp', None),
                P('tp', None, None), rep_vec, rep_vec, rep_vec, P(None, 'tp'), P('tp'), P('tp', None), rep_vec)
    out_specs = (act_spec, act_spec, part_vec, part_vec, P('dp', None, 'tp', None), P('dp', 'tp', None),
                 P(('dp', 'tp'), None, None), part_vec, part_vec, part_vec, P('dp', 'tp'), P(('dp', 'tp')),
                 P(('dp', 'tp'), None), part_vec)

    def device_step(x_in, grad_y, pad_mask, ln1_gain, ln1_bias, w_qkv, b_qkv, w_out, b_out, ln2_gain, ln2_bias, w_up, b_up, w_down, b_down):
        seq_len = pad_mask.shape[1]
        local_heads, head_dim = w_qkv.shape[2:]
        chunk, width = x_in.shape[1:]
        ff = w_up.shape[1]
        heads = local_heads * tp
        group = local_heads * head_dim
        qkv_rows = 3 * group
        ext = head_dim + head_dim // 2
        low_rows = seq_len // 4
        dims = (local_heads, head_dim)
        cos_tab, sin_tab = (jnp.asarray(table) for table in rope_tables(seq_len, head_dim))
        wq_own = w_qkv.transpose(0, 2, 3, 1).reshape(2, qkv_rows // 2, width)
        bq_own = b_qkv.transpose(1, 0, 2)
        wo_own = w_out.reshape(2, group // 2, width)
        wu_own = w_up.reshape(2, width // 2, ff)
        wd_own = w_down.reshape(2, ff // 2, width)
        act = shape((seq_len, width))
        by_head = shape((heads, head_dim, seq_len))
        ext_head = shape((heads, ext, seq_len))
        held = [act, shape((tp,) + wq_own.shape), act, ext_head, ext_head, by_head, by_head, shape(by_head.shape, F32), shape((heads, 1, seq_len), F32)]
        d_x1_t = shape((width, seq_len), F32)
        rows8 = shape((8, width), F32)
        ins = (x_in, wq_own, bq_own, pad_mask, b_out, ln2_gain, ln2_bias, b_down, ln1_gain, ln1_bias, b_up, cos_tab, sin_tab, wo_own, wu_own, wd_own, grad_y)
        outs = held + [act, act, d_x1_t, act, by_head, act, shape((tp - 1, low_rows, width)), shape((2, chunk, width)), rows8, rows8]
        scratch = held + [shape((width, seq_len)), shape((tp,) + bq_own.shape, F32), shape((tp,) + wo_own.shape), shape((tp,) + wu_own.shape), shape((tp,) + wd_own.shape), shape((tp,) + rows8.shape, F32), act,
                          shape((tp, ff, seq_len)), shape((3, seq_len, width)), d_x1_t, (5,), (11,), (6, 4), (4,), (4,), (6,), (6,), (3, 3), (3, 3), (4, 5), (4, 5)]
        (x_full, wq_all, h1, q_ext, k_ext, v_heads, attn_o, attn_wide, lse, y_seq, h2, dx1_t, dx1_b, d_o, dy_full, h2_low, dy_cross, mid_sums, vec) = single_call(
            functools.partial(forward_kernel, (chunk,) + dims), 'forward', 0, ins, (0, 1, 2, 13, 14, 15, 16), outs, range(17), scratch)
        ins = (q_ext, k_ext, v_heads, d_o, attn_wide, lse, cos_tab, sin_tab, attn_o, dx1_b, h1, h2, grad_y, dy_full, y_seq, wq_all.reshape(tp, qkv_rows, width), x_full, dx1_t, mid_sums, vec, w_up, w_down, h2_low, dy_cross)
        gwq = shape((qkv_rows, width), F32)
        gwo = shape((group, width), F32)
        outs = [shape((tp, chunk, width)), gwo, shape((tp, chunk, width)), gwq, shape((8, qkv_rows), F32), rows8, shape(w_up.shape, F32), shape((8, ff), F32), shape(w_down.shape, F32),
                shape((tp - 1, seq_len - low_rows, width)), shape((tp - 1, seq_len, width))]
        scratch = [shape((tp, qkv_rows, seq_len)), shape((tp, qkv_rows, 128), F32), act, shape((2, group, width), F32), gwo, gwq, gwq, gwq, shape((2, qkv_rows, width), F32), shape((tp, 8, qkv_rows), F32), shape((3, 8, qkv_rows), F32), rows8, shape((3, 8, width), F32), act,
                   (5,), (6, 4), (3,), (16,), (6,), (6,), (2, 4), (2, 4), (3,), (3,), (5,), (5,), (4,), (4,), (4,), (4,)]
        y_out, grad_w_out, grad_x, grad_w_qkv, grad_b_qkv, sums, grad_w_up, grad_b_up, grad_w_down, _, _ = single_call(
            functools.partial(backward_kernel, dims), 'backward', 1, ins, set(range(len(ins))) - {6, 7, 18, 19}, outs, (0, 9, 10), scratch)
        moved = (y_out, grad_x, grad_w_qkv, grad_w_out, grad_w_up, grad_w_down)
        ins = moved + (sums, grad_b_up, grad_b_qkv)
        vector = shape((width,), F32)
        moved_shapes = [shape(a.shape, a.dtype) for a in moved]
        outs = moved_shapes + [vector] * 6 + [shape((ff,), F32), shape((local_heads, 3, head_dim), F32)]
        y_out, grad_x, grad_w_qkv, grad_w_out, grad_w_up, grad_w_down, *vectors, grad_b_up, grad_b_qkv = single_call(
            finish_kernel, 'finish', None, ins, range(6), outs, range(6), moved_shapes + [(6,), (6,)])
        grad_w_qkv = grad_w_qkv.reshape(3, local_heads, head_dim, width).transpose(0, 3, 1, 2)
        grad_b_qkv = grad_b_qkv.transpose(1, 0, 2)
        grad_w_out = grad_w_out.reshape(local_heads, head_dim, width)
        return (y_out, grad_x, vectors[4], vectors[5], grad_w_qkv, grad_b_qkv, grad_w_out, vectors[3],
                vectors[1], vectors[2], grad_w_up, grad_b_up, grad_w_down, vectors[0])

    return jax.shard_map(device_step, mesh=mesh, in_specs=in_specs, out_specs=out_specs, check_vma=False)
```

```python
import functools

import jax
import jax.numpy as jnp
import numpy as np
from jax import lax
from jax.experimental import pallas as pl
from jax.experimental.pallas import tpu as pltpu
from jax.sharding import PartitionSpec as P

LN_EPS = 1e-5
ROPE_BASE = 10000.0
INV_SQRT2 = 0.7071067811865476
INV_SQRT_2PI = 0.3989422804014327
NEG_LARGE = -1e30
F32 = jnp.float32
BF16 = jnp.bfloat16
MESH = pl.DeviceIdType.MESH


def dot(lhs, rhs):
    return jnp.dot(lhs, rhs, preferred_element_type=F32)


def layer_norm(values, ln_gain, ln_bias):
    centered = values - jnp.mean(values, axis=-1, keepdims=True)
    inv_std = lax.rsqrt(jnp.mean(centered * centered, axis=-1, keepdims=True) + LN_EPS)
    x_hat = centered * inv_std
    return x_hat * ln_gain + ln_bias, x_hat, inv_std


def rope_tables(seq_len, head_dim):
    half_dim = head_dim // 2
    inv_freq = np.float32(ROPE_BASE) ** (np.float32(-2.0) * np.arange(half_dim, dtype=np.float32) / np.float32(head_dim))
    angles = inv_freq[:, None] * np.arange(seq_len, dtype=np.float32)[None, :]
    return np.cos(angles), np.sin(angles)


def remote(src, dst, send_sem, recv_sem, device):
    return pltpu.make_async_remote_copy(src_ref=src, dst_ref=dst, send_sem=send_sem, recv_sem=recv_sem, device_id={'tp': device}, device_id_type=MESH)


def greet(me, groups=False):
    barrier = pltpu.get_barrier_semaphore()
    for mask in (1, 2, 3):
        pl.semaphore_signal(barrier, inc=1, device_id={'tp': me ^ mask}, device_id_type=MESH)
    if groups:
        pl.semaphore_signal(barrier, inc=1, device_id={'dp': lax.axis_index('dp') ^ 1}, device_id_type=MESH)
    pl.semaphore_wait(barrier, 4 if groups else 3)


class Gather:
    def __init__(self, src, dst, base, send_sem, recv_sem, me):
        self.near = remote(src, dst.at[1 - base], send_sem.at[0], recv_sem.at[0], me ^ 1)
        self.far = remote(src, dst.at[2 - base], send_sem.at[1], recv_sem.at[1], me ^ 2)
        self.relay = remote(dst.at[2 - base], dst.at[3 - base], send_sem.at[2], recv_sem.at[2], me ^ 1)

    def start(self):
        self.far.start()
        self.near.start()

    def forward(self):
        self.far.wait_recv()
        self.relay.start()

    def finish(self):
        self.near.wait()
        self.far.wait_send()
        self.relay.wait()


class SharedGather:
    def __init__(self, src, dst, send_sem, recv_sem, me):
        group = lax.axis_index('dp')
        half, rest = group, group ^ 1
        self.near = remote(src, dst.at[1], send_sem.at[0], recv_sem.at[0], me ^ 1)
        self.far = remote(src.at[half], dst.at[2, half], send_sem.at[1], recv_sem.at[1], me ^ 2)
        self.side = pltpu.make_async_remote_copy(src_ref=dst.at[2, half], dst_ref=dst.at[2, half], send_sem=send_sem.at[2], recv_sem=recv_sem.at[2], device_id={'dp': rest}, device_id_type=MESH)
        self.relay = Copies([remote(dst.at[2, part], dst.at[3, part], send_sem.at[3 + i], recv_sem.at[3 + i], me ^ 1) for i, part in enumerate((half, rest))])

    def start(self):
        self.far.start()
        self.near.start()

    def forward(self):
        self.far.wait_recv()
        self.side.start()
        self.relay.copies[0].start()

    def forward_rest(self):
        self.side.wait_recv()
        self.relay.copies[1].start()

    def wait_send(self):
        for copy in (self.near, self.far, self.side, self.relay):
            copy.wait_send()


def layer_norm_rows(values, ln_gain, ln_bias):
    centered = values - jnp.mean(values, axis=0, keepdims=True)
    inv_std = lax.rsqrt(jnp.mean(centered * centered, axis=0, keepdims=True) + LN_EPS)
    x_hat = centered * inv_std
    return x_hat * ln_gain + ln_bias, x_hat, inv_std


def layer_norm_rows_grad(d_out, x_hat, inv_std, ln_gain):
    d_hat = d_out * ln_gain
    return inv_std * (d_hat - jnp.mean(d_hat, axis=0, keepdims=True) - x_hat * jnp.mean(d_hat * x_hat, axis=0, keepdims=True))


def dot_tn(lhs, rhs):
    return lax.dot_general(lhs, rhs, (((0,), (0,)), ((), ())), preferred_element_type=F32)


def dot_nt(lhs, rhs):
    return lax.dot_general(lhs, rhs, (((1,), (1,)), ((), ())), preferred_element_type=F32)


def gelu(pre_act):
    half_erf = 0.5 * (1.0 + lax.erf(pre_act * INV_SQRT2))
    act = (pre_act * half_erf).astype(BF16)
    return act, half_erf + pre_act * jnp.exp(-0.5 * pre_act * pre_act) * INV_SQRT_2PI


class Copies:
    def __init__(self, copies):
        self.copies = copies

    def start(self):
        for copy in self.copies:
            copy.start()

    def wait(self):
        for copy in self.copies:
            copy.wait()

    def wait_recv(self):
        for copy in self.copies:
            copy.wait_recv()

    def wait_send(self):
        for copy in self.copies:
            copy.wait_send()


def rows_of(owner, chunk):
    return pl.ds(pl.multiple_of(owner * chunk, chunk), chunk)


def to_sequence(src, dst, send_sem, recv_sem, me, chunk):
    return Copies([remote(src.at[me ^ mask], dst.at[rows_of(me, chunk)], send_sem.at[mask], recv_sem.at[mask], me ^ mask) for mask in (2, 3, 1)])


def from_sequence(src, dst, send_sem, recv_sem, me, chunk):
    return Copies([remote(src.at[rows_of(me ^ mask, chunk)], dst.at[me], send_sem.at[mask], recv_sem.at[mask], me ^ mask) for mask in (2, 3, 1)])


def lane_sum(value):
    return jnp.sum(value, axis=1, keepdims=True)


def forward_kernel(dims, x_ref, wq_ref, bq_ref, mask_ref, b_out_ref, gain2_ref, bias2_ref, b_down_ref, gain1_ref, bias1_ref, b_up_ref, cos_ref, sin_ref, wo_ref, wu_ref, wd_ref, dy_ref,
                   x_out, wq_out, h1_out, q_out, k_out, v_out, o_out, wide_out, lse_out, y_out, h2_out, dx1t_out, dx1b_out, do_out, dy_out, h2_all, dy_cross, sums_ref, vec_ref,
                   x_full, wq_all, h1_ref, q_all, k_all, v_all, o_ref, wide_ref, lse_ref, h1t_ref, bq_all, wo_all, wu_all, wd_all, vec_all, dy_full,
                   act_ref, stage_ref, wide_stage, own_sem, once_sem, store_sem, x_send, x_recv, dy_send, dy_recv, send_sem, recv_sem, wide_send, wide_recv):
    chunk, local_heads, head_dim = dims
    me = lax.axis_index('tp')
    half = head_dim // 2
    seq_len, width = x_full.shape
    tp, ff = wu_all.shape[0], wu_ref.shape[2]
    for i, row in enumerate((b_out_ref, gain2_ref, bias2_ref, b_down_ref, gain1_ref, bias1_ref, b_up_ref, b_up_ref)):
        vec_ref[i:i + 1] = row[...].reshape(1, width)
    greet(me, True)
    x_move = to_sequence(x_ref, x_full, x_send, x_recv, me, chunk)
    dy_move = to_sequence(dy_ref, dy_full, dy_send, dy_recv, me, chunk)
    dy_far = Copies([remote(dy_ref.at[me ^ i], dy_cross.at[i], dy_send.at[4 + i], dy_recv.at[4 + i], me ^ 2) for i in (0, 1)])
    vec_all[0] = vec_ref[...]
    gathered = ((bq_ref, bq_all), (vec_ref, vec_all))
    moves = [Gather(source, dst, 0, send_sem.at[i], recv_sem.at[i], me) for i, (source, dst) in enumerate(gathered)]
    bq, vec = moves
    weights = ((wq_ref, wq_all), (wo_ref, wo_all), (wu_ref, wu_all), (wd_ref, wd_all))
    shared = [SharedGather(source, dst, wide_send.at[i], wide_recv.at[i], me) for i, (source, dst) in enumerate(weights)]
    wq, wo, wu, wd = shared
    own = [pltpu.make_async_copy(source, dst.at[0], own_sem.at[i]) for i, (source, dst) in enumerate(gathered[:1] + weights)]
    x_move.start()
    bq.start()
    wq.start()
    for copy in own:
        copy.start()
    vec.start()
    wo.start()
    own_rows = rows_of(me, chunk)
    own_x = pltpu.make_async_copy(x_ref.at[me], x_full.at[own_rows], once_sem.at[0])
    own_dy = pltpu.make_async_copy(dy_ref.at[me], dy_full.at[own_rows], once_sem.at[1])
    own_x.start()
    own_dy.start()
    valid = mask_ref[pl.ds(me, 1)] > 0
    first = lax.broadcasted_iota(jnp.int32, (half, seq_len), 0) == 0
    ones = first.astype(F32).astype(BF16)
    key_bias = jnp.where(first, jnp.where(valid, 0.0, NEG_LARGE), 0.0).astype(BF16)
    for copy in own:
        copy.wait()
    own_x.wait()
    x_move.wait_recv()
    for move in (wu, wd, dy_move, dy_far):
        move.start()
    h1, _, _ = layer_norm(x_full[...].astype(F32), vec_all[0, 4:5], vec_all[0, 5:6])
    h1 = h1.astype(BF16)
    h1_ref[...] = h1
    h1t_ref[...] = h1.T
    once = [pltpu.make_async_copy(source, dst, once_sem.at[2 + i]) for i, (source, dst) in enumerate((
        (x_full, x_out), (h1_ref, h1_out), (wq_all, wq_out), (stage_ref.at[0], h2_out), (stage_ref.at[1], y_out), (stage_ref.at[2], dx1b_out), (wide_stage, dx1t_out), (dy_full, dy_out)))]
    once[0].start()
    once[1].start()

    def stores(m):
        heads = pl.ds(m * local_heads, local_heads)
        pairs = ((q_all, q_out), (k_all, k_out), (v_all, v_out), (o_ref, o_out), (wide_ref, wide_out), (lse_ref, lse_out))
        return Copies([pltpu.make_async_copy(source.at[heads], dst.at[heads], store_sem.at[i, m]) for i, (source, dst) in enumerate(pairs)])

    @pl.loop(0, 4)
    def _(m):
        @pl.when(m == 1)
        def _():
            bq.near.wait_recv()
            wq.near.wait_recv()
            bq.forward()
            wq.forward()

        @pl.when(m == 2)
        def _():
            wq.forward_rest()
            vec.forward()
            wo.forward()
            wu.forward()

        @pl.when(m == 3)
        def _():
            bq.relay.wait_recv()
            wq.relay.wait_recv()
            once[2].start()
            wo.forward_rest()
            wd.forward()

        biases = [bq_all[m, j].T for j in range(local_heads)]
        qkv = dot(wq_all[m].reshape(3 * local_heads * head_dim, width), h1t_ref[...])
        cos, sin = cos_ref[...], sin_ref[...]
        group = local_heads * head_dim
        for j in range(local_heads):
            head = m * local_heads + j
            for which, (dst, scale, extra) in enumerate(((q_all, head_dim ** -0.5, ones), (k_all, None, key_bias))):
                rows = qkv[which * group + j * head_dim:which * group + (j + 1) * head_dim] + biases[j][:, which:which + 1]
                rows = rows * scale if scale is not None else rows
                low, high = rows[:half], rows[half:]
                dst[head, :half] = (low * cos - high * sin).astype(BF16)
                dst[head, half:head_dim] = (high * cos + low * sin).astype(BF16)
                dst[head, head_dim:] = extra
            v_all[head] = (qkv[2 * group + j * head_dim:2 * group + (j + 1) * head_dim] + biases[j][:, 2:3]).astype(BF16)

        coming = dot(k_all[m * local_heads].T, q_all[m * local_heads])
        for j in range(local_heads):
            head, scores = m * local_heads + j, coming
            top = jnp.max(scores, axis=0, keepdims=True)
            if j + 1 < local_heads:
                coming = dot(k_all[head + 1].T, q_all[head + 1])
            weights = jnp.exp(scores - top)
            total = jnp.sum(weights, axis=0, keepdims=True)
            out = dot(v_all[head], weights.astype(BF16)) / total
            o_ref[head] = out.astype(BF16)
            wide_ref[head] = out
            lse_ref[head] = top + jnp.log(total)

        stores(m).start()

    wu.forward_rest()
    for move in (vec, wo):
        move.near.wait_recv()
        move.relay.wait_recv()
    rows = tp * local_heads * head_dim
    wo_full = wo_all[...].reshape(rows, width)
    cols = vec_all[0].T
    b_out, gain, bias, b_down = (cols[:, i:i + 1] for i in range(4))
    attn = dot_tn(wo_full, o_ref[...].reshape(rows, seq_len))
    x1 = (x_full[...].T.astype(F32) + (attn + b_out)).astype(BF16).astype(F32)
    h2_f, x_hat, inv_std = layer_norm_rows(x1, gain, bias)
    h2 = h2_f.astype(BF16)
    stage_ref[0] = h2.T
    wu.near.wait_recv()
    wu.relay.wait_recv()
    h2_move = Gather(stage_ref.at[0, :h2_all.shape[1]], h2_all, 1, send_sem.at[2], recv_sem.at[2], me)

    def mlp(slope_ref):
        @pl.loop(0, tp)
        def _(m):
            @pl.when(m == 1)
            def _():
                wd.forward_rest()
                h2_move.start()
                once[3].start()

            pre_act = dot_tn(wu_all[m].reshape(width, ff), h2) + vec_all[m].T[:, 6:7]
            act, slope = gelu(pre_act)
            act_ref[m] = act
            slope_ref[m] = slope

        wd.near.wait_recv()
        wd.relay.wait_recv()
        out = dot_tn(wd_all[...].reshape(tp * ff, width), act_ref[...].reshape(tp * ff, seq_len))
        stage_ref[1] = (x1 + (out + b_down)).astype(BF16).T
        own_dy.wait()
        dy_move.wait_recv()
        once[7].start()
        dy_t = dy_full[...].T
        wide_stage[...] = jnp.zeros_like(wide_stage)

        @pl.loop(0, tp)
        def _(m):
            @pl.when(m == 1)
            def _():
                once[4].start()

            d_pre = (dot(wd_all[m].reshape(ff, width), dy_t) * slope_ref[m]).astype(BF16)
            wide_stage[...] += dot(wu_all[m].reshape(width, ff), d_pre)

    pl.run_scoped(mlp, pltpu.VMEM((tp, ff, seq_len), F32))
    d_h2 = wide_stage[...]
    dy_f = dy_full[...].T.astype(F32)
    d_x1 = dy_f + layer_norm_rows_grad(d_h2, x_hat, inv_std, gain)
    d_x1_b = d_x1.astype(BF16)
    wide_stage[...] = d_x1
    stage_ref[2] = d_x1_b.T
    for m in range(4):
        stores(m).wait()
    o_ref[...] = dot(wo_full, d_x1_b).astype(BF16).reshape(o_ref.shape)
    h2_move.forward()
    once[5].start()
    once[6].start()
    sums = [lane_sum(dy_f), lane_sum(d_h2 * x_hat), lane_sum(d_h2), lane_sum(d_x1)]
    sums_ref[...] = jnp.concatenate(sums + [jnp.zeros((width, 124), F32)], axis=1).T[:8]
    last = pltpu.make_async_copy(o_ref, do_out, once_sem.at[10])
    last.start()
    x_move.wait_send()
    dy_move.wait_send()
    dy_far.wait()
    for move in moves:
        move.near.wait_send()
        move.far.wait_send()
        move.relay.wait_send()
    for move in shared:
        move.wait_send()
    for copy in once:
        copy.wait()
    last.wait()
    h2_move.finish()


def backward_kernel(dims, q_in, k_in, v_in, do_in, wide_in, lse_in, cos_ref, sin_ref, o_in, dx1b_in, h1_in, h2_ref, dy_ref, dy_full, y_ref,
                    wq_in, x_in, dx1t_in, sums_ref, vec_ref, wu_in, wd_in, h2_low, dy_cross,
                    y_out, gwo_ref, gx_ref, gwq_ref, gb_out, sums_out, gwu_ref, gbu_ref, gwd_ref, h2_high, dy_all,
                    dqkv_ref, gb_ref, h1_ref, near_buf, far_buf, near_gwq, far_gwq, near_last, part_gwq, gb_rows, gb_buf, sums_mine, sums_buf, gx_seq,
                    own_sem, load_sem, first_sem, tail_sem, red_send, red_recv, small_send, small_recv, h2_send, h2_recv, dy_send, dy_recv, y_send, y_recv, gx_send, gx_recv):
    local_heads, head_dim = dims
    me = lax.axis_index('tp')
    tp, chunk, width = dy_ref.shape
    half = head_dim // 2
    group = local_heads * head_dim
    rows = 3 * group
    seq_len = tp * chunk
    low_rows = h2_low.shape[1]
    mine, across, partner = rows_of(me, chunk), rows_of(me ^ 2, chunk), me ^ 1
    greet(me)
    h2_move = Gather(h2_ref.at[low_rows:], h2_high, 1, h2_send, h2_recv, me)
    y_move = from_sequence(y_ref, y_out, y_send, y_recv, me, chunk)
    dy_near = Copies([remote(source, dst, dy_send.at[i], dy_recv.at[i], partner) for i, (source, dst) in enumerate((
        (dy_full, dy_all.at[0]), (dy_ref.at[me ^ 2], dy_all.at[2, mine]), (dy_ref.at[me ^ 3], dy_all.at[1, mine])))])
    dy_relay = Copies([remote(dy_cross.at[i], dy_all.at[2 - i, across], dy_send.at[3 + i], dy_recv.at[3 + i], partner) for i in (0, 1)])
    own = Copies([pltpu.make_async_copy(dy_ref.at[me ^ 2], dy_all.at[1, mine], own_sem.at[0]), pltpu.make_async_copy(dy_ref.at[me ^ 3], dy_all.at[2, mine], own_sem.at[1]),
                  pltpu.make_async_copy(y_ref.at[mine], y_out.at[me], own_sem.at[2])]
                 + [pltpu.make_async_copy(dy_cross.at[i], dy_all.at[1 + i, across], own_sem.at[3 + i]) for i in (0, 1)])
    h2_move.start()
    y_move.start()
    dy_near.start()
    dy_relay.start()
    cos, sin = cos_ref[...], sin_ref[...]

    def store(m, j, which, low, high):
        grad = jnp.concatenate([low, high], axis=0)
        at = pl.ds(pl.multiple_of(which * group + j * head_dim, head_dim), head_dim)
        dqkv_ref[m, at] = grad.astype(BF16)
        gb_ref[m, at] = jnp.broadcast_to(lane_sum(grad), (head_dim, 128))

    def back(grad):
        low, high = grad[:half], grad[half:]
        return low * cos + high * sin, high * cos - low * sin

    def attention(q_all, k_all, v_all, do_ref, wide_ref, lse_ref, o_ref, dx1b_ref, part):
        def loads(m):
            heads = pl.ds(m * local_heads, local_heads)
            pairs = ((q_in, q_all), (k_in, k_all), (v_in, v_all), (do_in, do_ref), (wide_in, wide_ref), (lse_in, lse_ref))
            return Copies([pltpu.make_async_copy(source.at[heads], dst.at[heads], load_sem.at[i, m]) for i, (source, dst) in enumerate(pairs)])

        early = Copies([pltpu.make_async_copy(source, dst, first_sem.at[i]) for i, (source, dst) in enumerate(((o_in, o_ref), (dx1b_in, dx1b_ref), (h1_in, h1_ref)))])
        early.start()
        for m in range(tp - 1, -1, -1):
            loads(m).start()
        own.start()
        reduce_near = Copies([remote(part.at[source], near_buf.at[i], red_send.at[i], red_recv.at[i], partner) for i, source in enumerate((1, 3))])
        reduce_far = remote(part.at[2], far_buf, red_send.at[2], red_recv.at[2], me ^ 2)
        gwq_near = remote(part_gwq.at[1], near_gwq, red_send.at[3], red_recv.at[3], partner)
        gwq_far = remote(part_gwq.at[0], far_gwq, red_send.at[4], red_recv.at[4], me ^ 2)
        early.wait()

        @pl.loop(0, tp)
        def _(m):
            heads = pl.ds(m * local_heads, local_heads)
            part[m] = dot(o_ref[heads].reshape(group, seq_len), dx1b_ref[...])

        @pl.loop(0, tp * local_heads)
        def _(step):
            m = tp - 1 - lax.div(step, local_heads)
            j = lax.rem(step, local_heads)
            head = m * local_heads + j

            @pl.when(j == 0)
            def _():
                loads(m).wait()

            @pl.when(step == 1)
            def _():
                reduce_near.start()

            @pl.when(step == 3)
            def _():
                reduce_near.wait()
                part[0] += near_buf[0]
                part[2] += near_buf[1]

            @pl.when(step == 4)
            def _():
                reduce_far.start()

            @pl.when(step == 9)
            def _():
                h2_move.forward()

            @pl.when(step == 10)
            def _():
                @pl.loop(0, 2)
                def _(i):
                    part_gwq[i] = dot(dqkv_ref[2 + i], h1_ref[...])

            @pl.when(step == 11)
            def _():
                gwq_near.start()

            @pl.when(step == 12)
            def _():
                gwq_near.wait()
                part_gwq[0] += near_gwq[...]

            @pl.when(step == 13)
            def _():
                gwq_far.start()

            q, k, v, d_out = q_all[head], k_all[head], v_all[head], do_ref[head]
            delta = jnp.sum(d_out.astype(F32) * wide_ref[head], axis=0, keepdims=True)
            probs = jnp.exp(dot(k.T, q) - lse_ref[head])
            d_probs = dot(v.T, d_out)
            d_scores = (probs * (d_probs - delta)).astype(BF16)
            d_value = dot(probs.astype(BF16), d_out.T).T
            d_key = dot(d_scores, q[:head_dim].T).T
            d_query = dot(k[:head_dim], d_scores)
            low, high = back(d_query)
            scale = head_dim ** -0.5
            store(m, j, 0, low * scale, high * scale)
            low, high = back(d_key)
            store(m, j, 1, low, high)
            store(m, j, 2, d_value[:half], d_value[half:])

        own.wait()
        y_move.wait()
        h2_move.finish()
        dy_near.wait()
        dy_relay.wait()
        reduce_far.wait()
        gwo_ref[...] = part[0] + far_buf[...]

    heads_all = tp * local_heads

    def vm(array):
        return pltpu.VMEM(array.shape, array.dtype)

    pl.run_scoped(attention, vm(q_in), vm(k_in), vm(v_in), vm(do_in), vm(wide_in), vm(lse_in), vm(o_in), vm(dx1b_in), pltpu.VMEM((tp, group, width), F32))

    def tail(wq_ref, x_ref, dx1t_ref, wu_ref, wd_ref, h2_all, dy_full_all, part, acc_up, acc_bias):
        first = [pltpu.make_async_copy(source, dst, tail_sem.at[i]) for i, (source, dst) in enumerate(((wq_in, wq_ref), (x_in, x_ref), (dx1t_in, dx1t_ref), (wu_in, wu_ref), (wd_in, wd_ref)))]
        for m in range(tp):
            if m == 0:
                first.append(pltpu.make_async_copy(h2_ref, h2_all.at[0], tail_sem.at[5]))
                first.append(pltpu.make_async_copy(dy_full, dy_full_all.at[0], tail_sem.at[6]))
            else:
                first.append(pltpu.make_async_copy(h2_low.at[m - 1], h2_all.at[m, :low_rows], tail_sem.at[4 + 3 * m]))
                first.append(pltpu.make_async_copy(h2_high.at[m - 1], h2_all.at[m, low_rows:], tail_sem.at[5 + 3 * m]))
                first.append(pltpu.make_async_copy(dy_all.at[m - 1], dy_full_all.at[m], tail_sem.at[6 + 3 * m]))
        for load in first:
            load.start()
        near = remote(part.at[1], near_last, red_send.at[5], red_recv.at[5], partner)

        @pl.loop(0, 2)
        def _(i):
            part[i] = dot(dqkv_ref[i], h1_ref[...])

        cols = vec_ref[...].T
        gain, bias = cols[:, 4:5], cols[:, 5:6]
        first[0].wait()
        near.start()
        d_h1 = dot_tn(wq_ref[...].reshape(tp * rows, width), dqkv_ref[...].reshape(tp * rows, seq_len))
        for load in first[1:]:
            load.wait()
        _, x_hat, inv_std = layer_norm_rows(x_ref[...].T.astype(F32), gain, bias)
        grad_x = (dx1t_ref[...] + layer_norm_rows_grad(d_h1, x_hat, inv_std, gain)).astype(BF16)
        gx_seq[...] = grad_x.T
        sums = [lane_sum(d_h1 * x_hat), lane_sum(d_h1)]
        ln1 = jnp.concatenate(sums + [jnp.zeros((width, 126), F32)], axis=1).T
        sums_mine[...] = jnp.concatenate([sums_ref[:4], ln1[:4]], axis=0)
        gx_ref[me] = gx_seq[mine]
        for m in range(tp):
            gb_rows[m] = gb_ref[m].T[:8]
        small = [remote(gb_rows.at[m], gb_buf.at[m - 1], small_send.at[0, m], small_recv.at[0, m], me ^ m) for m in (1, 2, 3)]
        small += [remote(sums_mine, sums_buf.at[m - 1], small_send.at[1, m], small_recv.at[1, m], me ^ m) for m in (1, 2, 3)]
        for move in small:
            move.start()
        gx_move = from_sequence(gx_seq, gx_ref, gx_send, gx_recv, me, chunk)
        gx_move.start()
        acc_up[...] = jnp.zeros_like(acc_up)
        acc_bias[...] = jnp.zeros_like(acc_bias)
        gwd_ref[...] = jnp.zeros_like(gwd_ref)
        wu_t = wu_ref[...].T
        bu_col = cols[:, 6:7]

        @pl.loop(0, tp)
        def _(m):
            act, slope = gelu(dot_nt(wu_t, h2_all[m]) + bu_col)
            d_pre = dot_nt(wd_ref[...], dy_full_all[m]) * slope
            lanes = d_pre[:, :128]
            for i in range(1, seq_len // 128):
                lanes = lanes + d_pre[:, i * 128:(i + 1) * 128]
            acc_bias[...] += lanes
            gwd_ref[...] += dot(act, dy_full_all[m])
            acc_up[...] += dot(d_pre.astype(BF16), h2_all[m])

        gwu_ref[...] = acc_up[...].T
        gbu_ref[...] = jnp.broadcast_to(lane_sum(acc_bias[...]), acc_bias.shape).T[:8]
        near.wait()
        remote(part_gwq.at[0], far_gwq, red_send.at[4], red_recv.at[4], me ^ 2).wait()
        gwq_ref[...] = part[0] + near_last[...] + far_gwq[...]
        for move in small:
            move.wait()
        gb_out[...] = gb_rows[0] + gb_buf[0] + (gb_buf[1] + gb_buf[2])
        sums_out[...] = sums_mine[...] + sums_buf[0] + (sums_buf[1] + sums_buf[2])
        gx_move.wait()

    pl.run_scoped(tail, vm(wq_in), vm(x_in), vm(dx1t_in), vm(wu_in), vm(wd_in), pltpu.VMEM((tp, seq_len, width), BF16), pltpu.VMEM((tp, seq_len, width), BF16),
                  pltpu.VMEM((2, rows, width), F32), pltpu.VMEM((wd_in.shape[0], width), F32), pltpu.VMEM((wd_in.shape[0], 128), F32))


def finish_kernel(*refs):
    moved, small = refs[:6], refs[6:9]
    outs, vectors, bias_up, bias_qkv = refs[9:15], refs[15:21], refs[21], refs[22]
    bufs, load_sem, store_sem = refs[23:29], refs[29], refs[30]
    loads, stores = [], []
    for source, buf, dst in zip(moved, bufs, outs):
        rows, *_ = source.shape
        half = rows // 2
        for at in (slice(half), slice(half, rows)):
            sem = len(loads)
            loads.append(pltpu.make_async_copy(source.at[at], buf.at[at], load_sem.at[sem]))
            stores.append(pltpu.make_async_copy(buf.at[at], dst.at[at], store_sem.at[sem]))
    for load in loads:
        load.start()
    for load, store in zip(loads, stores):
        load.wait()
        store.start()
    sums, grad_up, grad_qkv = small
    for i, vector in enumerate(vectors):
        vector[...] = sums[i]
    bias_up[...] = grad_up[0]
    heads, kinds, head_dim = bias_qkv.shape
    row = grad_qkv[:1]
    for j in range(heads):
        for which in range(kinds):
            at = (which * heads + j) * head_dim
            bias_qkv[j, which:which + 1] = row[:, at:at + head_dim]
    for store in stores:
        store.wait()


VMEM_SPEC = pl.BlockSpec(memory_space=pltpu.VMEM)
ANY_SPEC = pl.BlockSpec(memory_space=pl.ANY)


def shape(dims, dtype=BF16):
    return jax.ShapeDtypeStruct(dims, dtype)


def single_call(kernel, name, collective_id, ins, in_any, outs, out_any, scratch, limit=67043328):
    dma = pltpu.SemaphoreType.DMA
    return pl.pallas_call(
        kernel,
        out_shape=outs,
        in_specs=[ANY_SPEC if i in in_any else VMEM_SPEC for i in range(len(ins))],
        out_specs=[ANY_SPEC if i in out_any else VMEM_SPEC for i in range(len(outs))],
        scratch_shapes=[dma(s) if isinstance(s, tuple) else pltpu.VMEM(s.shape, s.dtype) for s in scratch],
        compiler_params=pltpu.CompilerParams(collective_id=collective_id, has_side_effects=collective_id is not None, vmem_limit_bytes=limit),
        name=name,
    )(*ins)


def solution(mesh):
    tp = mesh.shape['tp']
    act_spec = P('dp', 'tp', None)
    rep_vec = P(None)
    part_vec = P('dp')
    in_specs = (act_spec, act_spec, P('dp', None), rep_vec, rep_vec, P(None, None, 'tp', None), P(None, 'tp', None),
                P('tp', None, None), rep_vec, rep_vec, rep_vec, P(None, 'tp'), P('tp'), P('tp', None), rep_vec)
    out_specs = (act_spec, act_spec, part_vec, part_vec, P('dp', None, 'tp', None), P('dp', 'tp', None),
                 P(('dp', 'tp'), None, None), part_vec, part_vec, part_vec, P('dp', 'tp'), P(('dp', 'tp')),
                 P(('dp', 'tp'), None), part_vec)

    def device_step(x_in, grad_y, pad_mask, ln1_gain, ln1_bias, w_qkv, b_qkv, w_out, b_out, ln2_gain, ln2_bias, w_up, b_up, w_down, b_down):
        seq_len = pad_mask.shape[1]
        local_heads, head_dim = w_qkv.shape[2:]
        chunk, width = x_in.shape[1:]
        ff = w_up.shape[1]
        heads = local_heads * tp
        group = local_heads * head_dim
        qkv_rows = 3 * group
        ext = head_dim + head_dim // 2
        low_rows = seq_len // 4
        dims = (local_heads, head_dim)
        cos_tab, sin_tab = (jnp.asarray(table) for table in rope_tables(seq_len, head_dim))
        wq_own = w_qkv.transpose(0, 2, 3, 1).reshape(2, qkv_rows // 2, width)
        bq_own = b_qkv.transpose(1, 0, 2)
        wo_own = w_out.reshape(2, group // 2, width)
        wu_own = w_up.reshape(2, width // 2, ff)
        wd_own = w_down.reshape(2, ff // 2, width)
        act = shape((seq_len, width))
        by_head = shape((heads, head_dim, seq_len))
        ext_head = shape((heads, ext, seq_len))
        held = [act, shape((tp,) + wq_own.shape), act, ext_head, ext_head, by_head, by_head, shape(by_head.shape, F32), shape((heads, 1, seq_len), F32)]
        d_x1_t = shape((width, seq_len), F32)
        rows8 = shape((8, width), F32)
        ins = (x_in, wq_own, bq_own, pad_mask, b_out, ln2_gain, ln2_bias, b_down, ln1_gain, ln1_bias, b_up, cos_tab, sin_tab, wo_own, wu_own, wd_own, grad_y)
        outs = held + [act, act, d_x1_t, act, by_head, act, shape((tp - 1, low_rows, width)), shape((2, chunk, width)), rows8, rows8]
        scratch = held + [shape((width, seq_len)), shape((tp,) + bq_own.shape, F32), shape((tp,) + wo_own.shape), shape((tp,) + wu_own.shape), shape((tp,) + wd_own.shape), shape((tp,) + rows8.shape, F32), act,
                          shape((tp, ff, seq_len)), shape((3, seq_len, width)), d_x1_t, (5,), (11,), (6, 4), (4,), (4,), (6,), (6,), (3, 3), (3, 3), (4, 5), (4, 5)]
        (x_full, wq_all, h1, q_ext, k_ext, v_heads, attn_o, attn_wide, lse, y_seq, h2, dx1_t, dx1_b, d_o, dy_full, h2_low, dy_cross, mid_sums, vec) = single_call(
            functools.partial(forward_kernel, (chunk,) + dims), 'forward', 0, ins, (0, 1, 2, 13, 14, 15, 16), outs, range(17), scratch)
        ins = (q_ext, k_ext, v_heads, d_o, attn_wide, lse, cos_tab, sin_tab, attn_o, dx1_b, h1, h2, grad_y, dy_full, y_seq, wq_all.reshape(tp, qkv_rows, width), x_full, dx1_t, mid_sums, vec, w_up, w_down, h2_low, dy_cross)
        gwq = shape((qkv_rows, width), F32)
        gwo = shape((group, width), F32)
        outs = [shape((tp, chunk, width)), gwo, shape((tp, chunk, width)), gwq, shape((8, qkv_rows), F32), rows8, shape(w_up.shape, F32), shape((8, ff), F32), shape(w_down.shape, F32),
                shape((tp - 1, seq_len - low_rows, width)), shape((tp - 1, seq_len, width))]
        scratch = [shape((tp, qkv_rows, seq_len)), shape((tp, qkv_rows, 128), F32), act, shape((2, group, width), F32), gwo, gwq, gwq, gwq, shape((2, qkv_rows, width), F32), shape((tp, 8, qkv_rows), F32), shape((3, 8, qkv_rows), F32), rows8, shape((3, 8, width), F32), act,
                   (5,), (6, 4), (3,), (16,), (6,), (6,), (2, 4), (2, 4), (3,), (3,), (5,), (5,), (4,), (4,), (4,), (4,)]
        y_out, grad_w_out, grad_x, grad_w_qkv, grad_b_qkv, sums, grad_w_up, grad_b_up, grad_w_down, _, _ = single_call(
            functools.partial(backward_kernel, dims), 'backward', 1, ins, set(range(len(ins))) - {6, 7, 18, 19}, outs, (0, 9, 10), scratch)
        moved = (y_out, grad_x, grad_w_qkv, grad_w_out, grad_w_up, grad_w_down)
        ins = moved + (sums, grad_b_up, grad_b_qkv)
        vector = shape((width,), F32)
        moved_shapes = [shape(a.shape, a.dtype) for a in moved]
        outs = moved_shapes + [vector] * 6 + [shape((ff,), F32), shape((local_heads, 3, head_dim), F32)]
        y_out, grad_x, grad_w_qkv, grad_w_out, grad_w_up, grad_w_down, *vectors, grad_b_up, grad_b_qkv = single_call(
            finish_kernel, 'finish', None, ins, range(6), outs, range(6), moved_shapes + [(12,), (12,)])
        grad_w_qkv = grad_w_qkv.reshape(3, local_heads, head_dim, width).transpose(0, 3, 1, 2)
        grad_b_qkv = grad_b_qkv.transpose(1, 0, 2)
        grad_w_out = grad_w_out.reshape(local_heads, head_dim, width)
        return (y_out, grad_x, vectors[4], vectors[5], grad_w_qkv, grad_b_qkv, grad_w_out, vectors[3],
                vectors[1], vectors[2], grad_w_up, grad_b_up, grad_w_down, vectors[0])

    return jax.shard_map(device_step, mesh=mesh, in_specs=in_specs, out_specs=out_specs, check_vma=False)
```
